128 devices in a mesh: band: 16 (over z_hi, x, core), ga: 8 (over y, z_lo).
Axes of the slice: x: 4, y: 4, z: 4 (z_hi: 2, z_lo: 2; z = z_hi * 2 + z_lo), core: 2. Of those that a mesh axis runs over, the one named last changes fastest.
Arguments:
- wave_coef: bfloat16 [8192, 32768], P('band', 'ga'), may hold values from -0.03125 to 0.03125
- projector: bfloat16 [64, 27, 32768], P('band', None, 'ga'), may hold values from -6 to 6
- occupation: float32 [8192], P('band'), may hold values from 0.25 to 4
- species: int32 [64], replicated, may hold values from 0 to 3
- layer_in: float32 [4, 729, 100], replicated, may hold values from -1.25 to 1.25
- bias_in: float32 [4, 100], replicated, may hold values from -3 to 3
- layer_out: float32 [4, 100], replicated, may hold values from -0.625 to 0.625
Outputs:
- corrected: bfloat16 [8192, 32768], P('band', 'ga')
The draws below stay inside these ranges and needn't reach their ends.
All inputs are finite; a program needn't handle non-finite values.
Results may differ from the reference program's by a relative error of at most 0.0049.
Values may be sent and summed in bfloat16 or wider, within the bound.
A program may use at most 128 MiB of HBM per device.

```python
import math
import jax
import jax.numpy as jnp
from jax import lax

K = 27
HID = 100
SPECIES = 4
NB = 8192
NG = 32768
ATOMS = 64


def plant(entries, own_key, smallest, top_value):
    place = [jax.random.randint(jax.random.fold_in(own_key, axis), (), 0, length) for axis, length in enumerate(entries.shape)]
    main_axis = entries.shape.index(max(entries.shape))
    beside = place[:main_axis] + [(place[main_axis] + 1) % entries.shape[main_axis]] + place[main_axis + 1:]
    return entries.at[tuple(place)].set(smallest).at[tuple(beside)].set(top_value)


def steps_of(stream_key, dims, split, low, high):
    level = 1.0
    for axis_at, blocks in split:
        draws = jax.random.uniform(jax.random.fold_in(jax.random.fold_in(stream_key, 6), axis_at), (blocks,), jnp.float32, low / len(split), high / len(split))
        level = level * jnp.repeat(jnp.exp(draws), dims[axis_at] // blocks).reshape((-1,) + (1,) * (len(dims) - 1 - axis_at))
    return level


def centred(rng, extent, scale, bound, cuts=(), held_as=jnp.bfloat16):
    gain = steps_of(rng, extent, cuts, -0.22, 0.18) if cuts else 1.0
    values = jax.random.normal(rng, extent, jnp.float32) * scale * gain
    return jnp.minimum(jnp.maximum(values, -bound), bound).astype(held_as)


def setup_inputs(seed: int = 0) -> dict:
    seeds = jax.random.split(jax.random.key(seed), 8)
    return {
        "wave_coef": centred(seeds[0], (NB, NG), NG ** -0.5, 0.03125, ((0, 16), (1, 8))),
        "projector": centred(seeds[1], (ATOMS, K, NG), 1.0, 6.0, ((0, 16), (2, 8))),
        "occupation": jnp.clip(jnp.exp(math.log(4.0) - 2.7725887 * jax.random.uniform(seeds[2], (NB,), jnp.float32) ** steps_of(seeds[2], (NB,), ((0, 16),), -0.2, 0.2)), 0.25, 4.0),
        "species": plant(jax.random.randint(seeds[3], (ATOMS,), 0, SPECIES), jax.random.fold_in(seeds[3], 1), 0, SPECIES - 1).astype(jnp.int32),
        "layer_in": centred(seeds[4], (SPECIES, K * K, HID), K ** -0.5, 1.25, (), jnp.float32),
        "bias_in": centred(seeds[5], (SPECIES, HID), 0.5, 3.0, (), jnp.float32),
        "layer_out": centred(seeds[6], (SPECIES, HID), HID ** -0.5, 0.625, (), jnp.float32),
    }


def reference(wave_coef, projector, occupation, species, layer_in, bias_in, layer_out):
    flattened = projector.reshape(ATOMS * K, NG)
    coefficient = lax.dot_general(wave_coef, flattened, (((1,), (1,)), ((), ())), preferred_element_type=jnp.float32)
    coefficient = coefficient.reshape(NB, ATOMS, K)
    density = jnp.einsum('n,nak,nal->akl', occupation, coefficient, coefficient, precision=lax.Precision.HIGHEST) / NB
    onehot = (species[:, None] == jnp.arange(SPECIES, dtype=jnp.int32)[None, :]).astype(jnp.float32)
    weight_atom = jnp.einsum('as,sfh->afh', onehot, layer_in, precision=lax.Precision.HIGHEST)
    bias_atom = jnp.dot(onehot, bias_in, precision=lax.Precision.HIGHEST)
    out_atom = jnp.dot(onehot, layer_out, precision=lax.Precision.HIGHEST)
    preact = jnp.einsum('af,afh->ah', density.reshape(ATOMS, K * K), weight_atom, precision=lax.Precision.HIGHEST) + bias_atom
    activation = jnp.tanh(preact)
    slopes = out_atom * (1.0 - activation * activation)
    gradient = jnp.einsum('afh,ah->af', weight_atom, slopes, precision=lax.Precision.HIGHEST).reshape(ATOMS, K, K)
    symmetric = gradient + jnp.swapaxes(gradient, 1, 2)
    factor = 1.0 / jnp.sqrt(jnp.float32(ATOMS * K))
    applied = (jnp.einsum('akl,nal->nak', symmetric, coefficient, precision=lax.Precision.HIGHEST) * factor).astype(jnp.bfloat16)
    corrected = jnp.dot(applied.reshape(NB, ATOMS * K), flattened, preferred_element_type=jnp.float32)
    return corrected.astype(jnp.bfloat16)
```

```python
import functools
import math

import jax
import jax.numpy as jnp
from jax import lax
from jax.experimental import pallas as pl
from jax.experimental.pallas import tpu as pltpu
from jax.sharding import PartitionSpec as P

MESH = pl.DeviceIdType.MESH
F32 = jnp.float32
BF16 = jnp.bfloat16

K = 27
KP = 28
SLOT = 4 * KP
PAIR = 2 * SLOT
NZ = 80
HID = 100

ORDER = ((0, 0), (0, 3), (0, 1), (1, 0), (1, 3), (1, 1), (0, 2), (1, 2))

TREE = (
    ("z10", 0, NZ), ("x10", NZ, 32),
    ("z03", 0, NZ), ("x03", NZ, 32), ("z01", 0, NZ), ("x01", NZ, 32),
    ("x02a", NZ, 16), ("x02b", NZ + 16, 16), ("z02a", 0, 48), ("z02b", 48, 32),
    ("z13", 0, NZ), ("z11", 0, NZ), ("x13", NZ, 32), ("x11", NZ, 32),
    ("x12a", NZ, 16), ("x12b", NZ + 16, 16), ("z12a", 0, 32), ("z12b", 32, 48),
)
TREE_ID = {name: i for i, (name, _, _) in enumerate(TREE)}
NT = len(TREE)


def body_kernel(bands_all, w_hbm, p_hbm, occ_ref, species_ref, lin_hbm, bias_ref, lout_ref, out_ref,
                w, tab, part, part16, ry, zs, zr, cfull, lin, dsend, dpart, drecv, xs, xall, appt, app, bd,
                lsem, tss, tsr, d2s, d2r, rys, ryr, zss, zsr, ags, agr, dens_s, dens_r, xss, xsr):
    band = lax.axis_index("band")
    ga = lax.axis_index("ga")
    zh, x, c = band // 8, (band // 2) % 4, band % 2
    y, zl = ga // 2, ga % 2

    def at(dz=0, dx=0, dc=0, dy=0, dl=0):
        nzh, nx, nc = (zh + dz) % 2, (x + dx) % 4, (c + dc) % 2
        ny, nzl = (y + dy) % 4, (zl + dl) % 2
        return (nzh * 8 + nx * 2 + nc, ny * 2 + nzl)

    def slot_row(dz, dx, dc):
        nzh, nx, nc = (zh + dz) % 2, (x + dx) % 4, (c + dc) % 2
        return (nzh * 8 + nx * 2 + nc) * SLOT

    def pair_row(dz, dx):
        return (((zh + dz) % 2) * 4 + (x + dx) % 4) * PAIR

    def rows(ref, start, count):
        return ref.at[pl.ds(pl.multiple_of(start, 16), count)]

    wcopy = pltpu.make_async_copy(w_hbm, w, lsem.at[0])
    own_row = slot_row(0, 0, 0)
    pcopy = pltpu.make_async_copy(p_hbm, rows(tab, own_row, SLOT), lsem.at[1])
    lcopy = pltpu.make_async_copy(lin_hbm, lin, lsem.at[2])
    pcopy.start()
    wcopy.start()
    lcopy.start()

    barrier = pltpu.get_barrier_semaphore()
    partners = [at(dc=1)]
    for dz in range(2):
        for dx in range(4):
            if dz or dx:
                partners.append(at(dz=dz, dx=dx))
    for dy in range(4):
        for dl in range(2):
            if dy or dl:
                partners.append(at(dy=dy, dl=dl))
                partners.append(at(dy=dy, dl=dl, dc=1))
    for partner in partners:
        pl.semaphore_signal(barrier, inc=1, device_id=partner, device_id_type=MESH)
    pl.semaphore_wait(barrier, len(partners))
    pcopy.wait()

    sends = []

    def remote(src, dst, ss, rs, device):
        copy = pltpu.make_async_remote_copy(
            src_ref=src, dst_ref=dst, send_sem=ss, recv_sem=rs, device_id=device, device_id_type=MESH
        )
        copy.start()
        sends.append(copy)

    def arrived(dst, ss, rs):
        pltpu.make_async_remote_copy(
            src_ref=dst, dst_ref=dst, send_sem=ss, recv_sem=rs, device_id=at(dc=1), device_id_type=MESH
        ).wait_recv()

    def tree_send(name, dz, dx, device):
        i = TREE_ID[name]
        _, first, count = TREE[i]
        ref = rows(tab, slot_row(dz, dx, 0) + first, count)
        remote(ref, ref, tss.at[i], tsr.at[i], device)

    def tree_wait(name, dz, dx):
        i = TREE_ID[name]
        _, first, count = TREE[i]
        arrived(rows(tab, slot_row(dz, dx, 0) + first, count), tss.at[i], tsr.at[i])

    def across(i, dz, dx):
        ref = rows(tab, slot_row(dz, dx, 0), SLOT)
        remote(ref, ref, d2s.at[i], d2r.at[i], at(dc=1))

    def across_wait(i, dz, dx):
        arrived(rows(tab, slot_row(dz, dx, 1), SLOT), d2s.at[i], d2r.at[i])

    right, left, over = at(dx=1), at(dx=3), at(dz=1)

    def project(i):
        dz, dx = ORDER[i]
        base = pl.multiple_of(pair_row(dz, dx), 16)

        def half(t, carry):
            wt = w[pl.ds(pl.multiple_of(t * 256, 256), 256), :]
            got = lax.dot_general(
                tab[pl.ds(base, PAIR), :], wt, (((1,), (1,)), ((), ())), preferred_element_type=F32
            )
            cols = pl.ds(pl.multiple_of(t * 256, 256), 256)
            part[i, :, cols] = got
            part16[i, :, cols] = got.astype(BF16)
            return carry

        lax.fori_loop(0, 2, half, 0)
        for dy in range(1, 4):
            piece = pl.ds(pl.multiple_of(((y + dy) % 4) * 128, 128), 128)
            remote(part16.at[i, :, piece], ry.at[i, 3 - dy], rys.at[i, 3 - dy], ryr.at[i, 3 - dy], at(dy=dy))

    mine = pl.ds(pl.multiple_of(y * 128, 128), 128)

    def reduce_y(i):
        total = part[i, :, mine]
        for j in range(3):
            arrived(ry.at[i, j], rys.at[i, j], ryr.at[i, j])
        for j in range(3):
            total = total + ry[i, j].astype(F32)
        zs[i] = total.astype(BF16)
        remote(zs.at[i], zr.at[i], zss.at[i], zsr.at[i], at(dl=1))

    def reduce_z(i):
        dz, dx = ORDER[i]
        pair = pl.ds(pl.multiple_of(pair_row(dz, dx), 16), PAIR)
        arrived(zr.at[i], zss.at[i], zsr.at[i])
        cfull[pair, mine] = (zs[i].astype(F32) + zr[i].astype(F32)).astype(BF16)
        for dy in range(1, 4):
            ref = cfull.at[pair, mine]
            remote(ref, ref, ags.at[i, 3 - dy], agr.at[i, 3 - dy], at(dy=dy))

    def gathered(i):
        dz, dx = ORDER[i]
        pair = pl.ds(pl.multiple_of(pair_row(dz, dx), 16), PAIR)
        for dy in range(1, 4):
            piece = pl.ds(pl.multiple_of(((y + dy) % 4) * 128, 128), 128)
            arrived(cfull.at[pair, piece], ags.at[i, dy - 1], agr.at[i, dy - 1])

    tree_send("z10", 0, 0, over)
    tree_send("x03", 0, 0, right)
    tree_send("x01", 0, 0, left)
    across(0, 0, 0)
    tree_send("z03", 0, 0, right)
    tree_send("z01", 0, 0, left)
    tree_send("x10", 0, 0, over)

    wcopy.wait()
    across_wait(0, 0, 0)
    project(0)
    tree_wait("x03", 0, 3)
    tree_send("x02a", 0, 3, right)
    tree_send("x13", 0, 3, over)
    tree_wait("x01", 0, 1)
    tree_send("x02b", 0, 1, left)
    tree_send("x11", 0, 1, over)
    reduce_y(0)
    reduce_z(0)

    tree_wait("z10", 1, 0)
    tree_send("z13", 1, 0, right)
    tree_send("z11", 1, 0, left)
    tree_wait("z03", 0, 3)
    tree_send("z02a", 0, 3, right)
    across(1, 0, 3)
    tree_wait("z01", 0, 1)
    tree_send("z02b", 0, 1, left)
    across(2, 0, 1)
    tree_wait("x10", 1, 0)
    across(3, 1, 0)
    across_wait(1, 0, 3)
    project(1)
    tree_wait("x02a", 0, 2)
    tree_send("x12a", 0, 2, over)
    tree_wait("x02b", 0, 2)
    tree_send("x12b", 0, 2, over)
    across_wait(2, 0, 1)
    project(2)
    reduce_y(1)
    across_wait(3, 1, 0)
    project(3)
    reduce_z(1)
    reduce_y(2)
    reduce_y(3)
    reduce_z(2)
    reduce_z(3)

    tree_wait("z13", 1, 3)
    tree_send("z12a", 1, 3, right)
    tree_wait("z11", 1, 1)
    tree_send("z12b", 1, 1, left)
    tree_wait("x13", 1, 3)
    across(4, 1, 3)
    tree_wait("x11", 1, 1)
    across(5, 1, 1)
    across_wait(4, 1, 3)
    project(4)
    across_wait(5, 1, 1)
    project(5)
    reduce_y(4)
    reduce_y(5)

    tree_wait("z02a", 0, 2)
    tree_wait("z02b", 0, 2)
    across(6, 0, 2)
    reduce_z(4)
    reduce_z(5)
    across_wait(6, 0, 2)
    project(6)
    reduce_y(6)
    for name in ("x12a", "x12b", "z12a", "z12b"):
        tree_wait(name, 1, 2)
    across(7, 1, 2)
    reduce_z(6)
    across_wait(7, 1, 2)
    project(7)
    for i in range(7):
        gathered(i)
    reduce_y(7)
    reduce_z(7)
    gathered(7)

    lane_atom = lax.broadcasted_iota(jnp.int32, (KP, SLOT), 1) // KP
    occ = occ_ref[...]
    for h in range(2):
        coef = cfull[pl.ds(pl.multiple_of(ga * PAIR + h * SLOT, 16), SLOT), :]
        weighted = coef.astype(F32) * occ
        high = weighted.astype(BF16)
        low = (weighted - high.astype(F32)).astype(BF16)
        dims = (((1,), (1,)), ((), ()))
        gram = lax.dot_general(high, coef, dims, preferred_element_type=F32) + lax.dot_general(
            low, coef, dims, preferred_element_type=F32
        )
        bd[...] = gram
        packed = jnp.zeros((KP, SLOT), F32)
        for a in range(4):
            packed = packed + jnp.where(lane_atom == a, bd[a * KP:(a + 1) * KP, :], 0.0)
        dsend[h, 0:KP, 0:SLOT] = packed
    remote(dsend.at[1 - c], drecv.at[7], dens_s.at[7], dens_r.at[7], at(dc=1))
    arrived(drecv.at[7], dens_s.at[7], dens_r.at[7])
    dpart[...] = dsend[c] + drecv[7]
    for dz in range(2):
        for dx in range(4):
            if dz or dx:
                j = dz * 4 + (4 - dx) % 4 - 1
                remote(dpart, drecv.at[j], dens_s.at[j], dens_r.at[j], at(dz=dz, dx=dx))
    lcopy.wait()
    for j in range(7):
        arrived(drecv.at[j], dens_s.at[j], dens_r.at[j])
    density = dpart[...]
    for j in range(7):
        density = density + drecv[j]
    density = density * (1.0 / bands_all)

    lane = lax.broadcasted_iota(jnp.int32, (K, SLOT), 1)
    grad_t = jnp.zeros((K, SLOT), F32)
    slot = 2 * ga + c
    for a in range(4):
        kind = species_ref[4 * slot + a]
        acc = jnp.zeros((K, HID), F32)
        for k in range(K):
            acc = acc + density[0:K, a * KP + k:a * KP + k + 1] * lin[kind, k * K:(k + 1) * K, :]
        preact = jnp.sum(acc, axis=0, keepdims=True) + bias_ref[kind]
        act = jnp.tanh(preact)
        slope = lout_ref[kind] * (1.0 - act * act)
        for k in range(K):
            column = jnp.sum(lin[kind, k * K:(k + 1) * K, :] * slope, axis=1, keepdims=True)
            grad_t = jnp.where(lane == a * KP + k, column, grad_t)
    bd[...] = jnp.zeros((SLOT, SLOT), F32)
    lane_atom_k = lane // KP
    for a in range(4):
        bd[a * KP:a * KP + K, :] = jnp.where(lane_atom_k == a, grad_t, 0.0)
    both = bd[...] + bd[...].T
    bd[...] = both
    packed = jnp.zeros((KP, SLOT), F32)
    for a in range(4):
        packed = packed + bd[a * KP:(a + 1) * KP, :]
    xs[0:KP, 0:SLOT] = packed
    xall[slot] = xs[...]
    for dy in range(4):
        for dl in range(2):
            for dc in range(2):
                if dy or dl or dc:
                    j = (((4 - dy) % 4) * 2 + dl) * 2 + dc
                    remote(xs, xall.at[slot], xss.at[j], xsr.at[j], at(dy=dy, dl=dl, dc=dc))
    for dy in range(4):
        for dl in range(2):
            for dc in range(2):
                if dy or dl or dc:
                    j = (dy * 2 + dl) * 2 + dc
                    from_slot = 2 * (((y + dy) % 4) * 2 + (zl + dl) % 2) + (c + dc) % 2
                    arrived(xall.at[from_slot], xss.at[j], xsr.at[j])

    factor = 1.0 / math.sqrt(64 * K)
    rows4 = lax.broadcasted_iota(jnp.int32, (SLOT, SLOT), 0) // KP
    lanes4 = lax.broadcasted_iota(jnp.int32, (SLOT, SLOT), 1) // KP
    same = rows4 == lanes4

    def apply(j, carry):
        packed = xall[j, 0:KP, 0:SLOT]
        for a in range(4):
            bd[a * KP:(a + 1) * KP, :] = packed
        full = jnp.where(same, bd[...], 0.0)
        high = full.astype(BF16)
        low = (full - high.astype(F32)).astype(BF16)
        at_rows = pl.ds(pl.multiple_of(j * SLOT, 16), SLOT)
        coef = cfull[at_rows, :]
        got = jnp.dot(high, coef, preferred_element_type=F32) + jnp.dot(low, coef, preferred_element_type=F32)
        appt[at_rows, :] = (got * factor).astype(BF16)
        return carry

    lax.fori_loop(0, 16, apply, 0)

    def turn(j, carry):
        block = pl.ds(pl.multiple_of(j * 256, 256), 256)
        app[:, block] = appt[block, :].T
        return carry

    lax.fori_loop(0, 7, turn, 0)

    def correct(t, carry):
        cols = pl.ds(pl.multiple_of(t * 512, 512), 512)
        out_ref[:, cols] = jnp.dot(app[...], tab[:, cols], preferred_element_type=F32).astype(BF16)
        return carry

    lax.fori_loop(0, 8, correct, 0)
    for copy in sends:
        copy.wait_send()


def body(wave_coef, projector, occupation, species, layer_in, bias_in, layer_out):
    atoms_here, orbitals, gs = projector.shape
    bands = wave_coef.shape[0]
    bands_all = bands * lax.axis_size("band")
    assert atoms_here == 4 and orbitals == K and bands == 512
    packed = jnp.pad(projector, ((0, 0), (0, KP - K), (0, 0))).reshape(SLOT, gs)
    any_space = pl.BlockSpec(memory_space=pl.ANY)
    vmem = pl.BlockSpec(memory_space=pltpu.VMEM)
    smem = pl.BlockSpec(memory_space=pltpu.SMEM)
    dma = pltpu.SemaphoreType.DMA
    return pl.pallas_call(
        functools.partial(body_kernel, bands_all),
        out_shape=jax.ShapeDtypeStruct((bands, gs), BF16),
        in_specs=[any_space, any_space, vmem, smem, any_space, vmem, vmem],
        out_specs=vmem,
        scratch_shapes=[
            pltpu.VMEM((bands, gs), BF16),
            pltpu.VMEM((16 * SLOT, gs), BF16),
            pltpu.VMEM((8, PAIR, bands), F32),
            pltpu.VMEM((8, PAIR, bands), BF16),
            pltpu.VMEM((8, 3, PAIR, 128), BF16),
            pltpu.VMEM((8, PAIR, 128), BF16),
            pltpu.VMEM((8, PAIR, 128), BF16),
            pltpu.VMEM((16 * SLOT, bands), BF16),
            pltpu.VMEM(layer_in.shape, F32),
            pltpu.VMEM((2, 32, 128), F32),
            pltpu.VMEM((32, 128), F32),
            pltpu.VMEM((8, 32, 128), F32),
            pltpu.VMEM((32, 128), F32),
            pltpu.VMEM((16, 32, 128), F32),
            pltpu.VMEM((16 * SLOT, bands), BF16),
            pltpu.VMEM((bands, 16 * SLOT), BF16),
            pltpu.VMEM((SLOT, SLOT), F32),
            dma((3,)), dma((NT,)), dma((NT,)), dma((8,)), dma((8,)),
            dma((8, 3)), dma((8, 3)), dma((8,)), dma((8,)), dma((8, 3)), dma((8, 3)),
            dma((8,)), dma((8,)), dma((16,)), dma((16,)),
        ],
        compiler_params=pltpu.CompilerParams(
            collective_id=0, has_side_effects=True, vmem_limit_bytes=62 * 2**20
        ),
        name="step",
    )(wave_coef, packed, occupation.reshape(1, bands), species, layer_in,
      bias_in.reshape(-1, 1, HID), layer_out.reshape(-1, 1, HID))


def solution(mesh):
    in_specs = (P("band", "ga"), P("band", None, "ga"), P("band"), P(), P(), P(), P())
    out_specs = P("band", "ga")
    return jax.shard_map(body, mesh=mesh, in_specs=in_specs, out_specs=out_specs, check_vma=False)
```

```python
import functools
import math

import jax
import jax.numpy as jnp
from jax import lax
from jax.experimental import pallas as pl
from jax.experimental.pallas import tpu as pltpu
from jax.sharding import PartitionSpec as P

MESH = pl.DeviceIdType.MESH
F32 = jnp.float32
BF16 = jnp.bfloat16

K = 27
KP = 28
SLOT = 4 * KP
PAIR = 2 * SLOT
HID = 100
SPECIES = 4

ORDER = ((0, 0), (0, 3), (0, 1), (1, 0), (1, 3), (1, 1), (0, 2), (1, 2))

PIECES = tuple((i, 0, PAIR) for i in range(7)) + ((7, 0, 80), (7, 144, 80), (7, 80, 64))

TREE = (
    ("z10", 32, 80), ("x10", 0, 32),
    ("z03", 32, 80), ("x03", 0, 32), ("z01", 32, 80), ("x01", 0, 32),
    ("x02a", 0, 16), ("x02b", 16, 16), ("z02a", 32, 48), ("z02b", 80, 32),
    ("z13", 32, 80), ("z11", 32, 80), ("x13", 0, 32), ("x11", 0, 32),
    ("x12a", 0, 16), ("x12b", 16, 16), ("z12a", 64, 16), ("z12b", 32, 32),
    ("z12c", 80, 16), ("z12d", 96, 16),
)
TREE_ID = {name: i for i, (name, _, _) in enumerate(TREE)}
NT = len(TREE)


def body_kernel(bands_all, w_hbm, p_hbm, occ_ref, species_ref, lin_hbm, bias_ref, lout_ref, app_out,
                tab_out, w, tab, pin, lraw, part, part16, ry, zs, zr, cfull, lin, dsend, dpart, drecv, xs, xall, appt, app, bd, bds,
                lsem, tabs, apps, tss, tsr, d2s, d2r, rys, ryr, zss, zsr, ags, agr, dens_s, dens_r, xss, xsr):
    band = lax.axis_index("band")
    ga = lax.axis_index("ga")
    zh, x, c = band // 8, (band // 2) % 4, band % 2
    y, zl = ga // 2, ga % 2

    def at(dz=0, dx=0, dc=0, dy=0, dl=0):
        nzh, nx, nc = (zh + dz) % 2, (x + dx) % 4, (c + dc) % 2
        ny, nzl = (y + dy) % 4, (zl + dl) % 2
        return (nzh * 8 + nx * 2 + nc, ny * 2 + nzl)

    def slot_row(dz, dx, dc):
        nzh, nx, nc = (zh + dz) % 2, (x + dx) % 4, (c + dc) % 2
        return (nzh * 8 + nx * 2 + nc) * SLOT

    def pair_row(dz, dx):
        return (((zh + dz) % 2) * 4 + (x + dx) % 4) * PAIR

    def row_in_slot(first, count, dc=0):
        return jnp.where((c + dc) % 2 == 0, first, SLOT - first - count)

    def rows(ref, start, count):
        return ref.at[pl.ds(pl.multiple_of(start, 16), count)]

    wcopy = pltpu.make_async_copy(w_hbm, w, lsem.at[0])
    own_row = slot_row(0, 0, 0)
    pcopy = pltpu.make_async_copy(p_hbm, pin, lsem.at[1])
    lcopy = pltpu.make_async_copy(lin_hbm, lraw, lsem.at[2])
    pcopy.start()
    wcopy.start()
    lcopy.start()

    barrier = pltpu.get_barrier_semaphore()
    partners = [at(dc=1)]
    for dz in range(2):
        for dx in range(4):
            if dz or dx:
                partners.append(at(dz=dz, dx=dx))
    for dy in range(4):
        for dl in range(2):
            if dy or dl:
                partners.append(at(dy=dy, dl=dl))
                partners.append(at(dy=dy, dl=dl, dc=1))
    for partner in partners:
        pl.semaphore_signal(barrier, inc=1, device_id=partner, device_id_type=MESH)
    pcopy.wait()

    def pack(t, carry):
        cols = pl.ds(pl.multiple_of(t * 512, 512), 512)
        flat = pin[:, :, cols].astype(F32).reshape(4 * K, 512)
        full = jnp.concatenate([flat, jnp.zeros((SLOT - 4 * K, 512), F32)], axis=0)
        tab[pl.ds(pl.multiple_of(own_row, 16), SLOT), cols] = full.astype(BF16)
        return carry

    lax.fori_loop(0, 8, pack, 0)
    pl.semaphore_wait(barrier, len(partners))

    sends = []

    def remote(src, dst, ss, rs, device):
        copy = pltpu.make_async_remote_copy(
            src_ref=src, dst_ref=dst, send_sem=ss, recv_sem=rs, device_id=device, device_id_type=MESH
        )
        copy.start()
        sends.append(copy)

    def arrived(dst, ss, rs):
        pltpu.make_async_remote_copy(
            src_ref=dst, dst_ref=dst, send_sem=ss, recv_sem=rs, device_id=at(dc=1), device_id_type=MESH
        ).wait_recv()

    def tree_send(name, dz, dx, device):
        i = TREE_ID[name]
        _, first, count = TREE[i]
        ref = rows(tab, slot_row(dz, dx, 0) + row_in_slot(first, count), count)
        remote(ref, ref, tss.at[i], tsr.at[i], device)

    def tree_wait(name, dz, dx):
        i = TREE_ID[name]
        _, first, count = TREE[i]
        arrived(rows(tab, slot_row(dz, dx, 0) + row_in_slot(first, count), count), tss.at[i], tsr.at[i])

    def across(i, dz, dx, first=0, count=SLOT):
        ref = rows(tab, slot_row(dz, dx, 0) + row_in_slot(first, count), count)
        remote(ref, ref, d2s.at[i], d2r.at[i], at(dc=1))

    def across_wait(i, dz, dx, first=0, count=SLOT):
        arrived(rows(tab, slot_row(dz, dx, 1) + row_in_slot(first, count, 1), count), d2s.at[i], d2r.at[i])

    flushes = []

    def flush(i):
        ref = rows(tab, pair_row(*ORDER[i]), PAIR)
        copy = pltpu.make_async_copy(ref, rows(tab_out, pair_row(*ORDER[i]), PAIR), tabs.at[i])
        copy.start()
        flushes.append(copy)

    right, left, over = at(dx=1), at(dx=3), at(dz=1)

    def project(*pieces):
        i = PIECES[pieces[0]][0]
        base = pair_row(*ORDER[i])

        def half(t, carry):
            cols = pl.ds(pl.multiple_of(t * 256, 256), 256)
            table = [tab[pl.ds(pl.multiple_of(base + PIECES[s][1], 16), PIECES[s][2]), :] for s in pieces]
            table = table[0] if len(pieces) == 1 else jnp.concatenate(table, axis=0)
            got = lax.dot_general(table, w[cols, :], (((1,), (1,)), ((), ())), preferred_element_type=F32)
            done = 0
            for s in pieces:
                _, first, count = PIECES[s]
                part[i, first:first + count, cols] = got[done:done + count]
                part16[i, first:first + count, cols] = got[done:done + count].astype(BF16)
                done += count
            return carry

        lax.fori_loop(0, 2, half, 0)
        for s in pieces:
            here = pl.ds(PIECES[s][1], PIECES[s][2])
            for dy in (2, 1, 3):
                lanes = pl.ds(pl.multiple_of(((y + dy) % 4) * 128, 128), 128)
                remote(part16.at[i, here, lanes], ry.at[i, 3 - dy, here], rys.at[s, 3 - dy], ryr.at[s, 3 - dy], at(dy=dy))

    mine = pl.ds(pl.multiple_of(y * 128, 128), 128)

    def reduce_y(s):
        i, first, count = PIECES[s]
        here = pl.ds(first, count)
        for j in range(3):
            arrived(ry.at[i, j, here], rys.at[s, j], ryr.at[s, j])
        total = part[i, here, mine]
        for j in range(3):
            total = total + ry[i, j, here].astype(F32)
        part[i, here, mine] = total
        zs[i, here] = total.astype(BF16)
        remote(zs.at[i, here], zr.at[i, here], zss.at[s], zsr.at[s], at(dl=1))

    def in_full(s):
        i, first, count = PIECES[s]
        return pl.ds(pl.multiple_of(pair_row(*ORDER[i]) + first, 16), count)

    def reduce_z(s):
        i, first, count = PIECES[s]
        here = pl.ds(first, count)
        arrived(zr.at[i, here], zss.at[s], zsr.at[s])
        cfull[in_full(s), mine] = (part[i, here, mine] + zr[i, here].astype(F32)).astype(BF16)
        for dy in (2, 1, 3):
            ref = cfull.at[in_full(s), mine]
            remote(ref, ref, ags.at[s, 3 - dy], agr.at[s, 3 - dy], at(dy=dy))

    def gathered(s):
        for dy in range(1, 4):
            lanes = pl.ds(pl.multiple_of(((y + dy) % 4) * 128, 128), 128)
            arrived(cfull.at[in_full(s), lanes], ags.at[s, dy - 1], agr.at[s, dy - 1])

    tree_send("z10", 0, 0, over)
    tree_send("x03", 0, 0, right)
    tree_send("x01", 0, 0, left)
    across(0, 0, 0)
    tree_send("z03", 0, 0, right)
    tree_send("z01", 0, 0, left)
    tree_send("x10", 0, 0, over)

    wcopy.wait()
    across_wait(0, 0, 0)
    project(0)
    flush(0)
    tree_wait("x03", 0, 3)
    tree_send("x02a", 0, 3, right)
    tree_send("x13", 0, 3, over)
    tree_wait("x01", 0, 1)
    tree_send("x02b", 0, 1, left)
    tree_send("x11", 0, 1, over)
    reduce_y(0)

    lcopy.wait()
    for kind in range(SPECIES):
        lin[kind] = lraw[:, kind, :].T

    tree_wait("z10", 1, 0)
    tree_send("z13", 1, 0, right)
    tree_send("z11", 1, 0, left)
    tree_wait("z03", 0, 3)
    tree_send("z02a", 0, 3, right)
    across(1, 0, 3)
    tree_wait("z01", 0, 1)
    tree_send("z02b", 0, 1, left)
    across(2, 0, 1)
    tree_wait("x10", 1, 0)
    across(3, 1, 0)
    tree_wait("x02a", 0, 2)
    tree_send("x12a", 0, 2, over)
    tree_wait("x02b", 0, 2)
    tree_send("x12b", 0, 2, over)
    across_wait(1, 0, 3)
    project(1)
    across_wait(2, 0, 1)
    project(2)
    across_wait(3, 1, 0)
    project(3)
    for i in (1, 2, 3):
        flush(i)
    reduce_z(0)
    reduce_y(1)
    reduce_y(2)
    reduce_y(3)

    tree_wait("z13", 1, 3)
    tree_send("z12a", 1, 3, right)
    tree_send("z12c", 1, 3, right)
    tree_wait("z11", 1, 1)
    tree_send("z12b", 1, 1, left)
    tree_send("z12d", 1, 1, left)
    tree_wait("x13", 1, 3)
    across(4, 1, 3)
    tree_wait("x11", 1, 1)
    across(5, 1, 1)
    reduce_z(1)
    across_wait(4, 1, 3)
    project(4)
    across_wait(5, 1, 1)
    project(5)
    flush(4)
    flush(5)
    reduce_z(2)
    reduce_z(3)
    reduce_y(4)

    tree_wait("z02a", 0, 2)
    tree_wait("z02b", 0, 2)
    across(6, 0, 2)
    reduce_y(5)
    across_wait(6, 0, 2)
    project(6)
    flush(6)
    reduce_z(4)
    reduce_z(5)
    tree_wait("x12a", 1, 2)
    tree_wait("x12b", 1, 2)
    tree_wait("z12a", 1, 2)
    tree_wait("z12b", 1, 2)
    across(7, 1, 2, 0, 80)
    across_wait(7, 1, 2, 0, 80)
    project(7, 8)
    tree_wait("z12c", 1, 2)
    tree_wait("z12d", 1, 2)
    across(8, 1, 2, 80, 32)
    across_wait(8, 1, 2, 80, 32)
    project(9)
    flush(7)
    reduce_y(6)
    reduce_y(7)
    reduce_y(8)
    reduce_y(9)
    reduce_z(6)
    reduce_z(7)
    reduce_z(8)
    reduce_z(9)
    for s in range(10):
        gathered(s)

    lane_atom = lax.broadcasted_iota(jnp.int32, (KP, SLOT), 1) % 4
    occ = occ_ref[...]
    for h in range(2):
        coef = cfull[pl.ds(pl.multiple_of(ga * PAIR + h * SLOT, 16), SLOT), :]
        weighted = coef.astype(F32) * occ
        high = weighted.astype(BF16)
        low = (weighted - high.astype(F32)).astype(BF16)
        dims = (((1,), (1,)), ((), ()))
        gram = lax.dot_general(high, coef, dims, preferred_element_type=F32) + lax.dot_general(
            low, coef, dims, preferred_element_type=F32
        )
        bd[:, 0:SLOT] = gram
        packed = jnp.zeros((KP, SLOT), F32)
        for a in range(4):
            packed = packed + jnp.where(lane_atom == a, bd[pl.ds(a, KP, stride=4), :][:, 0:SLOT], 0.0)
        dsend[h, 0:KP, 0:SLOT] = packed
    remote(dsend.at[1 - c], drecv.at[7], dens_s.at[7], dens_r.at[7], at(dc=1))
    arrived(drecv.at[7], dens_s.at[7], dens_r.at[7])
    dpart[...] = dsend[c] + drecv[7]
    for dz in range(2):
        for dx in range(4):
            if dz or dx:
                j = dz * 4 + (4 - dx) % 4 - 1
                remote(dpart, drecv.at[j], dens_s.at[j], dens_r.at[j], at(dz=dz, dx=dx))
    for j in range(7):
        arrived(drecv.at[j], dens_s.at[j], dens_r.at[j])
    density = dpart[...]
    for j in range(7):
        density = density + drecv[j]
    density = density * (1.0 / bands_all)

    lane = lax.broadcasted_iota(jnp.int32, (K, SLOT), 1)
    grad_t = jnp.zeros((K, SLOT), F32)
    slot = 2 * ga + c
    for a in range(4):
        kind = species_ref[4 * slot + a]
        acc = jnp.zeros((K, HID), F32)
        for k in range(K):
            acc = acc + density[0:K, 4 * k + a:4 * k + a + 1] * lin[kind, k * K:(k + 1) * K, :]
        preact = jnp.sum(acc, axis=0, keepdims=True) + bias_ref[kind]
        act = jnp.tanh(preact)
        slope = lout_ref[kind] * (1.0 - act * act)
        for k in range(K):
            column = jnp.sum(lin[kind, k * K:(k + 1) * K, :] * slope, axis=1, keepdims=True)
            grad_t = jnp.where(lane == 4 * k + a, column, grad_t)
    bd[...] = jnp.zeros((SLOT, 128), F32)
    pad = jnp.zeros((K, 128 - SLOT), F32)
    for a in range(4):
        bd[pl.ds(a, K, stride=4), :] = jnp.concatenate([jnp.where(lane % 4 == a, grad_t, 0.0), pad], axis=1)
    square = bd[:, 0:SLOT]
    bd[:, 0:SLOT] = square + square.T
    packed = jnp.zeros((KP, 128), F32)
    for a in range(4):
        packed = packed + bd[pl.ds(a, KP, stride=4), :]
    xs[0:KP, :] = packed
    xall[slot] = xs[...]
    for dy in range(4):
        for dl in range(2):
            for dc in range(2):
                if dy or dl or dc:
                    j = (((4 - dy) % 4) * 2 + dl) * 2 + dc
                    remote(xs, xall.at[slot], xss.at[j], xsr.at[j], at(dy=dy, dl=dl, dc=dc))
    for dy in range(4):
        for dl in range(2):
            for dc in range(2):
                if dy or dl or dc:
                    j = (dy * 2 + dl) * 2 + dc
                    from_slot = 2 * (((y + dy) % 4) * 2 + (zl + dl) % 2) + (c + dc) % 2
                    arrived(xall.at[from_slot], xss.at[j], xsr.at[j])

    factor = 1.0 / math.sqrt(64 * K)
    rows4 = lax.broadcasted_iota(jnp.int32, (SLOT, SLOT), 0) % 4
    lanes4 = lax.broadcasted_iota(jnp.int32, (SLOT, SLOT), 1) % 4
    same = rows4 == lanes4

    def apply(j, carry):
        for a in range(4):
            bds[j, pl.ds(a, KP, stride=4), :] = xall[j, 0:KP, :]
        full = jnp.where(same, bds[j, :, 0:SLOT], 0.0)
        high = full.astype(BF16)
        low = (full - high.astype(F32)).astype(BF16)
        at_rows = pl.ds(pl.multiple_of(j * SLOT, 16), SLOT)
        coef = cfull[at_rows, :]
        got = jnp.dot(high, coef, preferred_element_type=F32) + jnp.dot(low, coef, preferred_element_type=F32)
        appt[at_rows, :] = (got * factor).astype(BF16)
        return carry

    lax.fori_loop(0, 16, apply, 0, unroll=4)

    def turn(j, carry):
        block = pl.ds(pl.multiple_of(j * 256, 256), 256)
        app[:, block] = appt[block, :].T
        return carry

    lax.fori_loop(0, 7, turn, 0)
    last = pltpu.make_async_copy(app, app_out, apps)
    last.start()
    last.wait()
    for copy in flushes:
        copy.wait()
    for copy in sends:
        copy.wait_send()


def correct_kernel(app_ref, tab_ref, out_ref):
    out_ref[...] = jnp.dot(app_ref[...], tab_ref[...], preferred_element_type=F32).astype(BF16)


def body(wave_coef, projector, occupation, species, layer_in, bias_in, layer_out):
    atoms_here, orbitals, gs = projector.shape
    bands = wave_coef.shape[0]
    bands_all = bands * lax.axis_size("band")
    assert atoms_here == 4 and orbitals == K and bands == 512
    any_space = pl.BlockSpec(memory_space=pl.ANY)
    vmem = pl.BlockSpec(memory_space=pltpu.VMEM)
    smem = pl.BlockSpec(memory_space=pltpu.SMEM)
    dma = pltpu.SemaphoreType.DMA
    applied, table = pl.pallas_call(
        functools.partial(body_kernel, bands_all),
        out_shape=[jax.ShapeDtypeStruct((bands, 16 * SLOT), BF16), jax.ShapeDtypeStruct((16 * SLOT, gs), BF16)],
        in_specs=[any_space, any_space, vmem, smem, any_space, vmem, vmem],
        out_specs=[any_space, any_space],
        scratch_shapes=[
            pltpu.VMEM((bands, gs), BF16),
            pltpu.VMEM((16 * SLOT, gs), BF16),
            pltpu.VMEM((K, 4, gs), BF16),
            pltpu.VMEM((HID, SPECIES, K * K), F32),
            pltpu.VMEM((8, PAIR, bands), F32),
            pltpu.VMEM((8, PAIR, bands), BF16),
            pltpu.VMEM((8, 3, PAIR, 128), BF16),
            pltpu.VMEM((8, PAIR, 128), BF16),
            pltpu.VMEM((8, PAIR, 128), BF16),
            pltpu.VMEM((16 * SLOT, bands), BF16),
            pltpu.VMEM((SPECIES, K * K, HID), F32),
            pltpu.VMEM((2, 32, 128), F32),
            pltpu.VMEM((32, 128), F32),
            pltpu.VMEM((8, 32, 128), F32),
            pltpu.VMEM((32, 128), F32),
            pltpu.VMEM((16, 32, 128), F32),
            pltpu.VMEM((16 * SLOT, bands), BF16),
            pltpu.VMEM((bands, 16 * SLOT), BF16),
            pltpu.VMEM((SLOT, 128), F32),
            pltpu.VMEM((16, SLOT, 128), F32),
            dma((3,)), dma((8,)), dma, dma((NT,)), dma((NT,)), dma((9,)), dma((9,)),
            dma((10, 3)), dma((10, 3)), dma((10,)), dma((10,)), dma((10, 3)), dma((10, 3)),
            dma((8,)), dma((8,)), dma((16,)), dma((16,)),
        ],
        compiler_params=pltpu.CompilerParams(
            collective_id=0, has_side_effects=True, vmem_limit_bytes=62 * 2**20
        ),
        name="step",
    )(wave_coef, jnp.transpose(projector, (1, 0, 2)), occupation.reshape(1, bands), species,
      jnp.transpose(layer_in, (2, 0, 1)), bias_in.reshape(-1, 1, HID), layer_out.reshape(-1, 1, HID))
    step = 512
    return pl.pallas_call(
        correct_kernel,
        grid=(gs // step,),
        out_shape=jax.ShapeDtypeStruct((bands, gs), BF16),
        in_specs=[pl.BlockSpec((bands, 16 * SLOT), lambda t: (0, 0)), pl.BlockSpec((16 * SLOT, step), lambda t: (0, t))],
        out_specs=pl.BlockSpec((bands, step), lambda t: (0, t)),
        compiler_params=pltpu.CompilerParams(vmem_limit_bytes=40 * 2**20),
        name="correct",
    )(applied, table)


def solution(mesh):
    in_specs = (P("band", "ga"), P("band", None, "ga"), P("band"), P(), P(), P(), P())
    out_specs = P("band", "ga")
    return jax.shard_map(body, mesh=mesh, in_specs=in_specs, out_specs=out_specs, check_vma=False)
```

```python
import functools
import math

import jax
import jax.numpy as jnp
from jax import lax
from jax.experimental import pallas as pl
from jax.experimental.pallas import tpu as pltpu
from jax.sharding import PartitionSpec as P

MESH = pl.DeviceIdType.MESH
F32 = jnp.float32
BF16 = jnp.bfloat16

K = 27
KP = 28
SLOT = 4 * KP
PAIR = 2 * SLOT
HID = 100
SPECIES = 4

ORDER = ((0, 0), (0, 3), (0, 1), (1, 0), (1, 3), (1, 1), (0, 2), (1, 2))

SPLIT = (1, 2, 4, 5, 7)
PIECES = []
EARLY, LATE = {}, {}
for _i in range(8):
    if _i in SPLIT:
        EARLY[_i] = (len(PIECES), len(PIECES) + 1)
        LATE[_i] = (len(PIECES) + 2,)
        PIECES += [(_i, 0, 80), (_i, 144, 80), (_i, 80, 64)]
    else:
        EARLY[_i] = (len(PIECES),)
        PIECES += [(_i, 0, PAIR)]
NP = len(PIECES)

TREE = (
    ("z10", 32, 80), ("x10", 0, 32),
    ("z03a", 32, 48), ("z03b", 80, 32), ("x03", 0, 32), ("z01a", 32, 48), ("z01b", 80, 32), ("x01", 0, 32),
    ("x02a", 0, 16), ("x02b", 16, 16), ("z02a", 32, 48), ("z02b", 80, 32),
    ("z13a", 32, 48), ("z13b", 80, 32), ("z11a", 32, 48), ("z11b", 80, 32), ("x13", 0, 32), ("x11", 0, 32),
    ("x12a", 0, 16), ("x12b", 16, 16), ("z12a", 64, 16), ("z12b", 32, 32),
    ("z12c", 80, 16), ("z12d", 96, 16),
)
TREE_ID = {name: i for i, (name, _, _) in enumerate(TREE)}
NT = len(TREE)


def body_kernel(bands_all, w_hbm, p_hbm, occ_ref, species_ref, lin_hbm, bias_ref, lout_ref, app_out,
                tab_out, w, tab, pin, lraw, part, part16, ry, zs, zr, cfull, lin, dsend, dpart, drecv, xs, xall, appt, app, bd, bds,
                lsem, tabs, apps, tss, tsr, d2s, d2r, rys, ryr, zss, zsr, ags, agr, dens_s, dens_r, xss, xsr):
    band = lax.axis_index("band")
    ga = lax.axis_index("ga")
    zh, x, c = band // 8, (band // 2) % 4, band % 2
    y, zl = ga // 2, ga % 2

    def at(dz=0, dx=0, dc=0, dy=0, dl=0):
        nzh, nx, nc = (zh + dz) % 2, (x + dx) % 4, (c + dc) % 2
        ny, nzl = (y + dy) % 4, (zl + dl) % 2
        return (nzh * 8 + nx * 2 + nc, ny * 2 + nzl)

    def slot_row(dz, dx, dc):
        nzh, nx, nc = (zh + dz) % 2, (x + dx) % 4, (c + dc) % 2
        return (nzh * 8 + nx * 2 + nc) * SLOT

    def pair_row(dz, dx):
        return (((zh + dz) % 2) * 4 + (x + dx) % 4) * PAIR

    def row_in_slot(first, count, dc=0):
        return jnp.where((c + dc) % 2 == 0, first, SLOT - first - count)

    def rows(ref, start, count):
        return ref.at[pl.ds(pl.multiple_of(start, 16), count)]

    wcopy = pltpu.make_async_copy(w_hbm, w, lsem.at[0])
    own_row = slot_row(0, 0, 0)
    pcopy = pltpu.make_async_copy(p_hbm, pin, lsem.at[1])
    lcopy = pltpu.make_async_copy(lin_hbm, lraw, lsem.at[2])
    pcopy.start()
    wcopy.start()
    lcopy.start()

    barrier = pltpu.get_barrier_semaphore()
    partners = [at(dc=1)]
    for dz in range(2):
        for dx in range(4):
            if dz or dx:
                partners.append(at(dz=dz, dx=dx))
    for dy in range(4):
        for dl in range(2):
            if dy or dl:
                partners.append(at(dy=dy, dl=dl))
                partners.append(at(dy=dy, dl=dl, dc=1))
    for partner in partners:
        pl.semaphore_signal(barrier, inc=1, device_id=partner, device_id_type=MESH)
    pcopy.wait()

    def pack(t, carry):
        cols = pl.ds(pl.multiple_of(t * 512, 512), 512)
        flat = pin[:, :, cols].astype(F32).reshape(4 * K, 512)
        full = jnp.concatenate([flat, jnp.zeros((SLOT - 4 * K, 512), F32)], axis=0)
        tab[pl.ds(pl.multiple_of(own_row, 16), SLOT), cols] = full.astype(BF16)
        return carry

    lax.fori_loop(0, 8, pack, 0)
    pl.semaphore_wait(barrier, len(partners))

    sends = []

    def remote(src, dst, ss, rs, device):
        copy = pltpu.make_async_remote_copy(
            src_ref=src, dst_ref=dst, send_sem=ss, recv_sem=rs, device_id=device, device_id_type=MESH
        )
        copy.start()
        sends.append(copy)

    def arrived(dst, ss, rs):
        pltpu.make_async_remote_copy(
            src_ref=dst, dst_ref=dst, send_sem=ss, recv_sem=rs, device_id=at(dc=1), device_id_type=MESH
        ).wait_recv()

    def tree_send(name, dz, dx, device):
        i = TREE_ID[name]
        _, first, count = TREE[i]
        ref = rows(tab, slot_row(dz, dx, 0) + row_in_slot(first, count), count)
        remote(ref, ref, tss.at[i], tsr.at[i], device)

    def tree_wait(name, dz, dx):
        i = TREE_ID[name]
        _, first, count = TREE[i]
        arrived(rows(tab, slot_row(dz, dx, 0) + row_in_slot(first, count), count), tss.at[i], tsr.at[i])

    def crossing(i, part):
        first, count = ((0, SLOT), (0, 80), (80, 32))[part]
        return ORDER[i], first, count, i + 8 * (part == 2)

    def across(i, part=0):
        (dz, dx), first, count, sem = crossing(i, part)
        ref = rows(tab, slot_row(dz, dx, 0) + row_in_slot(first, count), count)
        remote(ref, ref, d2s.at[sem], d2r.at[sem], at(dc=1))

    def across_wait(i, part=0):
        (dz, dx), first, count, sem = crossing(i, part)
        arrived(rows(tab, slot_row(dz, dx, 1) + row_in_slot(first, count, 1), count), d2s.at[sem], d2r.at[sem])

    flushes = []

    def flush(i):
        ref = rows(tab, pair_row(*ORDER[i]), PAIR)
        copy = pltpu.make_async_copy(ref, rows(tab_out, pair_row(*ORDER[i]), PAIR), tabs.at[i])
        copy.start()
        flushes.append(copy)

    right, left, over = at(dx=1), at(dx=3), at(dz=1)

    def project(pieces):
        i = PIECES[pieces[0]][0]
        base = pair_row(*ORDER[i])

        def half(t, carry):
            cols = pl.ds(pl.multiple_of(t * 256, 256), 256)
            table = [tab[pl.ds(pl.multiple_of(base + PIECES[s][1], 16), PIECES[s][2]), :] for s in pieces]
            table = table[0] if len(pieces) == 1 else jnp.concatenate(table, axis=0)
            got = lax.dot_general(table, w[cols, :], (((1,), (1,)), ((), ())), preferred_element_type=F32)
            done = 0
            for s in pieces:
                _, first, count = PIECES[s]
                part[i, first:first + count, cols] = got[done:done + count]
                part16[i, first:first + count, cols] = got[done:done + count].astype(BF16)
                done += count
            return carry

        lax.fori_loop(0, 2, half, 0)
        for s in pieces:
            here = pl.ds(PIECES[s][1], PIECES[s][2])
            for dy in (2, 1, 3):
                lanes = pl.ds(pl.multiple_of(((y + dy) % 4) * 128, 128), 128)
                remote(part16.at[i, here, lanes], ry.at[i, 3 - dy, here], rys.at[s, 3 - dy], ryr.at[s, 3 - dy], at(dy=dy))

    mine = pl.ds(pl.multiple_of(y * 128, 128), 128)

    def reduce_y(s):
        i, first, count = PIECES[s]
        here = pl.ds(first, count)
        for j in range(3):
            arrived(ry.at[i, j, here], rys.at[s, j], ryr.at[s, j])
        total = part[i, here, mine]
        for j in range(3):
            total = total + ry[i, j, here].astype(F32)
        part[i, here, mine] = total
        zs[i, here] = total.astype(BF16)
        remote(zs.at[i, here], zr.at[i, here], zss.at[s], zsr.at[s], at(dl=1))

    def in_full(s):
        i, first, count = PIECES[s]
        return pl.ds(pl.multiple_of(pair_row(*ORDER[i]) + first, 16), count)

    def direct(s):
        return PIECES[s][0] == 7

    def block(s, dy):
        lanes = pl.ds(pl.multiple_of(((y + dy) % 4) * 128, 128), 128)
        return cfull.at[in_full(s), lanes]

    def reduce_z(s):
        i, first, count = PIECES[s]
        here = pl.ds(first, count)
        arrived(zr.at[i, here], zss.at[s], zsr.at[s])
        cfull[in_full(s), mine] = (part[i, here, mine] + zr[i, here].astype(F32)).astype(BF16)
        for dy in (2, 1, 3) if direct(s) else (1, 3):
            remote(block(s, 0), block(s, 0), ags.at[s, 3 - dy], agr.at[s, 3 - dy], at(dy=dy))

    def relay(s):
        for dy in (1, 3):
            arrived(block(s, dy), ags.at[s, dy - 1], agr.at[s, dy - 1])
        dy = 1 + 2 * (s % 2)
        remote(block(s, dy), block(s, dy), ags.at[s, 1], agr.at[s, 1], at(dy=4 - dy))

    def gathered(s):
        for dy in (1, 2, 3) if direct(s) else (2,):
            arrived(block(s, dy), ags.at[s, dy - 1], agr.at[s, dy - 1])

    tree_send("z10", 0, 0, over)
    tree_send("x03", 0, 0, right)
    tree_send("x01", 0, 0, left)
    across(0)
    tree_send("z03a", 0, 0, right)
    tree_send("z01a", 0, 0, left)
    tree_send("z03b", 0, 0, right)
    tree_send("z01b", 0, 0, left)
    wcopy.wait()
    across_wait(0)
    project(EARLY[0])
    flush(0)
    tree_wait("x03", 0, 3)
    tree_send("x02a", 0, 3, right)
    tree_wait("x01", 0, 1)
    tree_send("x02b", 0, 1, left)
    for s in EARLY[0]:
        reduce_y(s)
    tree_send("x10", 0, 0, over)
    tree_send("x13", 0, 3, over)
    tree_send("x11", 0, 1, over)
    lcopy.wait()
    for kind in range(SPECIES):
        lin[kind] = lraw[:, kind, :].T
    tree_wait("z03a", 0, 3)
    across(1, 1)
    tree_wait("z01a", 0, 1)
    across(2, 1)
    tree_wait("z10", 1, 0)
    tree_send("z13a", 1, 0, right)
    tree_send("z11a", 1, 0, left)
    tree_send("z13b", 1, 0, right)
    tree_send("z11b", 1, 0, left)
    tree_send("z02a", 0, 3, right)
    for s in EARLY[0]:
        reduce_z(s)
    across_wait(1, 1)
    project(EARLY[1])
    across_wait(2, 1)
    project(EARLY[2])
    tree_wait("z03b", 0, 3)
    across(1, 2)
    tree_wait("z01b", 0, 1)
    tree_send("z02b", 0, 1, left)
    across(2, 2)
    tree_wait("x10", 1, 0)
    across(3)
    across_wait(1, 2)
    project(LATE[1])
    for s in EARLY[0]:
        relay(s)
    for s in EARLY[1]:
        reduce_y(s)
    across_wait(2, 2)
    project(LATE[2])
    for s in EARLY[2]:
        reduce_y(s)
    across_wait(3)
    project(EARLY[3])
    flush(1)
    flush(2)
    flush(3)
    for s in LATE[1]:
        reduce_y(s)
    for s in LATE[2]:
        reduce_y(s)
    tree_wait("x02a", 0, 2)
    tree_wait("x02b", 0, 2)
    tree_send("x12a", 0, 2, over)
    tree_send("x12b", 0, 2, over)
    tree_wait("z13a", 1, 3)
    tree_send("z12a", 1, 3, right)
    tree_wait("z11a", 1, 1)
    tree_send("z12b", 1, 1, left)
    tree_wait("x13", 1, 3)
    across(4, 1)
    tree_wait("x11", 1, 1)
    across(5, 1)
    for s in EARLY[3]:
        reduce_y(s)
    across_wait(4, 1)
    project(EARLY[4])
    across_wait(5, 1)
    project(EARLY[5])
    for s in EARLY[1]:
        reduce_z(s)
    for s in EARLY[2]:
        reduce_z(s)
    tree_wait("z13b", 1, 3)
    tree_send("z12c", 1, 3, right)
    across(4, 2)
    tree_wait("z11b", 1, 1)
    tree_send("z12d", 1, 1, left)
    across(5, 2)
    for s in LATE[1]:
        reduce_z(s)
    for s in LATE[2]:
        reduce_z(s)
    across_wait(4, 2)
    project(LATE[4])
    for s in EARLY[4]:
        reduce_y(s)
    across_wait(5, 2)
    project(LATE[5])
    for s in EARLY[5]:
        reduce_y(s)
    for s in EARLY[3]:
        reduce_z(s)
    for s in EARLY[1]:
        relay(s)
    for s in EARLY[2]:
        relay(s)
    flush(4)
    flush(5)
    tree_wait("z02a", 0, 2)
    across(6, 1)
    tree_wait("z02b", 0, 2)
    across(6, 2)
    for s in LATE[4]:
        reduce_y(s)
    for s in LATE[5]:
        reduce_y(s)
    for s in LATE[1]:
        relay(s)
    for s in LATE[2]:
        relay(s)
    for s in EARLY[4]:
        reduce_z(s)
    across_wait(6, 1)
    across_wait(6, 2)
    project(EARLY[6])
    flush(6)
    for s in EARLY[5]:
        reduce_z(s)
    for s in EARLY[3]:
        relay(s)
    tree_wait("x12a", 1, 2)
    tree_wait("x12b", 1, 2)
    tree_wait("z12a", 1, 2)
    tree_wait("z12b", 1, 2)
    across(7, 1)
    for s in LATE[4]:
        reduce_z(s)
    for s in LATE[5]:
        reduce_z(s)
    across_wait(7, 1)
    project(EARLY[7])
    tree_wait("z12c", 1, 2)
    tree_wait("z12d", 1, 2)
    across(7, 2)
    for s in EARLY[6]:
        reduce_y(s)
    for s in EARLY[4]:
        relay(s)
    for s in EARLY[5]:
        relay(s)
    across_wait(7, 2)
    project(LATE[7])
    flush(7)
    for s in EARLY[7]:
        reduce_y(s)
    for s in LATE[4]:
        relay(s)
    for s in LATE[5]:
        relay(s)
    for s in LATE[7]:
        reduce_y(s)
    for s in EARLY[6]:
        reduce_z(s)
    for s in EARLY[7]:
        reduce_z(s)
    for s in LATE[7]:
        reduce_z(s)
    for s in EARLY[6]:
        relay(s)
    for s in range(NP):
        gathered(s)

    lane_atom = lax.broadcasted_iota(jnp.int32, (KP, SLOT), 1) % 4
    occ = occ_ref[...]
    for h in range(2):
        coef = cfull[pl.ds(pl.multiple_of(ga * PAIR + h * SLOT, 16), SLOT), :]
        weighted = coef.astype(F32) * occ
        high = weighted.astype(BF16)
        low = (weighted - high.astype(F32)).astype(BF16)
        dims = (((1,), (1,)), ((), ()))
        gram = lax.dot_general(high, coef, dims, preferred_element_type=F32) + lax.dot_general(
            low, coef, dims, preferred_element_type=F32
        )
        bd[:, 0:SLOT] = gram
        packed = jnp.zeros((KP, SLOT), F32)
        for a in range(4):
            packed = packed + jnp.where(lane_atom == a, bd[pl.ds(a, KP, stride=4), :][:, 0:SLOT], 0.0)
        dsend[h, 0:KP, 0:SLOT] = packed
    remote(dsend.at[1 - c], drecv.at[7], dens_s.at[7], dens_r.at[7], at(dc=1))
    arrived(drecv.at[7], dens_s.at[7], dens_r.at[7])
    dpart[...] = dsend[c] + drecv[7]
    for dz in range(2):
        for dx in range(4):
            if dz or dx:
                j = dz * 4 + (4 - dx) % 4 - 1
                remote(dpart, drecv.at[j], dens_s.at[j], dens_r.at[j], at(dz=dz, dx=dx))
    for j in range(7):
        arrived(drecv.at[j], dens_s.at[j], dens_r.at[j])
    density = dpart[...]
    for j in range(7):
        density = density + drecv[j]
    density = density * (1.0 / bands_all)

    lane = lax.broadcasted_iota(jnp.int32, (K, SLOT), 1)
    grad_t = jnp.zeros((K, SLOT), F32)
    slot = 2 * ga + c
    for a in range(4):
        kind = species_ref[4 * slot + a]
        acc = jnp.zeros((K, HID), F32)
        for k in range(K):
            acc = acc + density[0:K, 4 * k + a:4 * k + a + 1] * lin[kind, k * K:(k + 1) * K, :]
        preact = jnp.sum(acc, axis=0, keepdims=True) + bias_ref[kind]
        act = jnp.tanh(preact)
        slope = lout_ref[kind] * (1.0 - act * act)
        for k in range(K):
            column = jnp.sum(lin[kind, k * K:(k + 1) * K, :] * slope, axis=1, keepdims=True)
            grad_t = jnp.where(lane == 4 * k + a, column, grad_t)
    bd[...] = jnp.zeros((SLOT, 128), F32)
    pad = jnp.zeros((K, 128 - SLOT), F32)
    for a in range(4):
        bd[pl.ds(a, K, stride=4), :] = jnp.concatenate([jnp.where(lane % 4 == a, grad_t, 0.0), pad], axis=1)
    square = bd[:, 0:SLOT]
    bd[:, 0:SLOT] = square + square.T
    packed = jnp.zeros((KP, 128), F32)
    for a in range(4):
        packed = packed + bd[pl.ds(a, KP, stride=4), :]
    xs[0:KP, :] = packed
    xall[slot] = xs[...]
    for dy in range(4):
        for dl in range(2):
            for dc in range(2):
                if dy or dl or dc:
                    j = (((4 - dy) % 4) * 2 + dl) * 2 + dc
                    remote(xs, xall.at[slot], xss.at[j], xsr.at[j], at(dy=dy, dl=dl, dc=dc))
    for dy in range(4):
        for dl in range(2):
            for dc in range(2):
                if dy or dl or dc:
                    j = (dy * 2 + dl) * 2 + dc
                    from_slot = 2 * (((y + dy) % 4) * 2 + (zl + dl) % 2) + (c + dc) % 2
                    arrived(xall.at[from_slot], xss.at[j], xsr.at[j])

    factor = 1.0 / math.sqrt(64 * K)
    rows4 = lax.broadcasted_iota(jnp.int32, (SLOT, SLOT), 0) % 4
    lanes4 = lax.broadcasted_iota(jnp.int32, (SLOT, SLOT), 1) % 4
    same = rows4 == lanes4

    def apply(j, carry):
        for a in range(4):
            bds[j, pl.ds(a, KP, stride=4), :] = xall[j, 0:KP, :]
        full = jnp.where(same, bds[j, :, 0:SLOT], 0.0)
        high = full.astype(BF16)
        low = (full - high.astype(F32)).astype(BF16)
        at_rows = pl.ds(pl.multiple_of(j * SLOT, 16), SLOT)
        coef = cfull[at_rows, :]
        got = jnp.dot(high, coef, preferred_element_type=F32) + jnp.dot(low, coef, preferred_element_type=F32)
        appt[at_rows, :] = (got * factor).astype(BF16)
        return carry

    lax.fori_loop(0, 16, apply, 0, unroll=4)

    def turn(j, carry):
        block = pl.ds(pl.multiple_of(j * 256, 256), 256)
        app[:, block] = appt[block, :].T
        pltpu.make_async_copy(app.at[:, block], app_out.at[:, block], apps.at[j]).start()
        return carry

    lax.fori_loop(0, 7, turn, 0)
    for j in range(7):
        block = pl.ds(j * 256, 256)
        pltpu.make_async_copy(app.at[:, block], app_out.at[:, block], apps.at[j]).wait()
    for copy in flushes:
        copy.wait()
    for copy in sends:
        copy.wait_send()


def body(wave_coef, projector, occupation, species, layer_in, bias_in, layer_out):
    atoms_here, orbitals, gs = projector.shape
    bands = wave_coef.shape[0]
    bands_all = bands * lax.axis_size("band")
    assert atoms_here == 4 and orbitals == K and bands == 512
    any_space = pl.BlockSpec(memory_space=pl.ANY)
    vmem = pl.BlockSpec(memory_space=pltpu.VMEM)
    smem = pl.BlockSpec(memory_space=pltpu.SMEM)
    dma = pltpu.SemaphoreType.DMA
    applied, table = pl.pallas_call(
        functools.partial(body_kernel, bands_all),
        out_shape=[jax.ShapeDtypeStruct((bands, 16 * SLOT), BF16), jax.ShapeDtypeStruct((16 * SLOT, gs), BF16)],
        in_specs=[any_space, any_space, vmem, smem, any_space, vmem, vmem],
        out_specs=[any_space, any_space],
        scratch_shapes=[
            pltpu.VMEM((bands, gs), BF16),
            pltpu.VMEM((16 * SLOT, gs), BF16),
            pltpu.VMEM((K, 4, gs), BF16),
            pltpu.VMEM((HID, SPECIES, K * K), F32),
            pltpu.VMEM((8, PAIR, bands), F32),
            pltpu.VMEM((8, PAIR, bands), BF16),
            pltpu.VMEM((8, 3, PAIR, 128), BF16),
            pltpu.VMEM((8, PAIR, 128), BF16),
            pltpu.VMEM((8, PAIR, 128), BF16),
            pltpu.VMEM((16 * SLOT, bands), BF16),
            pltpu.VMEM((SPECIES, K * K, HID), F32),
            pltpu.VMEM((2, 32, 128), F32),
            pltpu.VMEM((32, 128), F32),
            pltpu.VMEM((8, 32, 128), F32),
            pltpu.VMEM((32, 128), F32),
            pltpu.VMEM((16, 32, 128), F32),
            pltpu.VMEM((16 * SLOT, bands), BF16),
            pltpu.VMEM((bands, 16 * SLOT), BF16),
            pltpu.VMEM((SLOT, 128), F32),
            pltpu.VMEM((16, SLOT, 128), F32),
            dma((3,)), dma((8,)), dma((7,)), dma((NT,)), dma((NT,)), dma((16,)), dma((16,)),
            dma((NP, 3)), dma((NP, 3)), dma((NP,)), dma((NP,)), dma((NP, 3)), dma((NP, 3)),
            dma((8,)), dma((8,)), dma((16,)), dma((16,)),
        ],
        compiler_params=pltpu.CompilerParams(
            collective_id=0, has_side_effects=True, vmem_limit_bytes=62 * 2**20
        ),
        name="step",
    )(wave_coef, jnp.transpose(projector, (1, 0, 2)), occupation.reshape(1, bands), species,
      jnp.transpose(layer_in, (2, 0, 1)), bias_in.reshape(-1, 1, HID), layer_out.reshape(-1, 1, HID))
    return jnp.dot(applied, table, preferred_element_type=F32).astype(BF16)


def solution(mesh):
    in_specs = (P("band", "ga"), P("band", None, "ga"), P("band"), P(), P(), P(), P())
    out_specs = P("band", "ga")
    return jax.shard_map(body, mesh=mesh, in_specs=in_specs, out_specs=out_specs, check_vma=False)
```

```python
import functools
import math

import jax
import jax.numpy as jnp
from jax import lax
from jax.experimental import pallas as pl
from jax.experimental.pallas import tpu as pltpu
from jax.sharding import PartitionSpec as P

MESH = pl.DeviceIdType.MESH
F32 = jnp.float32
BF16 = jnp.bfloat16

K = 27
KP = 28
SLOT = 4 * KP
PAIR = 2 * SLOT
HID = 100
SPECIES = 4

ORDER = ((0, 0), (0, 3), (0, 1), (1, 0), (1, 3), (1, 1), (0, 2), (1, 2))

SPLIT = (1, 2, 4, 5, 7)
PIECES = []
EARLY, LATE = {}, {}
for _i in range(8):
    if _i in SPLIT:
        EARLY[_i] = (len(PIECES), len(PIECES) + 1)
        LATE[_i] = (len(PIECES) + 2,)
        PIECES += [(_i, 0, 80), (_i, 144, 80), (_i, 80, 64)]
    else:
        EARLY[_i] = (len(PIECES),)
        PIECES += [(_i, 0, PAIR)]
NP = len(PIECES)

TREE = (
    ("z10", 32, 80), ("x10", 0, 32),
    ("z03a", 32, 48), ("z03b", 80, 32), ("x03", 0, 32), ("z01a", 32, 48), ("z01b", 80, 32), ("x01", 0, 32),
    ("x02a", 0, 16), ("x02b", 16, 16), ("z02a", 32, 48), ("z02b", 80, 32),
    ("z13a", 32, 48), ("z13b", 80, 32), ("z11a", 32, 48), ("z11b", 80, 32), ("x13", 0, 32), ("x11", 0, 32),
    ("x12a", 0, 16), ("x12b", 16, 16), ("z12a", 64, 16), ("z12b", 32, 32),
    ("z12c", 80, 16), ("z12d", 96, 16),
)
TREE_ID = {name: i for i, (name, _, _) in enumerate(TREE)}
NT = len(TREE)


def body_kernel(bands_all, w_hbm, p_hbm, occ_ref, species_ref, lin_hbm, bias_ref, lout_ref, out_ref,
                w, tab, pin, lraw, part, part16, ry, zs, zr, cfull, lin, dsend, dpart, drecv, xs, xall, appt, app, bd, bds,
                lsem, tss, tsr, d2s, d2r, rys, ryr, zss, zsr, ags, agr, dens_s, dens_r, xss, xsr):
    band = lax.axis_index("band")
    ga = lax.axis_index("ga")
    zh, x, c = band // 8, (band // 2) % 4, band % 2
    y, zl = ga // 2, ga % 2

    def at(dz=0, dx=0, dc=0, dy=0, dl=0):
        nzh, nx, nc = (zh + dz) % 2, (x + dx) % 4, (c + dc) % 2
        ny, nzl = (y + dy) % 4, (zl + dl) % 2
        return (nzh * 8 + nx * 2 + nc, ny * 2 + nzl)

    def slot_row(dz, dx, dc):
        nzh, nx, nc = (zh + dz) % 2, (x + dx) % 4, (c + dc) % 2
        return (nzh * 8 + nx * 2 + nc) * SLOT

    def pair_row(dz, dx):
        return (((zh + dz) % 2) * 4 + (x + dx) % 4) * PAIR

    def row_in_slot(first, count, dc=0):
        return jnp.where((c + dc) % 2 == 0, first, SLOT - first - count)

    def rows(ref, start, count):
        return ref.at[pl.ds(pl.multiple_of(start, 16), count)]

    wcopy = pltpu.make_async_copy(w_hbm, w, lsem.at[0])
    own_row = slot_row(0, 0, 0)
    pcopy = pltpu.make_async_copy(p_hbm, pin, lsem.at[1])
    lcopy = pltpu.make_async_copy(lin_hbm, lraw, lsem.at[2])
    pcopy.start()
    wcopy.start()
    lcopy.start()

    barrier = pltpu.get_barrier_semaphore()
    partners = [at(dc=1)]
    for dz in range(2):
        for dx in range(4):
            if dz or dx:
                partners.append(at(dz=dz, dx=dx))
    for dy in range(4):
        for dl in range(2):
            if dy or dl:
                partners.append(at(dy=dy, dl=dl))
                partners.append(at(dy=dy, dl=dl, dc=1))
    for partner in partners:
        pl.semaphore_signal(barrier, inc=1, device_id=partner, device_id_type=MESH)
    pcopy.wait()

    def pack(t, carry):
        cols = pl.ds(pl.multiple_of(t * 512, 512), 512)
        flat = pin[:, :, cols].astype(F32).reshape(4 * K, 512)
        full = jnp.concatenate([flat, jnp.zeros((SLOT - 4 * K, 512), F32)], axis=0)
        tab[pl.ds(pl.multiple_of(own_row, 16), SLOT), cols] = full.astype(BF16)
        return carry

    lax.fori_loop(0, 8, pack, 0)
    pl.semaphore_wait(barrier, len(partners))

    sends = []

    def remote(src, dst, ss, rs, device):
        copy = pltpu.make_async_remote_copy(
            src_ref=src, dst_ref=dst, send_sem=ss, recv_sem=rs, device_id=device, device_id_type=MESH
        )
        copy.start()
        sends.append(copy)

    def arrived(dst, ss, rs):
        pltpu.make_async_remote_copy(
            src_ref=dst, dst_ref=dst, send_sem=ss, recv_sem=rs, device_id=at(dc=1), device_id_type=MESH
        ).wait_recv()

    def tree_send(name, dz, dx, device):
        i = TREE_ID[name]
        _, first, count = TREE[i]
        ref = rows(tab, slot_row(dz, dx, 0) + row_in_slot(first, count), count)
        remote(ref, ref, tss.at[i], tsr.at[i], device)

    def tree_wait(name, dz, dx):
        i = TREE_ID[name]
        _, first, count = TREE[i]
        arrived(rows(tab, slot_row(dz, dx, 0) + row_in_slot(first, count), count), tss.at[i], tsr.at[i])

    def crossing(i, part):
        first, count = ((0, SLOT), (0, 80), (80, 32))[part]
        return ORDER[i], first, count, i + 8 * (part == 2)

    def across(i, part=0):
        (dz, dx), first, count, sem = crossing(i, part)
        ref = rows(tab, slot_row(dz, dx, 0) + row_in_slot(first, count), count)
        remote(ref, ref, d2s.at[sem], d2r.at[sem], at(dc=1))

    def across_wait(i, part=0):
        (dz, dx), first, count, sem = crossing(i, part)
        arrived(rows(tab, slot_row(dz, dx, 1) + row_in_slot(first, count, 1), count), d2s.at[sem], d2r.at[sem])

    right, left, over = at(dx=1), at(dx=3), at(dz=1)

    def project(pieces):
        i = PIECES[pieces[0]][0]
        base = pair_row(*ORDER[i])

        def half(t, carry):
            cols = pl.ds(pl.multiple_of(t * 256, 256), 256)
            table = [tab[pl.ds(pl.multiple_of(base + PIECES[s][1], 16), PIECES[s][2]), :] for s in pieces]
            table = table[0] if len(pieces) == 1 else jnp.concatenate(table, axis=0)
            got = lax.dot_general(table, w[cols, :], (((1,), (1,)), ((), ())), preferred_element_type=F32)
            done = 0
            for s in pieces:
                _, first, count = PIECES[s]
                part[i, first:first + count, cols] = got[done:done + count]
                part16[i, first:first + count, cols] = got[done:done + count].astype(BF16)
                done += count
            return carry

        lax.fori_loop(0, 2, half, 0)
        for s in pieces:
            here = pl.ds(PIECES[s][1], PIECES[s][2])
            for dy in (2, 1, 3):
                lanes = pl.ds(pl.multiple_of(((y + dy) % 4) * 128, 128), 128)
                remote(part16.at[i, here, lanes], ry.at[i, 3 - dy, here], rys.at[s, 3 - dy], ryr.at[s, 3 - dy], at(dy=dy))

    mine = pl.ds(pl.multiple_of(y * 128, 128), 128)

    def reduce_y(s):
        i, first, count = PIECES[s]
        here = pl.ds(first, count)
        for j in range(3):
            arrived(ry.at[i, j, here], rys.at[s, j], ryr.at[s, j])
        total = part[i, here, mine]
        for j in range(3):
            total = total + ry[i, j, here].astype(F32)
        part[i, here, mine] = total
        zs[i, here] = total.astype(BF16)
        remote(zs.at[i, here], zr.at[i, here], zss.at[s], zsr.at[s], at(dl=1))

    def in_full(s):
        i, first, count = PIECES[s]
        return pl.ds(pl.multiple_of(pair_row(*ORDER[i]) + first, 16), count)

    def direct(s):
        return PIECES[s][0] == 7

    def block(s, dy):
        lanes = pl.ds(pl.multiple_of(((y + dy) % 4) * 128, 128), 128)
        return cfull.at[in_full(s), lanes]

    def reduce_z(s):
        i, first, count = PIECES[s]
        here = pl.ds(first, count)
        arrived(zr.at[i, here], zss.at[s], zsr.at[s])
        cfull[in_full(s), mine] = (part[i, here, mine] + zr[i, here].astype(F32)).astype(BF16)
        for dy in (2, 1, 3) if direct(s) else (1, 3):
            remote(block(s, 0), block(s, 0), ags.at[s, 3 - dy], agr.at[s, 3 - dy], at(dy=dy))

    def relay(s):
        for dy in (1, 3):
            arrived(block(s, dy), ags.at[s, dy - 1], agr.at[s, dy - 1])
        dy = 1 + 2 * (s % 2)
        remote(block(s, dy), block(s, dy), ags.at[s, 1], agr.at[s, 1], at(dy=4 - dy))

    def gathered(s):
        for dy in (1, 2, 3) if direct(s) else (2,):
            arrived(block(s, dy), ags.at[s, dy - 1], agr.at[s, dy - 1])

    tree_send("z10", 0, 0, over)
    tree_send("x03", 0, 0, right)
    tree_send("x01", 0, 0, left)
    across(0)
    tree_send("z03a", 0, 0, right)
    tree_send("z01a", 0, 0, left)
    tree_send("z03b", 0, 0, right)
    tree_send("z01b", 0, 0, left)
    wcopy.wait()
    across_wait(0)
    project(EARLY[0])
    tree_wait("x03", 0, 3)
    tree_send("x02a", 0, 3, right)
    tree_wait("x01", 0, 1)
    tree_send("x02b", 0, 1, left)
    for s in EARLY[0]:
        reduce_y(s)
    tree_send("x10", 0, 0, over)
    tree_send("x13", 0, 3, over)
    tree_send("x11", 0, 1, over)
    lcopy.wait()
    for kind in range(SPECIES):
        lin[kind] = lraw[:, kind, :].T
    tree_wait("z03a", 0, 3)
    across(1, 1)
    tree_wait("z01a", 0, 1)
    across(2, 1)
    tree_wait("z10", 1, 0)
    tree_send("z13a", 1, 0, right)
    tree_send("z11a", 1, 0, left)
    tree_send("z13b", 1, 0, right)
    tree_send("z11b", 1, 0, left)
    tree_send("z02a", 0, 3, right)
    for s in EARLY[0]:
        reduce_z(s)
    across_wait(1, 1)
    project(EARLY[1])
    across_wait(2, 1)
    project(EARLY[2])
    tree_wait("z03b", 0, 3)
    across(1, 2)
    tree_wait("z01b", 0, 1)
    tree_send("z02b", 0, 1, left)
    across(2, 2)
    tree_wait("x10", 1, 0)
    across(3)
    across_wait(1, 2)
    project(LATE[1])
    for s in EARLY[0]:
        relay(s)
    for s in EARLY[1]:
        reduce_y(s)
    across_wait(2, 2)
    project(LATE[2])
    for s in EARLY[2]:
        reduce_y(s)
    across_wait(3)
    project(EARLY[3])
    for s in LATE[1]:
        reduce_y(s)
    for s in LATE[2]:
        reduce_y(s)
    tree_wait("x02a", 0, 2)
    tree_wait("x02b", 0, 2)
    tree_send("x12a", 0, 2, over)
    tree_send("x12b", 0, 2, over)
    tree_wait("z13a", 1, 3)
    tree_send("z12a", 1, 3, right)
    tree_wait("z11a", 1, 1)
    tree_send("z12b", 1, 1, left)
    tree_wait("x13", 1, 3)
    across(4, 1)
    tree_wait("x11", 1, 1)
    across(5, 1)
    for s in EARLY[3]:
        reduce_y(s)
    across_wait(4, 1)
    project(EARLY[4])
    across_wait(5, 1)
    project(EARLY[5])
    for s in EARLY[1]:
        reduce_z(s)
    for s in EARLY[2]:
        reduce_z(s)
    tree_wait("z13b", 1, 3)
    tree_send("z12c", 1, 3, right)
    across(4, 2)
    tree_wait("z11b", 1, 1)
    tree_send("z12d", 1, 1, left)
    across(5, 2)
    for s in LATE[1]:
        reduce_z(s)
    for s in LATE[2]:
        reduce_z(s)
    across_wait(4, 2)
    project(LATE[4])
    for s in EARLY[4]:
        reduce_y(s)
    across_wait(5, 2)
    project(LATE[5])
    for s in EARLY[5]:
        reduce_y(s)
    for s in EARLY[3]:
        reduce_z(s)
    for s in EARLY[1]:
        relay(s)
    for s in EARLY[2]:
        relay(s)
    tree_wait("z02a", 0, 2)
    across(6, 1)
    tree_wait("z02b", 0, 2)
    across(6, 2)
    for s in LATE[4]:
        reduce_y(s)
    for s in LATE[5]:
        reduce_y(s)
    for s in LATE[1]:
        relay(s)
    for s in LATE[2]:
        relay(s)
    for s in EARLY[4]:
        reduce_z(s)
    across_wait(6, 1)
    across_wait(6, 2)
    project(EARLY[6])
    for s in EARLY[5]:
        reduce_z(s)
    for s in EARLY[3]:
        relay(s)
    tree_wait("x12a", 1, 2)
    tree_wait("x12b", 1, 2)
    tree_wait("z12a", 1, 2)
    tree_wait("z12b", 1, 2)
    across(7, 1)
    for s in LATE[4]:
        reduce_z(s)
    for s in LATE[5]:
        reduce_z(s)
    across_wait(7, 1)
    project(EARLY[7])
    tree_wait("z12c", 1, 2)
    tree_wait("z12d", 1, 2)
    across(7, 2)
    for s in EARLY[6]:
        reduce_y(s)
    for s in EARLY[4]:
        relay(s)
    for s in EARLY[5]:
        relay(s)
    across_wait(7, 2)
    project(LATE[7])
    for s in EARLY[7]:
        reduce_y(s)
    for s in LATE[4]:
        relay(s)
    for s in LATE[5]:
        relay(s)
    for s in LATE[7]:
        reduce_y(s)
    for s in EARLY[6]:
        reduce_z(s)
    for s in EARLY[7]:
        reduce_z(s)
    for s in LATE[7]:
        reduce_z(s)
    for s in EARLY[6]:
        relay(s)
    for s in range(NP):
        gathered(s)

    lane_atom = lax.broadcasted_iota(jnp.int32, (KP, SLOT), 1) % 4
    occ = occ_ref[...]
    for h in range(2):
        coef = cfull[pl.ds(pl.multiple_of(ga * PAIR + h * SLOT, 16), SLOT), :]
        weighted = coef.astype(F32) * occ
        high = weighted.astype(BF16)
        low = (weighted - high.astype(F32)).astype(BF16)
        dims = (((1,), (1,)), ((), ()))
        gram = lax.dot_general(high, coef, dims, preferred_element_type=F32) + lax.dot_general(
            low, coef, dims, preferred_element_type=F32
        )
        bd[:, 0:SLOT] = gram
        packed = jnp.zeros((KP, SLOT), F32)
        for a in range(4):
            packed = packed + jnp.where(lane_atom == a, bd[pl.ds(a, KP, stride=4), :][:, 0:SLOT], 0.0)
        dsend[h, 0:KP, 0:SLOT] = packed
    remote(dsend.at[1 - c], drecv.at[7], dens_s.at[7], dens_r.at[7], at(dc=1))
    arrived(drecv.at[7], dens_s.at[7], dens_r.at[7])
    dpart[...] = dsend[c] + drecv[7]
    for dz in range(2):
        for dx in range(4):
            if dz or dx:
                j = dz * 4 + (4 - dx) % 4 - 1
                remote(dpart, drecv.at[j], dens_s.at[j], dens_r.at[j], at(dz=dz, dx=dx))
    for j in range(7):
        arrived(drecv.at[j], dens_s.at[j], dens_r.at[j])
    density = dpart[...]
    for j in range(7):
        density = density + drecv[j]
    density = density * (1.0 / bands_all)

    lane = lax.broadcasted_iota(jnp.int32, (K, SLOT), 1)
    grad_t = jnp.zeros((K, SLOT), F32)
    slot = 2 * ga + c
    for a in range(4):
        kind = species_ref[4 * slot + a]
        acc = jnp.zeros((K, HID), F32)
        for k in range(K):
            acc = acc + density[0:K, 4 * k + a:4 * k + a + 1] * lin[kind, k * K:(k + 1) * K, :]
        preact = jnp.sum(acc, axis=0, keepdims=True) + bias_ref[kind]
        act = jnp.tanh(preact)
        slope = lout_ref[kind] * (1.0 - act * act)
        for k in range(K):
            column = jnp.sum(lin[kind, k * K:(k + 1) * K, :] * slope, axis=1, keepdims=True)
            grad_t = jnp.where(lane == 4 * k + a, column, grad_t)
    bd[...] = jnp.zeros((SLOT, 128), F32)
    pad = jnp.zeros((K, 128 - SLOT), F32)
    for a in range(4):
        bd[pl.ds(a, K, stride=4), :] = jnp.concatenate([jnp.where(lane % 4 == a, grad_t, 0.0), pad], axis=1)
    square = bd[:, 0:SLOT]
    bd[:, 0:SLOT] = square + square.T
    packed = jnp.zeros((KP, 128), F32)
    for a in range(4):
        packed = packed + bd[pl.ds(a, KP, stride=4), :]
    xs[0:KP, :] = packed
    xall[slot] = xs[...]
    for dy in range(4):
        for dl in range(2):
            for dc in range(2):
                if dy or dl or dc:
                    j = (((4 - dy) % 4) * 2 + dl) * 2 + dc
                    remote(xs, xall.at[slot], xss.at[j], xsr.at[j], at(dy=dy, dl=dl, dc=dc))
    for dy in range(4):
        for dl in range(2):
            for dc in range(2):
                if dy or dl or dc:
                    j = (dy * 2 + dl) * 2 + dc
                    from_slot = 2 * (((y + dy) % 4) * 2 + (zl + dl) % 2) + (c + dc) % 2
                    arrived(xall.at[from_slot], xss.at[j], xsr.at[j])

    factor = 1.0 / math.sqrt(64 * K)
    rows4 = lax.broadcasted_iota(jnp.int32, (SLOT, SLOT), 0) % 4
    lanes4 = lax.broadcasted_iota(jnp.int32, (SLOT, SLOT), 1) % 4
    same = rows4 == lanes4

    def apply(j, carry):
        for a in range(4):
            bds[j, pl.ds(a, KP, stride=4), :] = xall[j, 0:KP, :]
        full = jnp.where(same, bds[j, :, 0:SLOT], 0.0)
        high = full.astype(BF16)
        low = (full - high.astype(F32)).astype(BF16)
        at_rows = pl.ds(pl.multiple_of(j * SLOT, 16), SLOT)
        coef = cfull[at_rows, :]
        got = jnp.dot(high, coef, preferred_element_type=F32) + jnp.dot(low, coef, preferred_element_type=F32)
        appt[at_rows, :] = (got * factor).astype(BF16)
        return carry

    lax.fori_loop(0, 16, apply, 0, unroll=4)

    def turn(j, carry):
        block = pl.ds(pl.multiple_of(j * 256, 256), 256)
        app[:, block] = appt[block, :].T
        return carry

    lax.fori_loop(0, 7, turn, 0)

    def correct(t, carry):
        cols = pl.ds(pl.multiple_of(t * 512, 512), 512)
        out_ref[:, cols] = jnp.dot(app[...], tab[:, cols], preferred_element_type=F32).astype(BF16)
        return carry

    lax.fori_loop(0, 8, correct, 0)
    for copy in sends:
        copy.wait_send()


def body(wave_coef, projector, occupation, species, layer_in, bias_in, layer_out):
    atoms_here, orbitals, gs = projector.shape
    bands = wave_coef.shape[0]
    bands_all = bands * lax.axis_size("band")
    assert atoms_here == 4 and orbitals == K and bands == 512
    hbm = pl.BlockSpec(memory_space=pltpu.HBM)
    vmem = pl.BlockSpec(memory_space=pltpu.VMEM)
    smem = pl.BlockSpec(memory_space=pltpu.SMEM)
    dma = pltpu.SemaphoreType.DMA
    return pl.pallas_call(
        functools.partial(body_kernel, bands_all),
        out_shape=pltpu.VMEM((bands, gs), BF16),
        in_specs=[hbm, hbm, vmem, smem, hbm, vmem, vmem],
        out_specs=vmem,
        scratch_shapes=[
            pltpu.VMEM((bands, gs), BF16),
            pltpu.VMEM((16 * SLOT, gs), BF16),
            pltpu.VMEM((K, 4, gs), BF16),
            pltpu.VMEM((HID, SPECIES, K * K), F32),
            pltpu.VMEM((8, PAIR, bands), F32),
            pltpu.VMEM((8, PAIR, bands), BF16),
            pltpu.VMEM((8, 3, PAIR, 128), BF16),
            pltpu.VMEM((8, PAIR, 128), BF16),
            pltpu.VMEM((8, PAIR, 128), BF16),
            pltpu.VMEM((16 * SLOT, bands), BF16),
            pltpu.VMEM((SPECIES, K * K, HID), F32),
            pltpu.VMEM((2, 32, 128), F32),
            pltpu.VMEM((32, 128), F32),
            pltpu.VMEM((8, 32, 128), F32),
            pltpu.VMEM((32, 128), F32),
            pltpu.VMEM((16, 32, 128), F32),
            pltpu.VMEM((16 * SLOT, bands), BF16),
            pltpu.VMEM((bands, 16 * SLOT), BF16),
            pltpu.VMEM((SLOT, 128), F32),
            pltpu.VMEM((16, SLOT, 128), F32),
            dma((3,)), dma((NT,)), dma((NT,)), dma((16,)), dma((16,)),
            dma((NP, 3)), dma((NP, 3)), dma((NP,)), dma((NP,)), dma((NP, 3)), dma((NP, 3)),
            dma((8,)), dma((8,)), dma((16,)), dma((16,)),
        ],
        compiler_params=pltpu.CompilerParams(
            collective_id=0, has_side_effects=True, vmem_limit_bytes=57 * 2**20
        ),
        name="step",
    )(wave_coef, jnp.transpose(projector, (1, 0, 2)), occupation.reshape(1, bands), species,
      jnp.transpose(layer_in, (2, 0, 1)), bias_in.reshape(-1, 1, HID), layer_out.reshape(-1, 1, HID))


def solution(mesh):
    in_specs = (P("band", "ga"), P("band", None, "ga"), P("band"), P(), P(), P(), P())
    out_specs = P("band", "ga")
    return jax.shard_map(body, mesh=mesh, in_specs=in_specs, out_specs=out_specs, check_vma=False)
```

```python
import functools
import math

import jax
import jax.numpy as jnp
from jax import lax
from jax.experimental import pallas as pl
from jax.experimental.pallas import tpu as pltpu
from jax.sharding import PartitionSpec as P

MESH = pl.DeviceIdType.MESH
F32 = jnp.float32
BF16 = jnp.bfloat16

K = 27
KP = 28
SLOT = 4 * KP
PAIR = 2 * SLOT
HID = 100
SPECIES = 4

ORDER = ((0, 0), (0, 3), (0, 1), (1, 0), (1, 3), (1, 1), (0, 2), (1, 2))

SPLIT = (1, 2, 4, 5, 7)
TABLE_ROWS = ((0, 80), (144, 80), (80, 64))
PIECES = []
EARLY, LATE = {}, {}
for _i in range(8):
    EARLY[_i] = len(PIECES)
    if _i in SPLIT:
        LATE[_i] = EARLY[_i] + 1
        PIECES += [(_i, 0, 160), (_i, 160, 64)]
    else:
        PIECES += [(_i, 0, PAIR)]
NP = len(PIECES)
POOL = 64

TREE = (
    ("z10", 32, 80), ("x10", 0, 32),
    ("z03a", 32, 48), ("z03b", 80, 32), ("x03", 0, 32), ("z01a", 32, 48), ("z01b", 80, 32), ("x01", 0, 32),
    ("x02a", 0, 16), ("x02b", 16, 16), ("z02a", 32, 48), ("z02b", 80, 32),
    ("z13a", 32, 48), ("z13b", 80, 32), ("z11a", 32, 48), ("z11b", 80, 32), ("x13", 0, 32), ("x11", 0, 32),
    ("x12a", 0, 16), ("x12b", 16, 16), ("z12a", 64, 16), ("z12b", 32, 32),
    ("z12c", 80, 16), ("z12d", 96, 16),
)
TREE_ID = {name: i for i, (name, _, _) in enumerate(TREE)}
NT = len(TREE)


def body_kernel(bands_all, w_hbm, p_hbm, occ_ref, species_ref, lin_hbm, bias_ref, lout_ref, app, tab,
                w, pin, lraw, part, part16, ry, zs, zr, cfull, lin, dsend, dpart, drecv, xs, xall, appt, bd, bds,
                lsem, pool, tsr, d2r, ryr, zsr, agr, dens_r, xsr):
    band = lax.axis_index("band")
    ga = lax.axis_index("ga")
    zh, x, c = band // 8, (band // 2) % 4, band % 2
    y, zl = ga // 2, ga % 2

    def at(dz=0, dx=0, dc=0, dy=0, dl=0):
        nzh, nx, nc = (zh + dz) % 2, (x + dx) % 4, (c + dc) % 2
        ny, nzl = (y + dy) % 4, (zl + dl) % 2
        return (nzh * 8 + nx * 2 + nc, ny * 2 + nzl)

    def slot_row(dz, dx, dc):
        nzh, nx, nc = (zh + dz) % 2, (x + dx) % 4, (c + dc) % 2
        return (nzh * 8 + nx * 2 + nc) * SLOT

    def pair_row(dz, dx):
        return (((zh + dz) % 2) * 4 + (x + dx) % 4) * PAIR

    def row_in_slot(first, count, dc=0):
        return jnp.where((c + dc) % 2 == 0, first, SLOT - first - count)

    def rows(ref, start, count):
        return ref.at[pl.ds(pl.multiple_of(start, 16), count)]

    wcopy = pltpu.make_async_copy(w_hbm, w, lsem.at[0])
    own_row = slot_row(0, 0, 0)
    pcopy = pltpu.make_async_copy(p_hbm, pin, lsem.at[1])
    lcopy = pltpu.make_async_copy(lin_hbm, lraw, lsem.at[2])
    pcopy.start()
    wcopy.start()
    lcopy.start()

    barrier = pltpu.get_barrier_semaphore()
    partners = [at(dc=1)]
    for dz in range(2):
        for dx in range(4):
            if dz or dx:
                partners.append(at(dz=dz, dx=dx))
    for dy in range(4):
        for dl in range(2):
            if dy or dl:
                partners.append(at(dy=dy, dl=dl))
                partners.append(at(dy=dy, dl=dl, dc=1))
    for partner in partners:
        pl.semaphore_signal(barrier, inc=1, device_id=partner, device_id_type=MESH)
    pcopy.wait()

    def pack(t, carry):
        cols = pl.ds(pl.multiple_of(t * 512, 512), 512)
        flat = pin[:, :, cols].astype(F32).reshape(4 * K, 512)
        full = jnp.concatenate([flat, jnp.zeros((SLOT - 4 * K, 512), F32)], axis=0)
        tab[pl.ds(pl.multiple_of(own_row, 16), SLOT), cols] = full.astype(BF16)
        return carry

    lax.fori_loop(0, 8, pack, 0)
    pl.semaphore_wait(barrier, len(partners))

    sends = []

    def remote(src, dst, rs, device):
        n = len(sends)
        if n >= POOL:
            sends[n - POOL].wait_send()
        copy = pltpu.make_async_remote_copy(
            src_ref=src, dst_ref=dst, send_sem=pool.at[n % POOL], recv_sem=rs, device_id=device, device_id_type=MESH
        )
        copy.start()
        sends.append(copy)

    def arrived(dst, rs):
        pltpu.make_async_remote_copy(
            src_ref=dst, dst_ref=dst, send_sem=pool.at[0], recv_sem=rs, device_id=at(dc=1), device_id_type=MESH
        ).wait_recv()

    def tree_send(name, dz, dx, device):
        i = TREE_ID[name]
        _, first, count = TREE[i]
        ref = rows(tab, slot_row(dz, dx, 0) + row_in_slot(first, count), count)
        remote(ref, ref, tsr.at[i], device)

    def tree_wait(name, dz, dx):
        i = TREE_ID[name]
        _, first, count = TREE[i]
        arrived(rows(tab, slot_row(dz, dx, 0) + row_in_slot(first, count), count), tsr.at[i])

    def crossing(i, part):
        first, count = ((0, SLOT), (0, 80), (80, 32))[part]
        return ORDER[i], first, count, i + 8 * (part == 2)

    def across(i, part=0):
        (dz, dx), first, count, sem = crossing(i, part)
        ref = rows(tab, slot_row(dz, dx, 0) + row_in_slot(first, count), count)
        remote(ref, ref, d2r.at[sem], at(dc=1))

    def across_wait(i, part=0):
        (dz, dx), first, count, sem = crossing(i, part)
        arrived(rows(tab, slot_row(dz, dx, 1) + row_in_slot(first, count, 1), count), d2r.at[sem])

    right, left, over = at(dx=1), at(dx=3), at(dz=1)

    def project(s):
        i, first, count = PIECES[s]
        base = pair_row(*ORDER[i])

        def read(start, size):
            return tab[pl.ds(pl.multiple_of(base + start, 16), size), :]

        def half(t, carry):
            cols = pl.ds(pl.multiple_of(t * 256, 256), 256)

            def times(table):
                return lax.dot_general(table, w[cols, :], (((1,), (1,)), ((), ())), preferred_element_type=F32)

            def keep(to, got):
                part[i, to:to + got.shape[0], cols] = got
                part16[i, to:to + got.shape[0], cols] = got.astype(BF16)

            if count == PAIR:
                got = times(read(0, PAIR))
                to = 0
                for start, size in TABLE_ROWS:
                    keep(to, got[start:start + size])
                    to += size
            elif first == 0:
                keep(0, times(jnp.concatenate([read(*span) for span in TABLE_ROWS[:2]], axis=0)))
            else:
                keep(first, times(read(*TABLE_ROWS[2])))
            return carry

        lax.fori_loop(0, 2, half, 0)
        here = pl.ds(first, count)
        for dy in (2, 1, 3):
            lanes = pl.ds(pl.multiple_of(((y + dy) % 4) * 128, 128), 128)
            remote(part16.at[i, here, lanes], ry.at[i, 3 - dy, here], ryr.at[s], at(dy=dy))

    mine = pl.ds(pl.multiple_of(y * 128, 128), 128)

    def reduce_y(s):
        i, first, count = PIECES[s]
        here = pl.ds(first, count)
        total = part[i, here, mine]
        arrived(ry.at[i, :, here], ryr.at[s])
        for j in range(3):
            total = total + ry[i, j, here].astype(F32)
        part[i, here, mine] = total
        zs[i, here] = total.astype(BF16)
        remote(zs.at[i, here], zr.at[i, here], zsr.at[s], at(dl=1))

    def direct(s):
        return PIECES[s][0] == 7

    def block_at(s, dy):
        i, first, count = PIECES[s]
        lanes = pl.ds(pl.multiple_of(((y + dy) % 4) * 128, 128), 128)
        return pl.ds(pl.multiple_of(pair_row(*ORDER[i]) + first, 16), count), lanes

    def block(s, dy):
        return cfull.at[block_at(s, dy)]

    def reduce_z(s):
        i, first, count = PIECES[s]
        here = pl.ds(first, count)
        arrived(zr.at[i, here], zsr.at[s])
        cfull[block_at(s, 0)] = (part[i, here, mine] + zr[i, here].astype(F32)).astype(BF16)
        for dy in (2, 1, 3) if direct(s) else (1, 3):
            remote(block(s, 0), block(s, 0), agr.at[s, 3 - dy], at(dy=dy))

    def relay(s):
        for dy in (1, 3):
            arrived(block(s, dy), agr.at[s, dy - 1])
        dy = 1 + 2 * (s % 2)
        remote(block(s, dy), block(s, dy), agr.at[s, 1], at(dy=4 - dy))

    def gathered(s):
        for dy in (1, 2, 3) if direct(s) else (2,):
            arrived(block(s, dy), agr.at[s, dy - 1])

    def coef_of(pair, h):
        cuts = ((0, 80), (160, 32)) if h == 0 else ((192, 32), (80, 80))
        return jnp.concatenate([cfull[pl.ds(pl.multiple_of(pair * PAIR + a, 16), n), :] for a, n in cuts], axis=0)

    tree_send("z10", 0, 0, over)
    tree_send("x03", 0, 0, right)
    tree_send("x01", 0, 0, left)
    across(0)
    tree_send("z03a", 0, 0, right)
    tree_send("z01a", 0, 0, left)
    tree_send("z03b", 0, 0, right)
    tree_send("z01b", 0, 0, left)
    wcopy.wait()
    across_wait(0)
    project(EARLY[0])
    tree_wait("x03", 0, 3)
    tree_send("x02a", 0, 3, right)
    tree_wait("x01", 0, 1)
    tree_send("x02b", 0, 1, left)
    reduce_y(EARLY[0])
    tree_send("x10", 0, 0, over)
    tree_send("x13", 0, 3, over)
    tree_send("x11", 0, 1, over)
    lcopy.wait()
    for kind in range(SPECIES):
        lin[kind] = lraw[:, kind, :].T
    tree_wait("z03a", 0, 3)
    across(1, 1)
    tree_wait("z01a", 0, 1)
    across(2, 1)
    tree_wait("z10", 1, 0)
    tree_send("z13a", 1, 0, right)
    tree_send("z11a", 1, 0, left)
    tree_send("z13b", 1, 0, right)
    tree_send("z11b", 1, 0, left)
    tree_send("z02a", 0, 3, right)
    reduce_z(EARLY[0])
    across_wait(1, 1)
    project(EARLY[1])
    across_wait(2, 1)
    project(EARLY[2])
    tree_wait("z03b", 0, 3)
    across(1, 2)
    tree_wait("z01b", 0, 1)
    tree_send("z02b", 0, 1, left)
    across(2, 2)
    tree_wait("x10", 1, 0)
    across(3)
    across_wait(1, 2)
    project(LATE[1])
    relay(EARLY[0])
    reduce_y(EARLY[1])
    across_wait(2, 2)
    project(LATE[2])
    reduce_y(EARLY[2])
    across_wait(3)
    project(EARLY[3])
    reduce_y(LATE[1])
    reduce_y(LATE[2])
    tree_wait("x02a", 0, 2)
    tree_wait("x02b", 0, 2)
    tree_send("x12a", 0, 2, over)
    tree_send("x12b", 0, 2, over)
    tree_wait("z13a", 1, 3)
    tree_send("z12a", 1, 3, right)
    tree_wait("z11a", 1, 1)
    tree_send("z12b", 1, 1, left)
    tree_wait("x13", 1, 3)
    across(4, 1)
    tree_wait("x11", 1, 1)
    across(5, 1)
    reduce_y(EARLY[3])
    across_wait(4, 1)
    project(EARLY[4])
    across_wait(5, 1)
    project(EARLY[5])
    reduce_z(EARLY[1])
    reduce_z(EARLY[2])
    tree_wait("z13b", 1, 3)
    tree_send("z12c", 1, 3, right)
    across(4, 2)
    tree_wait("z11b", 1, 1)
    tree_send("z12d", 1, 1, left)
    across(5, 2)
    reduce_z(LATE[1])
    reduce_z(LATE[2])
    across_wait(4, 2)
    project(LATE[4])
    reduce_y(EARLY[4])
    across_wait(5, 2)
    project(LATE[5])
    reduce_y(EARLY[5])
    reduce_z(EARLY[3])
    relay(EARLY[1])
    relay(EARLY[2])
    tree_wait("z02a", 0, 2)
    across(6, 1)
    tree_wait("z02b", 0, 2)
    across(6, 2)
    reduce_y(LATE[4])
    reduce_y(LATE[5])
    relay(LATE[1])
    relay(LATE[2])
    reduce_z(EARLY[4])
    across_wait(6, 1)
    across_wait(6, 2)
    project(EARLY[6])
    reduce_z(EARLY[5])
    relay(EARLY[3])
    tree_wait("x12a", 1, 2)
    tree_wait("x12b", 1, 2)
    tree_wait("z12a", 1, 2)
    tree_wait("z12b", 1, 2)
    across(7, 1)
    reduce_z(LATE[4])
    reduce_z(LATE[5])
    across_wait(7, 1)
    project(EARLY[7])
    tree_wait("z12c", 1, 2)
    tree_wait("z12d", 1, 2)
    across(7, 2)
    across_wait(7, 2)
    project(LATE[7])
    reduce_y(EARLY[6])
    relay(EARLY[4])
    relay(EARLY[5])
    reduce_y(EARLY[7])
    reduce_y(LATE[7])
    relay(LATE[4])
    relay(LATE[5])
    reduce_z(EARLY[6])
    reduce_z(EARLY[7])
    reduce_z(LATE[7])
    relay(EARLY[6])
    for s in range(NP):
        gathered(s)

    lane_atom = lax.broadcasted_iota(jnp.int32, (KP, SLOT), 1) % 4
    occ = occ_ref[...]
    for h in range(2):
        coef = coef_of(ga, h)
        weighted = coef.astype(F32) * occ
        high = weighted.astype(BF16)
        low = (weighted - high.astype(F32)).astype(BF16)
        dims = (((1,), (1,)), ((), ()))
        gram = lax.dot_general(high, coef, dims, preferred_element_type=F32) + lax.dot_general(
            low, coef, dims, preferred_element_type=F32
        )
        bd[:, 0:SLOT] = gram
        packed = jnp.zeros((KP, SLOT), F32)
        for a in range(4):
            packed = packed + jnp.where(lane_atom == a, bd[pl.ds(a, KP, stride=4), :][:, 0:SLOT], 0.0)
        dsend[h, 0:KP, 0:SLOT] = packed
    remote(dsend.at[1 - c], drecv.at[7], dens_r.at[7], at(dc=1))
    arrived(drecv.at[7], dens_r.at[7])
    dpart[...] = dsend[c] + drecv[7]
    for dz in range(2):
        for dx in range(4):
            if dz or dx:
                j = dz * 4 + (4 - dx) % 4 - 1
                remote(dpart, drecv.at[j], dens_r.at[j], at(dz=dz, dx=dx))
    for j in range(7):
        arrived(drecv.at[j], dens_r.at[j])
    density = dpart[...]
    for j in range(7):
        density = density + drecv[j]
    density = density * (1.0 / bands_all)

    lane = lax.broadcasted_iota(jnp.int32, (K, SLOT), 1)
    grad_t = jnp.zeros((K, SLOT), F32)
    slot = 2 * ga + c
    for a in range(4):
        kind = species_ref[4 * slot + a]
        acc = jnp.zeros((K, HID), F32)
        for k in range(K):
            acc = acc + density[0:K, 4 * k + a:4 * k + a + 1] * lin[kind, k * K:(k + 1) * K, :]
        preact = jnp.sum(acc, axis=0, keepdims=True) + bias_ref[kind]
        act = jnp.tanh(preact)
        slope = lout_ref[kind] * (1.0 - act * act)
        for k in range(K):
            column = jnp.sum(lin[kind, k * K:(k + 1) * K, :] * slope, axis=1, keepdims=True)
            grad_t = jnp.where(lane == 4 * k + a, column, grad_t)
    bd[...] = jnp.zeros((SLOT, 128), F32)
    pad = jnp.zeros((K, 128 - SLOT), F32)
    for a in range(4):
        bd[pl.ds(a, K, stride=4), :] = jnp.concatenate([jnp.where(lane % 4 == a, grad_t, 0.0), pad], axis=1)
    square = bd[:, 0:SLOT]
    bd[:, 0:SLOT] = square + square.T
    packed = jnp.zeros((KP, 128), F32)
    for a in range(4):
        packed = packed + bd[pl.ds(a, KP, stride=4), :]
    xs[0:KP, :] = packed
    xall[slot] = xs[...]
    for dy in range(4):
        for dl in range(2):
            for dc in range(2):
                if dy or dl or dc:
                    j = (((4 - dy) % 4) * 2 + dl) * 2 + dc
                    remote(xs, xall.at[slot], xsr.at[j], at(dy=dy, dl=dl, dc=dc))
    for dy in range(4):
        for dl in range(2):
            for dc in range(2):
                if dy or dl or dc:
                    j = (dy * 2 + dl) * 2 + dc
                    from_slot = 2 * (((y + dy) % 4) * 2 + (zl + dl) % 2) + (c + dc) % 2
                    arrived(xall.at[from_slot], xsr.at[j])

    factor = 1.0 / math.sqrt(64 * K)
    rows4 = lax.broadcasted_iota(jnp.int32, (SLOT, SLOT), 0) % 4
    lanes4 = lax.broadcasted_iota(jnp.int32, (SLOT, SLOT), 1) % 4
    same = rows4 == lanes4

    def apply(pair, carry):
        for h in range(2):
            j = 2 * pair + h
            for a in range(4):
                bds[j, pl.ds(a, KP, stride=4), :] = xall[j, 0:KP, :]
            full = jnp.where(same, bds[j, :, 0:SLOT], 0.0)
            high = full.astype(BF16)
            low = (full - high.astype(F32)).astype(BF16)
            coef = coef_of(pair, h)
            got = jnp.dot(high, coef, preferred_element_type=F32) + jnp.dot(low, coef, preferred_element_type=F32)
            appt[pl.ds(pl.multiple_of(j * SLOT, 16), SLOT), :] = (got * factor).astype(BF16)
        return carry

    lax.fori_loop(0, 8, apply, 0, unroll=2)

    def turn(j, carry):
        block = pl.ds(pl.multiple_of(j * 256, 256), 256)
        app[:, block] = appt[block, :].T
        return carry

    lax.fori_loop(0, 7, turn, 0)
    for copy in sends[-POOL:]:
        copy.wait_send()


def correct_kernel(app, tab, out_hbm, out, sems):
    def store(t):
        cols = pl.ds(pl.multiple_of(t * 512, 512), 512)
        return pltpu.make_async_copy(out.at[:, cols], out_hbm.at[:, cols], sems.at[t])

    def one(t, carry):
        cols = pl.ds(pl.multiple_of(t * 512, 512), 512)
        out[:, cols] = jnp.dot(app[...], tab[:, cols], preferred_element_type=F32).astype(BF16)
        store(t).start()
        return carry

    steps = out.shape[1] // 512
    lax.fori_loop(0, steps, one, 0)
    for t in range(steps):
        store(t).wait()


def body(wave_coef, projector, occupation, species, layer_in, bias_in, layer_out):
    atoms_here, orbitals, gs = projector.shape
    bands = wave_coef.shape[0]
    bands_all = bands * lax.axis_size("band")
    assert atoms_here == 4 and orbitals == K and bands == 512
    hbm = pl.BlockSpec(memory_space=pltpu.HBM)
    vmem = pl.BlockSpec(memory_space=pltpu.VMEM)
    smem = pl.BlockSpec(memory_space=pltpu.SMEM)
    dma = pltpu.SemaphoreType.DMA
    applied, table = pl.pallas_call(
        functools.partial(body_kernel, bands_all),
        out_shape=[pltpu.VMEM((bands, 16 * SLOT), BF16), pltpu.VMEM((16 * SLOT, gs), BF16)],
        in_specs=[hbm, hbm, vmem, smem, hbm, vmem, vmem],
        out_specs=[vmem, vmem],
        scratch_shapes=[
            pltpu.VMEM((bands, gs), BF16),
            pltpu.VMEM((K, 4, gs), BF16),
            pltpu.VMEM((HID, SPECIES, K * K), F32),
            pltpu.VMEM((8, PAIR, bands), F32),
            pltpu.VMEM((8, PAIR, bands), BF16),
            pltpu.VMEM((8, 3, PAIR, 128), BF16),
            pltpu.VMEM((8, PAIR, 128), BF16),
            pltpu.VMEM((8, PAIR, 128), BF16),
            pltpu.VMEM((16 * SLOT, bands), BF16),
            pltpu.VMEM((SPECIES, K * K, HID), F32),
            pltpu.VMEM((2, 32, 128), F32),
            pltpu.VMEM((32, 128), F32),
            pltpu.VMEM((8, 32, 128), F32),
            pltpu.VMEM((32, 128), F32),
            pltpu.VMEM((16, 32, 128), F32),
            pltpu.VMEM((16 * SLOT, bands), BF16),
            pltpu.VMEM((SLOT, 128), F32),
            pltpu.VMEM((16, SLOT, 128), F32),
            dma((3,)), dma((POOL,)), dma((NT,)), dma((16,)), dma((NP,)), dma((NP,)), dma((NP, 3)), dma((8,)), dma((16,)),
        ],
        compiler_params=pltpu.CompilerParams(
            collective_id=0, has_side_effects=True, vmem_limit_bytes=44 * 2**20
        ),
        name="step",
    )(wave_coef, jnp.transpose(projector, (1, 0, 2)), occupation.reshape(1, bands), species,
      jnp.transpose(layer_in, (2, 0, 1)), bias_in.reshape(-1, 1, HID), layer_out.reshape(-1, 1, HID))
    return pl.pallas_call(
        correct_kernel,
        out_shape=jax.ShapeDtypeStruct((bands, gs), BF16),
        in_specs=[vmem, vmem],
        out_specs=pl.BlockSpec(memory_space=pl.ANY),
        scratch_shapes=[pltpu.VMEM((bands, gs), BF16), dma((gs // 512,))],
        compiler_params=pltpu.CompilerParams(vmem_limit_bytes=16 * 2**20),
        name="correct",
    )(applied, table)


def solution(mesh):
    in_specs = (P("band", "ga"), P("band", None, "ga"), P("band"), P(), P(), P(), P())
    out_specs = P("band", "ga")
    return jax.shard_map(body, mesh=mesh, in_specs=in_specs, out_specs=out_specs, check_vma=False)
```

```python
import functools
import math

import jax
import jax.numpy as jnp
from jax import lax
from jax.experimental import pallas as pl
from jax.experimental.pallas import tpu as pltpu
from jax.sharding import PartitionSpec as P

MESH = pl.DeviceIdType.MESH
F32 = jnp.float32
BF16 = jnp.bfloat16

K = 27
KP = 28
SLOT = 4 * KP
PAIR = 2 * SLOT
HID = 100
SPECIES = 4

ORDER = ((0, 0), (0, 3), (0, 1), (1, 0), (1, 3), (1, 1), (0, 2), (1, 2))

SPANS = ((0, 32), (192, 32), (32, 48), (144, 48), (80, 64))
CUTS = {0: "E", 3: "E", 6: "XL", 7: "XEL"}
SIZES = {"E": (224,), "EL": (160, 64), "XL": (64, 160), "XEL": (64, 96, 64)}
PIECES = []
PART = {}
for _i in range(8):
    _cut = CUTS.get(_i, "EL")
    _row = 0
    for _name, _size in zip(_cut, SIZES[_cut]):
        PART[str(_i) + _name] = len(PIECES)
        PIECES.append((_i, _row, _size))
        _row += _size
NP = len(PIECES)
POOL = 64

TREE = (
    ("z10", 32, 80), ("x10", 0, 32),
    ("z03a", 32, 48), ("z03b", 80, 32), ("x03", 0, 32), ("z01a", 32, 48), ("z01b", 80, 32), ("x01", 0, 32),
    ("x02a", 0, 16), ("x02b", 16, 16), ("z02a", 32, 48), ("z02b", 80, 32),
    ("z13a", 32, 48), ("z13b", 80, 32), ("z11a", 32, 48), ("z11b", 80, 32), ("x13", 0, 32), ("x11", 0, 32),
    ("x12a", 0, 16), ("x12b", 16, 16), ("z12a", 64, 16), ("z12b", 32, 32),
    ("z12c", 80, 16), ("z12d", 96, 16),
)
TREE_ID = {name: i for i, (name, _, _) in enumerate(TREE)}
NT = len(TREE)


def body_kernel(bands_all, w_hbm, p_hbm, occ_ref, species_ref, lin_hbm, bias_ref, lout_ref, app, tab,
                w, wt, pin, lraw, part, part16, ry, zs, zr, cfull, lin, dsend, dpart, drecv, xs, xall, appt, bd, bds,
                lsem, pool, tsr, d2r, ryr, zsr, agr, dens_r, xsr):
    band = lax.axis_index("band")
    ga = lax.axis_index("ga")
    zh, x, c = band // 8, (band // 2) % 4, band % 2
    y, zl = ga // 2, ga % 2

    def at(dz=0, dx=0, dc=0, dy=0, dl=0):
        nzh, nx, nc = (zh + dz) % 2, (x + dx) % 4, (c + dc) % 2
        ny, nzl = (y + dy) % 4, (zl + dl) % 2
        return (nzh * 8 + nx * 2 + nc, ny * 2 + nzl)

    def slot_row(dz, dx, dc):
        nzh, nx, nc = (zh + dz) % 2, (x + dx) % 4, (c + dc) % 2
        return (nzh * 8 + nx * 2 + nc) * SLOT

    def pair_row(dz, dx):
        return (((zh + dz) % 2) * 4 + (x + dx) % 4) * PAIR

    def row_in_slot(first, count, dc=0):
        return jnp.where((c + dc) % 2 == 0, first, SLOT - first - count)

    def rows(ref, start, count):
        return ref.at[pl.ds(pl.multiple_of(start, 16), count)]

    wcopy = pltpu.make_async_copy(w_hbm, w, lsem.at[0])
    own_row = slot_row(0, 0, 0)
    pcopy = pltpu.make_async_copy(p_hbm, pin, lsem.at[1])
    lcopy = pltpu.make_async_copy(lin_hbm, lraw, lsem.at[2])
    pcopy.start()
    wcopy.start()
    lcopy.start()

    barrier = pltpu.get_barrier_semaphore()
    partners = [at(dc=1)]
    for dz in range(2):
        for dx in range(4):
            if dz or dx:
                partners.append(at(dz=dz, dx=dx))
    for dy in range(4):
        for dl in range(2):
            if dy or dl:
                partners.append(at(dy=dy, dl=dl))
                partners.append(at(dy=dy, dl=dl, dc=1))
    for partner in partners:
        pl.semaphore_signal(barrier, inc=1, device_id=partner, device_id_type=MESH)
    pcopy.wait()

    def pack(t, carry):
        cols = pl.ds(pl.multiple_of(t * 512, 512), 512)
        flat = pin[:, :, cols].astype(F32).reshape(4 * K, 512)
        full = jnp.concatenate([flat, jnp.zeros((SLOT - 4 * K, 512), F32)], axis=0)
        tab[pl.ds(pl.multiple_of(own_row, 16), SLOT), cols] = full.astype(BF16)
        return carry

    lax.fori_loop(0, 8, pack, 0)
    pl.semaphore_wait(barrier, len(partners))

    sends = []

    def remote(src, dst, rs, device):
        n = len(sends)
        if n >= POOL:
            sends[n - POOL].wait_send()
        copy = pltpu.make_async_remote_copy(
            src_ref=src, dst_ref=dst, send_sem=pool.at[n % POOL], recv_sem=rs, device_id=device, device_id_type=MESH
        )
        copy.start()
        sends.append(copy)

    def arrived(dst, rs):
        pltpu.make_async_remote_copy(
            src_ref=dst, dst_ref=dst, send_sem=pool.at[0], recv_sem=rs, device_id=at(dc=1), device_id_type=MESH
        ).wait_recv()

    def tree_send(name, dz, dx, device):
        i = TREE_ID[name]
        _, first, count = TREE[i]
        ref = rows(tab, slot_row(dz, dx, 0) + row_in_slot(first, count), count)
        remote(ref, ref, tsr.at[i], device)

    def tree_wait(name, dz, dx):
        i = TREE_ID[name]
        _, first, count = TREE[i]
        arrived(rows(tab, slot_row(dz, dx, 0) + row_in_slot(first, count), count), tsr.at[i])

    crossings = {}

    def crossing(i, part):
        first, count = ((0, SLOT), (0, 80), (80, 32), (0, 32), (32, 80), (32, 48))[part]
        return ORDER[i], first, count, crossings.setdefault((i, part), len(crossings))

    def across(i, part=0):
        (dz, dx), first, count, sem = crossing(i, part)
        ref = rows(tab, slot_row(dz, dx, 0) + row_in_slot(first, count), count)
        remote(ref, ref, d2r.at[sem], at(dc=1))

    def across_wait(i, part=0):
        (dz, dx), first, count, sem = crossing(i, part)
        arrived(rows(tab, slot_row(dz, dx, 1) + row_in_slot(first, count, 1), count), d2r.at[sem])

    right, left, over = at(dx=1), at(dx=3), at(dz=1)

    def project(s):
        i, first, count = PIECES[s]
        base = pair_row(*ORDER[i])

        def read(start, size):
            return tab[pl.ds(pl.multiple_of(base + start, 16), size), :]

        def half(t, carry):
            cols = pl.ds(pl.multiple_of(t * 256, 256), 256)

            def times(table):
                if i == 0:
                    dims, by = (((1,), (1,)), ((), ())), w[cols, :]
                else:
                    dims, by = (((1,), (0,)), ((), ())), wt[:, cols]
                return lax.dot_general(table, by, dims, preferred_element_type=F32)

            def keep(to, got):
                part[i, to:to + got.shape[0], cols] = got
                part16[i, to:to + got.shape[0], cols] = got.astype(BF16)

            spans = []
            to = 0
            for span in SPANS:
                if first <= to < first + count:
                    spans.append(span)
                to += span[1]
            if count == PAIR:
                got = times(read(0, PAIR))
                to = 0
                for start, size in spans:
                    keep(to, got[start:start + size])
                    to += size
            else:
                table = [read(*span) for span in spans]
                keep(first, times(table[0] if len(table) == 1 else jnp.concatenate(table, axis=0)))
            return carry

        lax.fori_loop(0, 2, half, 0)
        here = pl.ds(first, count)
        for dy in (2, 1, 3):
            lanes = pl.ds(pl.multiple_of(((y + dy) % 4) * 128, 128), 128)
            remote(part16.at[i, here, lanes], ry.at[i, 3 - dy, here], ryr.at[s], at(dy=dy))

    mine = pl.ds(pl.multiple_of(y * 128, 128), 128)

    def reduce_y(s):
        i, first, count = PIECES[s]
        here = pl.ds(first, count)
        total = part[i, here, mine]
        arrived(ry.at[i, :, here], ryr.at[s])
        for j in range(3):
            total = total + ry[i, j, here].astype(F32)
        part[i, here, mine] = total
        zs[i, here] = total.astype(BF16)
        remote(zs.at[i, here], zr.at[i, here], zsr.at[s], at(dl=1))

    def direct(s):
        return PIECES[s][0] == 7

    def block_at(s, dy):
        i, first, count = PIECES[s]
        lanes = pl.ds(pl.multiple_of(((y + dy) % 4) * 128, 128), 128)
        return pl.ds(pl.multiple_of(pair_row(*ORDER[i]) + first, 16), count), lanes

    def block(s, dy):
        return cfull.at[block_at(s, dy)]

    def reduce_z(s):
        i, first, count = PIECES[s]
        here = pl.ds(first, count)
        arrived(zr.at[i, here], zsr.at[s])
        cfull[block_at(s, 0)] = (part[i, here, mine] + zr[i, here].astype(F32)).astype(BF16)
        for dy in (2, 1, 3) if direct(s) else (1, 3):
            remote(block(s, 0), block(s, 0), agr.at[s, 3 - dy], at(dy=dy))

    def relay(s):
        for dy in (1, 3):
            arrived(block(s, dy), agr.at[s, dy - 1])
        dy = 1 + 2 * (s % 2)
        remote(block(s, dy), block(s, dy), agr.at[s, 1], at(dy=4 - dy))

    def gathered(s):
        for dy in (1, 2, 3) if direct(s) else (2,):
            arrived(block(s, dy), agr.at[s, dy - 1])

    def coef_of(pair, h):
        cuts = ((0, 32), (64, 48), (160, 32)) if h == 0 else ((192, 32), (112, 48), (32, 32))
        return jnp.concatenate([cfull[pl.ds(pl.multiple_of(pair * PAIR + a, 16), n), :] for a, n in cuts], axis=0)

    tree_send("z10", 0, 0, over)
    tree_send("x03", 0, 0, right)
    tree_send("x01", 0, 0, left)
    across(0, 0)
    tree_send("z03a", 0, 0, right)
    tree_send("z01a", 0, 0, left)
    tree_send("z03b", 0, 0, right)
    tree_send("z01b", 0, 0, left)
    wcopy.wait()
    across_wait(0, 0)
    project(PART["0E"])
    tree_wait("x03", 0, 3)
    tree_send("x02a", 0, 3, right)
    tree_wait("x01", 0, 1)
    tree_send("x02b", 0, 1, left)
    reduce_y(PART["0E"])
    tree_send("x10", 0, 0, over)
    tree_send("x13", 0, 3, over)
    tree_send("x11", 0, 1, over)

    def turn_wave(t, carry):
        block = pl.ds(pl.multiple_of(t * 256, 256), 256)
        wt[block, :] = w[:, block].T
        return carry

    lax.fori_loop(0, w.shape[1] // 256, turn_wave, 0)
    lcopy.wait()
    for kind in range(SPECIES):
        turned = lraw[:, kind, :].T
        for k in range(K):
            lin[kind, k, 0:K, :] = turned[k * K:(k + 1) * K, :]
    tree_wait("z03a", 0, 3)
    across(1, 1)
    tree_wait("z01a", 0, 1)
    across(2, 1)
    tree_wait("z10", 1, 0)
    tree_send("z13a", 1, 0, right)
    tree_send("z11a", 1, 0, left)
    tree_send("z13b", 1, 0, right)
    tree_send("z11b", 1, 0, left)
    tree_send("z02a", 0, 3, right)
    reduce_z(PART["0E"])
    across_wait(1, 1)
    project(PART["1E"])
    across_wait(2, 1)
    project(PART["2E"])
    tree_wait("z03b", 0, 3)
    across(1, 2)
    tree_wait("z01b", 0, 1)
    tree_send("z02b", 0, 1, left)
    across(2, 2)
    tree_wait("x10", 1, 0)
    across(3, 0)
    across_wait(1, 2)
    project(PART["1L"])
    relay(PART["0E"])
    reduce_y(PART["1E"])
    across_wait(2, 2)
    project(PART["2L"])
    reduce_y(PART["2E"])
    across_wait(3, 0)
    project(PART["3E"])
    tree_wait("x02a", 0, 2)
    tree_wait("x02b", 0, 2)
    across(6, 3)
    reduce_y(PART["1L"])
    reduce_y(PART["2L"])
    tree_send("x12a", 0, 2, over)
    tree_send("x12b", 0, 2, over)
    across_wait(6, 3)
    project(PART["6X"])
    tree_wait("z13a", 1, 3)
    tree_send("z12a", 1, 3, right)
    tree_wait("z11a", 1, 1)
    tree_send("z12b", 1, 1, left)
    tree_wait("x13", 1, 3)
    across(4, 1)
    tree_wait("x11", 1, 1)
    across(5, 1)
    reduce_y(PART["3E"])
    across_wait(4, 1)
    project(PART["4E"])
    across_wait(5, 1)
    project(PART["5E"])
    reduce_z(PART["1E"])
    reduce_z(PART["2E"])
    tree_wait("z13b", 1, 3)
    tree_send("z12c", 1, 3, right)
    across(4, 2)
    tree_wait("z11b", 1, 1)
    tree_send("z12d", 1, 1, left)
    across(5, 2)
    reduce_z(PART["1L"])
    reduce_z(PART["2L"])
    reduce_y(PART["6X"])
    across_wait(4, 2)
    project(PART["4L"])
    reduce_y(PART["4E"])
    across_wait(5, 2)
    project(PART["5L"])
    reduce_z(PART["3E"])
    reduce_z(PART["6X"])
    relay(PART["1E"])
    relay(PART["2E"])
    tree_wait("x12a", 1, 2)
    tree_wait("x12b", 1, 2)
    across(7, 3)
    reduce_y(PART["5E"])
    reduce_z(PART["4E"])
    tree_wait("z02a", 0, 2)
    tree_wait("z02b", 0, 2)
    across(6, 4)
    across_wait(7, 3)
    project(PART["7X"])
    reduce_y(PART["4L"])
    reduce_y(PART["5L"])
    relay(PART["1L"])
    relay(PART["2L"])
    reduce_z(PART["5E"])
    across_wait(6, 4)
    project(PART["6L"])
    tree_wait("z12a", 1, 2)
    tree_wait("z12b", 1, 2)
    across(7, 5)
    reduce_z(PART["4L"])
    reduce_z(PART["5L"])
    across_wait(7, 5)
    project(PART["7E"])
    relay(PART["3E"])
    relay(PART["6X"])
    reduce_y(PART["7X"])
    tree_wait("z12c", 1, 2)
    tree_wait("z12d", 1, 2)
    across(7, 2)
    relay(PART["4E"])
    relay(PART["5E"])
    across_wait(7, 2)
    project(PART["7L"])
    reduce_y(PART["6L"])
    reduce_z(PART["7X"])
    reduce_y(PART["7E"])
    reduce_y(PART["7L"])
    reduce_z(PART["6L"])
    reduce_z(PART["7E"])
    reduce_z(PART["7L"])
    relay(PART["4L"])
    relay(PART["5L"])
    relay(PART["6L"])
    for s in range(NP):
        gathered(s)

    lane_atom = lax.broadcasted_iota(jnp.int32, (KP, SLOT), 1) % 4
    occ = occ_ref[...]
    for h in range(2):
        coef = coef_of(ga, h)
        weighted = coef.astype(F32) * occ
        high = weighted.astype(BF16)
        low = (weighted - high.astype(F32)).astype(BF16)
        dims = (((1,), (1,)), ((), ()))
        gram = lax.dot_general(high, coef, dims, preferred_element_type=F32) + lax.dot_general(
            low, coef, dims, preferred_element_type=F32
        )
        bd[:, 0:SLOT] = gram
        packed = jnp.zeros((KP, SLOT), F32)
        for a in range(4):
            packed = packed + jnp.where(lane_atom == a, bd[pl.ds(a, KP, stride=4), :][:, 0:SLOT], 0.0)
        dsend[h, 0:KP, 0:SLOT] = packed
    remote(dsend.at[1 - c], drecv.at[7], dens_r.at[7], at(dc=1))
    arrived(drecv.at[7], dens_r.at[7])
    dpart[...] = dsend[c] + drecv[7]
    for dz in range(2):
        for dx in range(4):
            if dz or dx:
                j = dz * 4 + (4 - dx) % 4 - 1
                remote(dpart, drecv.at[j], dens_r.at[j], at(dz=dz, dx=dx))
    for j in range(7):
        arrived(drecv.at[j], dens_r.at[j])
    density = dpart[...]
    for j in range(7):
        density = density + drecv[j]
    density = density * (1.0 / bands_all)

    lane = lax.broadcasted_iota(jnp.int32, (K, SLOT), 1)
    grad_t = jnp.zeros((K, SLOT), F32)
    slot = 2 * ga + c
    for a in range(4):
        kind = species_ref[4 * slot + a]
        acc = jnp.zeros((K, HID), F32)
        for k in range(K):
            acc = acc + density[0:K, 4 * k + a:4 * k + a + 1] * lin[kind, k, 0:K, :]
        preact = jnp.sum(acc, axis=0, keepdims=True) + bias_ref[kind]
        act = jnp.tanh(preact)
        slope = lout_ref[kind] * (1.0 - act * act)
        for k in range(K):
            column = jnp.sum(lin[kind, k, 0:K, :] * slope, axis=1, keepdims=True)
            grad_t = jnp.where(lane == 4 * k + a, column, grad_t)
    bd[...] = jnp.zeros((SLOT, 128), F32)
    pad = jnp.zeros((K, 128 - SLOT), F32)
    for a in range(4):
        bd[pl.ds(a, K, stride=4), :] = jnp.concatenate([jnp.where(lane % 4 == a, grad_t, 0.0), pad], axis=1)
    square = bd[:, 0:SLOT]
    bd[:, 0:SLOT] = square + square.T
    packed = jnp.zeros((KP, 128), F32)
    for a in range(4):
        packed = packed + bd[pl.ds(a, KP, stride=4), :]
    xs[0:KP, :] = packed
    xall[slot] = xs[...]
    for dy in range(4):
        for dl in range(2):
            for dc in range(2):
                if dy or dl or dc:
                    j = (((4 - dy) % 4) * 2 + dl) * 2 + dc
                    remote(xs, xall.at[slot], xsr.at[j], at(dy=dy, dl=dl, dc=dc))
    for dy in range(4):
        for dl in range(2):
            for dc in range(2):
                if dy or dl or dc:
                    j = (dy * 2 + dl) * 2 + dc
                    from_slot = 2 * (((y + dy) % 4) * 2 + (zl + dl) % 2) + (c + dc) % 2
                    arrived(xall.at[from_slot], xsr.at[j])

    factor = 1.0 / math.sqrt(64 * K)
    rows4 = lax.broadcasted_iota(jnp.int32, (SLOT, SLOT), 0) % 4
    lanes4 = lax.broadcasted_iota(jnp.int32, (SLOT, SLOT), 1) % 4
    same = rows4 == lanes4

    def apply(pair, carry):
        for h in range(2):
            j = 2 * pair + h
            for a in range(4):
                bds[j, pl.ds(a, KP, stride=4), :] = xall[j, 0:KP, :]
            full = jnp.where(same, bds[j, :, 0:SLOT], 0.0)
            high = full.astype(BF16)
            low = (full - high.astype(F32)).astype(BF16)
            coef = coef_of(pair, h)
            got = jnp.dot(high, coef, preferred_element_type=F32) + jnp.dot(low, coef, preferred_element_type=F32)
            appt[pl.ds(pl.multiple_of(j * SLOT, 16), SLOT), :] = (got * factor).astype(BF16)
        return carry

    lax.fori_loop(0, 8, apply, 0, unroll=2)

    def turn(j, carry):
        block = pl.ds(pl.multiple_of(j * 256, 256), 256)
        app[:, block] = appt[block, :].T
        return carry

    lax.fori_loop(0, 7, turn, 0)
    for copy in sends[-POOL:]:
        copy.wait_send()


def correct_kernel(app, tab, out_hbm, out, sems):
    def store(t):
        cols = pl.ds(pl.multiple_of(t * 1024, 1024), 1024)
        return pltpu.make_async_copy(out.at[:, cols], out_hbm.at[:, cols], sems.at[t])

    def one(t, carry):
        cols = pl.ds(pl.multiple_of(t * 1024, 1024), 1024)
        out[:, cols] = jnp.dot(app[...], tab[:, cols], preferred_element_type=F32).astype(BF16)
        store(t).start()
        return carry

    steps = out.shape[1] // 1024
    lax.fori_loop(0, steps, one, 0)
    for t in range(steps):
        store(t).wait()


def body(wave_coef, projector, occupation, species, layer_in, bias_in, layer_out):
    atoms_here, orbitals, gs = projector.shape
    bands = wave_coef.shape[0]
    bands_all = bands * lax.axis_size("band")
    assert atoms_here == 4 and orbitals == K and bands == 512
    hbm = pl.BlockSpec(memory_space=pltpu.HBM)
    vmem = pl.BlockSpec(memory_space=pltpu.VMEM)
    smem = pl.BlockSpec(memory_space=pltpu.SMEM)
    dma = pltpu.SemaphoreType.DMA
    applied, table = pl.pallas_call(
        functools.partial(body_kernel, bands_all),
        out_shape=[pltpu.VMEM((bands, 16 * SLOT), BF16), pltpu.VMEM((16 * SLOT, gs), BF16)],
        in_specs=[hbm, hbm, vmem, smem, hbm, vmem, vmem],
        out_specs=[vmem, vmem],
        scratch_shapes=[
            pltpu.VMEM((bands, gs), BF16),
            pltpu.VMEM((gs, bands), BF16),
            pltpu.VMEM((K, 4, gs), BF16),
            pltpu.VMEM((HID, SPECIES, K * K), F32),
            pltpu.VMEM((8, PAIR, bands), F32),
            pltpu.VMEM((8, PAIR, bands), BF16),
            pltpu.VMEM((8, 3, PAIR, 128), BF16),
            pltpu.VMEM((8, PAIR, 128), BF16),
            pltpu.VMEM((8, PAIR, 128), BF16),
            pltpu.VMEM((16 * SLOT, bands), BF16),
            pltpu.VMEM((SPECIES, K, 32, HID), F32),
            pltpu.VMEM((2, 32, 128), F32),
            pltpu.VMEM((32, 128), F32),
            pltpu.VMEM((8, 32, 128), F32),
            pltpu.VMEM((32, 128), F32),
            pltpu.VMEM((16, 32, 128), F32),
            pltpu.VMEM((16 * SLOT, bands), BF16),
            pltpu.VMEM((SLOT, 128), F32),
            pltpu.VMEM((16, SLOT, 128), F32),
            dma((3,)), dma((POOL,)), dma((NT,)), dma((16,)), dma((NP,)), dma((NP,)), dma((NP, 3)), dma((8,)), dma((16,)),
        ],
        compiler_params=pltpu.CompilerParams(
            collective_id=0, has_side_effects=True, vmem_limit_bytes=44 * 2**20
        ),
        name="step",
    )(wave_coef, jnp.transpose(projector, (1, 0, 2)), occupation.reshape(1, bands), species,
      jnp.transpose(layer_in, (2, 0, 1)), bias_in.reshape(-1, 1, HID), layer_out.reshape(-1, 1, HID))
    return pl.pallas_call(
        correct_kernel,
        out_shape=jax.ShapeDtypeStruct((bands, gs), BF16),
        in_specs=[vmem, vmem],
        out_specs=pl.BlockSpec(memory_space=pl.ANY),
        scratch_shapes=[pltpu.VMEM((bands, gs), BF16), dma((gs // 1024,))],
        compiler_params=pltpu.CompilerParams(vmem_limit_bytes=16 * 2**20),
        name="correct",
    )(applied, table)


def solution(mesh):
    in_specs = (P("band", "ga"), P("band", None, "ga"), P("band"), P(), P(), P(), P())
    out_specs = P("band", "ga")
    return jax.shard_map(body, mesh=mesh, in_specs=in_specs, out_specs=out_specs, check_vma=False)
```

```python
import functools
import math

import jax
import jax.numpy as jnp
from jax import lax
from jax.experimental import pallas as pl
from jax.experimental.pallas import tpu as pltpu
from jax.sharding import PartitionSpec as P

MESH = pl.DeviceIdType.MESH
F32 = jnp.float32
BF16 = jnp.bfloat16

K = 27
KP = 28
SLOT = 4 * KP
PAIR = 2 * SLOT
HID = 100
SPECIES = 4

ORDER = ((0, 0), (0, 3), (0, 1), (1, 0), (1, 3), (1, 1), (0, 2), (1, 2))

SPANS = ((0, 32), (192, 32), (32, 48), (144, 48), (80, 64))
CUTS = {0: "E", 3: "E", 6: "XL", 7: "XEL"}
SIZES = {"E": (224,), "EL": (160, 64), "XL": (64, 160), "XEL": (64, 96, 64)}
PIECES = []
PART = {}
for _i in range(8):
    _cut = CUTS.get(_i, "EL")
    _row = 0
    for _name, _size in zip(_cut, SIZES[_cut]):
        PART[str(_i) + _name] = len(PIECES)
        PIECES.append((_i, _row, _size))
        _row += _size
NP = len(PIECES)
POOL = 40

TREE = (
    ("z10", 32, 80), ("x10", 0, 32),
    ("z03a", 32, 48), ("z03b", 80, 32), ("x03", 0, 32), ("z01a", 32, 48), ("z01b", 80, 32), ("x01", 0, 32),
    ("x02a", 0, 16), ("x02b", 16, 16), ("z02a", 32, 48), ("z02b", 80, 32),
    ("z13a", 32, 48), ("z13b", 80, 32), ("z11a", 32, 48), ("z11b", 80, 32), ("x13", 0, 32), ("x11", 0, 32),
    ("x12a", 0, 16), ("x12b", 16, 16), ("z12a", 64, 16), ("z12b", 32, 32),
    ("z12c", 80, 16), ("z12d", 96, 16),
)
TREE_ID = {name: i for i, (name, _, _) in enumerate(TREE)}
NT = len(TREE)


def body_kernel(bands_all, w_hbm, p_hbm, occ_ref, species_ref, lin_hbm, bias_ref, lout_ref, app, tab,
                w, wt, pin, lraw, part, part16, ry, zs, zr, cfull, lin, dsend, dpart, drecv, xs, xall, appt, bd, bds,
                lsem, pool, tss, tsr, d2r, ryr, zsr, agr, dens_r, xsr, rounds):
    band = lax.axis_index("band")
    ga = lax.axis_index("ga")
    zh, x, c = band // 8, (band // 2) % 4, band % 2
    y, zl = ga // 2, ga % 2

    def at(dz=0, dx=0, dc=0, dy=0, dl=0):
        nzh, nx, nc = (zh + dz) % 2, (x + dx) % 4, (c + dc) % 2
        ny, nzl = (y + dy) % 4, (zl + dl) % 2
        return (nzh * 8 + nx * 2 + nc, ny * 2 + nzl)

    def slot_row(dz, dx, dc):
        nzh, nx, nc = (zh + dz) % 2, (x + dx) % 4, (c + dc) % 2
        return (nzh * 8 + nx * 2 + nc) * SLOT

    def pair_row(dz, dx):
        return (((zh + dz) % 2) * 4 + (x + dx) % 4) * PAIR

    def row_in_slot(first, count, dc=0):
        return jnp.where((c + dc) % 2 == 0, first, SLOT - first - count)

    def rows(ref, start, count):
        return ref.at[pl.ds(pl.multiple_of(start, 16), count)]

    wcopy = pltpu.make_async_copy(w_hbm, w, lsem.at[0])
    own_row = slot_row(0, 0, 0)
    pcopy = pltpu.make_async_copy(p_hbm, pin, lsem.at[1])
    lcopy = pltpu.make_async_copy(lin_hbm, lraw, lsem.at[2])
    pcopy.start()
    wcopy.start()
    lcopy.start()

    barrier = pltpu.get_barrier_semaphore()
    near = [at(dc=1), at(dx=1), at(dx=3), at(dz=1), at(dy=1), at(dy=3), at(dl=1)]
    for partner in near:
        pl.semaphore_signal(barrier, inc=1, device_id=partner, device_id_type=MESH)
    pcopy.wait()

    def pack(t, carry):
        cols = pl.ds(pl.multiple_of(t * 512, 512), 512)
        flat = pin[:, :, cols].astype(F32).reshape(4 * K, 512)
        full = jnp.concatenate([flat, jnp.zeros((SLOT - 4 * K, 512), F32)], axis=0)
        tab[pl.ds(pl.multiple_of(own_row, 16), SLOT), cols] = full.astype(BF16)
        return carry

    lax.fori_loop(0, 8, pack, 0)
    pl.semaphore_wait(barrier, len(near))

    def tell(r):
        for partner in near:
            pl.semaphore_signal(rounds.at[r], inc=1, device_id=partner, device_id_type=MESH)

    def known(r):
        pl.semaphore_wait(rounds.at[r], len(near))
        if r < 2:
            tell(r + 1)


    sends = []

    pooled = []

    def remote(src, dst, rs, device, own=None):
        n = len(pooled)
        if own is None:
            if n >= POOL:
                pooled[n - POOL].wait_send()
            own = pool.at[n % POOL]
            keep = pooled
        else:
            keep = sends
        copy = pltpu.make_async_remote_copy(
            src_ref=src, dst_ref=dst, send_sem=own, recv_sem=rs, device_id=device, device_id_type=MESH
        )
        copy.start()
        keep.append(copy)

    def arrived(dst, rs):
        pltpu.make_async_remote_copy(
            src_ref=dst, dst_ref=dst, send_sem=pool.at[0], recv_sem=rs, device_id=at(dc=1), device_id_type=MESH
        ).wait_recv()

    def tree_send(name, dz, dx, device):
        i = TREE_ID[name]
        _, first, count = TREE[i]
        ref = rows(tab, slot_row(dz, dx, 0) + row_in_slot(first, count), count)
        remote(ref, ref, tsr.at[i], device, tss.at[i])

    def tree_wait(name, dz, dx):
        i = TREE_ID[name]
        _, first, count = TREE[i]
        arrived(rows(tab, slot_row(dz, dx, 0) + row_in_slot(first, count), count), tsr.at[i])

    crossings = {}

    def crossing(i, part):
        first, count = ((0, SLOT), (0, 80), (80, 32), (0, 32), (32, 80), (32, 48))[part]
        return ORDER[i], first, count, crossings.setdefault((i, part), len(crossings))

    def across(i, part=0):
        (dz, dx), first, count, sem = crossing(i, part)
        ref = rows(tab, slot_row(dz, dx, 0) + row_in_slot(first, count), count)
        remote(ref, ref, d2r.at[sem], at(dc=1))

    def across_wait(i, part=0):
        (dz, dx), first, count, sem = crossing(i, part)
        arrived(rows(tab, slot_row(dz, dx, 1) + row_in_slot(first, count, 1), count), d2r.at[sem])

    right, left, over = at(dx=1), at(dx=3), at(dz=1)

    def project(s):
        i, first, count = PIECES[s]
        base = pair_row(*ORDER[i])

        def read(start, size):
            return tab[pl.ds(pl.multiple_of(base + start, 16), size), :]

        def half(t, carry):
            cols = pl.ds(pl.multiple_of(t * 256, 256), 256)

            def times(table):
                if i == 0:
                    dims, by = (((1,), (1,)), ((), ())), w[cols, :]
                else:
                    dims, by = (((1,), (0,)), ((), ())), wt[:, cols]
                return lax.dot_general(table, by, dims, preferred_element_type=F32)

            def keep(to, got):
                part[i, to:to + got.shape[0], cols] = got
                part16[i, to:to + got.shape[0], cols] = got.astype(BF16)

            spans = []
            to = 0
            for span in SPANS:
                if first <= to < first + count:
                    spans.append(span)
                to += span[1]
            if count == PAIR:
                got = times(read(0, PAIR))
                to = 0
                for start, size in spans:
                    keep(to, got[start:start + size])
                    to += size
            else:
                table = [read(*span) for span in spans]
                keep(first, times(table[0] if len(table) == 1 else jnp.concatenate(table, axis=0)))
            return carry

        lax.fori_loop(0, 2, half, 0)
        here = pl.ds(first, count)
        for dy in (2, 1, 3):
            lanes = pl.ds(pl.multiple_of(((y + dy) % 4) * 128, 128), 128)
            remote(part16.at[i, here, lanes], ry.at[i, 3 - dy, here], ryr.at[s], at(dy=dy))

    mine = pl.ds(pl.multiple_of(y * 128, 128), 128)

    def reduce_y(s):
        i, first, count = PIECES[s]
        here = pl.ds(first, count)
        total = part[i, here, mine]
        arrived(ry.at[i, :, here], ryr.at[s])
        for j in range(3):
            total = total + ry[i, j, here].astype(F32)
        part[i, here, mine] = total
        zs[i, here] = total.astype(BF16)
        remote(zs.at[i, here], zr.at[i, here], zsr.at[s], at(dl=1))

    def direct(s):
        return PIECES[s][0] == 7

    def block_at(s, dy):
        i, first, count = PIECES[s]
        lanes = pl.ds(pl.multiple_of(((y + dy) % 4) * 128, 128), 128)
        return pl.ds(pl.multiple_of(pair_row(*ORDER[i]) + first, 16), count), lanes

    def block(s, dy):
        return cfull.at[block_at(s, dy)]

    def reduce_z(s):
        i, first, count = PIECES[s]
        here = pl.ds(first, count)
        arrived(zr.at[i, here], zsr.at[s])
        cfull[block_at(s, 0)] = (part[i, here, mine] + zr[i, here].astype(F32)).astype(BF16)
        for dy in (2, 1, 3) if direct(s) else (1, 3):
            remote(block(s, 0), block(s, 0), agr.at[s, 3 - dy], at(dy=dy))

    def relay(s):
        for dy in (1, 3):
            arrived(block(s, dy), agr.at[s, dy - 1])
        dy = 1 + 2 * (s % 2)
        remote(block(s, dy), block(s, dy), agr.at[s, 1], at(dy=4 - dy))

    def gathered(s):
        for dy in (1, 2, 3) if direct(s) else (2,):
            arrived(block(s, dy), agr.at[s, dy - 1])

    def coef_of(pair, h):
        cuts = ((0, 32), (64, 48), (160, 32)) if h == 0 else ((192, 32), (112, 48), (32, 32))
        return jnp.concatenate([cfull[pl.ds(pl.multiple_of(pair * PAIR + a, 16), n), :] for a, n in cuts], axis=0)

    tell(0)
    tree_send("z10", 0, 0, over)
    tree_send("x03", 0, 0, right)
    tree_send("x01", 0, 0, left)
    across(0, 0)
    tree_send("z03a", 0, 0, right)
    tree_send("z01a", 0, 0, left)
    tree_send("z03b", 0, 0, right)
    tree_send("z01b", 0, 0, left)
    wcopy.wait()
    known(0)
    across_wait(0, 0)
    project(PART["0E"])
    tree_wait("x03", 0, 3)
    tree_send("x02a", 0, 3, right)
    tree_wait("x01", 0, 1)
    tree_send("x02b", 0, 1, left)
    reduce_y(PART["0E"])
    known(1)
    tree_send("x10", 0, 0, over)
    tree_send("x13", 0, 3, over)
    tree_send("x11", 0, 1, over)

    def turn_wave(t, carry):
        block = pl.ds(pl.multiple_of(t * 256, 256), 256)
        wt[block, :] = w[:, block].T
        return carry

    lax.fori_loop(0, w.shape[1] // 256, turn_wave, 0)
    lcopy.wait()
    for kind in range(SPECIES):
        turned = lraw[:, kind, :].T
        for k in range(K):
            lin[kind, k, 0:K, :] = turned[k * K:(k + 1) * K, :]
    tree_wait("z03a", 0, 3)
    across(1, 1)
    tree_wait("z01a", 0, 1)
    across(2, 1)
    tree_wait("z10", 1, 0)
    tree_send("z13a", 1, 0, right)
    tree_send("z11a", 1, 0, left)
    tree_send("z13b", 1, 0, right)
    tree_send("z11b", 1, 0, left)
    tree_send("z02a", 0, 3, right)
    reduce_z(PART["0E"])
    across_wait(1, 1)
    project(PART["1E"])
    across_wait(2, 1)
    project(PART["2E"])
    tree_wait("z03b", 0, 3)
    across(1, 2)
    tree_wait("z01b", 0, 1)
    tree_send("z02b", 0, 1, left)
    across(2, 2)
    tree_wait("x10", 1, 0)
    across(3, 0)
    across_wait(1, 2)
    project(PART["1L"])
    relay(PART["0E"])
    known(2)
    reduce_y(PART["1E"])
    across_wait(2, 2)
    project(PART["2L"])
    reduce_y(PART["2E"])
    across_wait(3, 0)
    project(PART["3E"])
    tree_wait("x02a", 0, 2)
    tree_wait("x02b", 0, 2)
    across(6, 3)
    reduce_y(PART["1L"])
    reduce_y(PART["2L"])
    tree_send("x12a", 0, 2, over)
    tree_send("x12b", 0, 2, over)
    across_wait(6, 3)
    project(PART["6X"])
    tree_wait("z13a", 1, 3)
    tree_send("z12a", 1, 3, right)
    tree_wait("z11a", 1, 1)
    tree_send("z12b", 1, 1, left)
    tree_wait("x13", 1, 3)
    across(4, 1)
    tree_wait("x11", 1, 1)
    across(5, 1)
    reduce_y(PART["3E"])
    across_wait(4, 1)
    project(PART["4E"])
    across_wait(5, 1)
    project(PART["5E"])
    reduce_z(PART["1E"])
    reduce_z(PART["2E"])
    tree_wait("z13b", 1, 3)
    tree_send("z12c", 1, 3, right)
    across(4, 2)
    tree_wait("z11b", 1, 1)
    tree_send("z12d", 1, 1, left)
    across(5, 2)
    reduce_z(PART["1L"])
    reduce_z(PART["2L"])
    reduce_y(PART["6X"])
    across_wait(4, 2)
    project(PART["4L"])
    reduce_y(PART["4E"])
    across_wait(5, 2)
    project(PART["5L"])
    reduce_z(PART["3E"])
    reduce_z(PART["6X"])
    relay(PART["1E"])
    relay(PART["2E"])
    tree_wait("x12a", 1, 2)
    tree_wait("x12b", 1, 2)
    across(7, 3)
    reduce_y(PART["5E"])
    reduce_z(PART["4E"])
    tree_wait("z02a", 0, 2)
    tree_wait("z02b", 0, 2)
    across(6, 4)
    across_wait(7, 3)
    project(PART["7X"])
    reduce_y(PART["4L"])
    reduce_y(PART["5L"])
    relay(PART["1L"])
    relay(PART["2L"])
    reduce_z(PART["5E"])
    across_wait(6, 4)
    project(PART["6L"])
    tree_wait("z12a", 1, 2)
    tree_wait("z12b", 1, 2)
    across(7, 5)
    reduce_z(PART["4L"])
    reduce_z(PART["5L"])
    across_wait(7, 5)
    project(PART["7E"])
    tree_wait("z12c", 1, 2)
    tree_wait("z12d", 1, 2)
    across(7, 2)
    relay(PART["3E"])
    relay(PART["6X"])
    reduce_y(PART["7X"])
    relay(PART["4E"])
    relay(PART["5E"])
    across_wait(7, 2)
    project(PART["7L"])
    reduce_y(PART["6L"])
    reduce_z(PART["7X"])
    reduce_y(PART["7E"])
    reduce_y(PART["7L"])
    reduce_z(PART["6L"])
    reduce_z(PART["7E"])
    reduce_z(PART["7L"])
    relay(PART["4L"])
    relay(PART["5L"])
    relay(PART["6L"])
    for s in range(NP):
        gathered(s)

    lane_atom = lax.broadcasted_iota(jnp.int32, (KP, SLOT), 1) % 4
    occ = occ_ref[...]
    for h in range(2):
        coef = coef_of(ga, h)
        weighted = coef.astype(F32) * occ
        high = weighted.astype(BF16)
        low = (weighted - high.astype(F32)).astype(BF16)
        dims = (((1,), (1,)), ((), ()))
        gram = lax.dot_general(high, coef, dims, preferred_element_type=F32) + lax.dot_general(
            low, coef, dims, preferred_element_type=F32
        )
        bd[:, 0:SLOT] = gram
        packed = jnp.zeros((KP, SLOT), F32)
        for a in range(4):
            packed = packed + jnp.where(lane_atom == a, bd[pl.ds(a, KP, stride=4), :][:, 0:SLOT], 0.0)
        dsend[h, 0:KP, 0:SLOT] = packed
    remote(dsend.at[1 - c], drecv.at[7], dens_r.at[1], at(dc=1))
    arrived(drecv.at[7], dens_r.at[1])
    dpart[...] = dsend[c] + drecv[7]
    for dz in range(2):
        for dx in range(4):
            if dz or dx:
                j = dz * 4 + (4 - dx) % 4 - 1
                remote(dpart, drecv.at[j], dens_r.at[0], at(dz=dz, dx=dx))
    arrived(drecv.at[pl.ds(0, 7)], dens_r.at[0])
    density = dpart[...]
    for j in range(7):
        density = density + drecv[j]
    density = density * (1.0 / bands_all)

    lane = lax.broadcasted_iota(jnp.int32, (K, SLOT), 1)
    grad_t = jnp.zeros((K, SLOT), F32)
    slot = 2 * ga + c
    for a in range(4):
        kind = species_ref[4 * slot + a]
        acc = jnp.zeros((K, HID), F32)
        for k in range(K):
            acc = acc + density[0:K, 4 * k + a:4 * k + a + 1] * lin[kind, k, 0:K, :]
        preact = jnp.sum(acc, axis=0, keepdims=True) + bias_ref[kind]
        act = jnp.tanh(preact)
        slope = lout_ref[kind] * (1.0 - act * act)
        for k in range(K):
            column = jnp.sum(lin[kind, k, 0:K, :] * slope, axis=1, keepdims=True)
            grad_t = jnp.where(lane == 4 * k + a, column, grad_t)
    bd[...] = jnp.zeros((SLOT, 128), F32)
    pad = jnp.zeros((K, 128 - SLOT), F32)
    for a in range(4):
        bd[pl.ds(a, K, stride=4), :] = jnp.concatenate([jnp.where(lane % 4 == a, grad_t, 0.0), pad], axis=1)
    square = bd[:, 0:SLOT]
    bd[:, 0:SLOT] = square + square.T
    packed = jnp.zeros((KP, 128), F32)
    for a in range(4):
        packed = packed + bd[pl.ds(a, KP, stride=4), :]
    xs[0:KP, :] = packed
    xall[slot] = xs[...]
    for dy in range(4):
        for dl in range(2):
            for dc in range(2):
                if dy or dl or dc:
                    j = (((4 - dy) % 4) * 2 + dl) * 2 + dc
                    remote(xs, xall.at[slot], xsr.at[j], at(dy=dy, dl=dl, dc=dc))
    for dy in range(4):
        for dl in range(2):
            for dc in range(2):
                if dy or dl or dc:
                    j = (dy * 2 + dl) * 2 + dc
                    from_slot = 2 * (((y + dy) % 4) * 2 + (zl + dl) % 2) + (c + dc) % 2
                    arrived(xall.at[from_slot], xsr.at[j])

    factor = 1.0 / math.sqrt(64 * K)
    rows4 = lax.broadcasted_iota(jnp.int32, (SLOT, SLOT), 0) % 4
    lanes4 = lax.broadcasted_iota(jnp.int32, (SLOT, SLOT), 1) % 4
    same = rows4 == lanes4

    def apply(pair, carry):
        for h in range(2):
            j = 2 * pair + h
            for a in range(4):
                bds[j, pl.ds(a, KP, stride=4), :] = xall[j, 0:KP, :]
            full = jnp.where(same, bds[j, :, 0:SLOT], 0.0)
            high = full.astype(BF16)
            low = (full - high.astype(F32)).astype(BF16)
            coef = coef_of(pair, h)
            got = jnp.dot(high, coef, preferred_element_type=F32) + jnp.dot(low, coef, preferred_element_type=F32)
            appt[pl.ds(pl.multiple_of(j * SLOT, 16), SLOT), :] = (got * factor).astype(BF16)
        return carry

    lax.fori_loop(0, 8, apply, 0, unroll=2)

    def turn(j, carry):
        block = pl.ds(pl.multiple_of(j * 256, 256), 256)
        app[:, block] = appt[block, :].T
        return carry

    lax.fori_loop(0, 7, turn, 0)
    for copy in sends + pooled[-POOL:]:
        copy.wait_send()


def correct_kernel(app, tab, out_hbm, out, sems):
    def store(t):
        cols = pl.ds(pl.multiple_of(t * 1024, 1024), 1024)
        return pltpu.make_async_copy(out.at[:, cols], out_hbm.at[:, cols], sems.at[t])

    def one(t, carry):
        cols = pl.ds(pl.multiple_of(t * 1024, 1024), 1024)
        out[:, cols] = jnp.dot(app[...], tab[:, cols], preferred_element_type=F32).astype(BF16)
        store(t).start()
        return carry

    steps = out.shape[1] // 1024
    lax.fori_loop(0, steps, one, 0)
    for t in range(steps):
        store(t).wait()


def body(wave_coef, projector, occupation, species, layer_in, bias_in, layer_out):
    atoms_here, orbitals, gs = projector.shape
    bands = wave_coef.shape[0]
    bands_all = bands * lax.axis_size("band")
    assert atoms_here == 4 and orbitals == K and bands == 512
    hbm = pl.BlockSpec(memory_space=pltpu.HBM)
    vmem = pl.BlockSpec(memory_space=pltpu.VMEM)
    smem = pl.BlockSpec(memory_space=pltpu.SMEM)
    dma = pltpu.SemaphoreType.DMA
    applied, table = pl.pallas_call(
        functools.partial(body_kernel, bands_all),
        out_shape=[pltpu.VMEM((bands, 16 * SLOT), BF16), pltpu.VMEM((16 * SLOT, gs), BF16)],
        in_specs=[hbm, hbm, vmem, smem, hbm, vmem, vmem],
        out_specs=[vmem, vmem],
        scratch_shapes=[
            pltpu.VMEM((bands, gs), BF16),
            pltpu.VMEM((gs, bands), BF16),
            pltpu.VMEM((K, 4, gs), BF16),
            pltpu.VMEM((HID, SPECIES, K * K), F32),
            pltpu.VMEM((8, PAIR, bands), F32),
            pltpu.VMEM((8, PAIR, bands), BF16),
            pltpu.VMEM((8, 3, PAIR, 128), BF16),
            pltpu.VMEM((8, PAIR, 128), BF16),
            pltpu.VMEM((8, PAIR, 128), BF16),
            pltpu.VMEM((16 * SLOT, bands), BF16),
            pltpu.VMEM((SPECIES, K, 32, HID), F32),
            pltpu.VMEM((2, 32, 128), F32),
            pltpu.VMEM((32, 128), F32),
            pltpu.VMEM((8, 32, 128), F32),
            pltpu.VMEM((32, 128), F32),
            pltpu.VMEM((16, 32, 128), F32),
            pltpu.VMEM((16 * SLOT, bands), BF16),
            pltpu.VMEM((SLOT, 128), F32),
            pltpu.VMEM((16, SLOT, 128), F32),
            dma((3,)), dma((POOL,)), dma((NT,)), dma((NT,)), dma((16,)), dma((NP,)), dma((NP,)), dma((NP, 3)), dma((2,)), dma((16,)), pltpu.SemaphoreType.REGULAR((3,)),
        ],
        compiler_params=pltpu.CompilerParams(
            collective_id=0, has_side_effects=True, vmem_limit_bytes=44 * 2**20
        ),
        name="step",
    )(wave_coef, jnp.transpose(projector, (1, 0, 2)), occupation.reshape(1, bands), species,
      jnp.transpose(layer_in, (2, 0, 1)), bias_in.reshape(-1, 1, HID), layer_out.reshape(-1, 1, HID))
    return pl.pallas_call(
        correct_kernel,
        out_shape=jax.ShapeDtypeStruct((bands, gs), BF16),
        in_specs=[vmem, vmem],
        out_specs=pl.BlockSpec(memory_space=pl.ANY),
        scratch_shapes=[pltpu.VMEM((bands, gs), BF16), dma((gs // 1024,))],
        compiler_params=pltpu.CompilerParams(vmem_limit_bytes=16 * 2**20),
        name="correct",
    )(applied, table)


def solution(mesh):
    in_specs = (P("band", "ga"), P("band", None, "ga"), P("band"), P(), P(), P(), P())
    out_specs = P("band", "ga")
    return jax.shard_map(body, mesh=mesh, in_specs=in_specs, out_specs=out_specs, check_vma=False)
```

```python
import functools
import math

import jax
import jax.numpy as jnp
from jax import lax
from jax.experimental import pallas as pl
from jax.experimental.pallas import tpu as pltpu
from jax.sharding import PartitionSpec as P

MESH = pl.DeviceIdType.MESH
F32 = jnp.float32
BF16 = jnp.bfloat16

K = 27
KP = 28
SLOT = 4 * KP
PAIR = 2 * SLOT
HID = 100
SPECIES = 4

ORDER = ((0, 0), (0, 3), (0, 1), (1, 0), (1, 3), (1, 1), (0, 2), (1, 2))

SPANS = ((0, 32), (192, 32), (32, 48), (144, 48), (80, 64))
CUTS = {0: "E", 3: "E", 6: "XL", 7: "XEL"}
SIZES = {"E": (224,), "EL": (160, 64), "XL": (64, 160), "XEL": (64, 96, 64)}
PIECES = []
PART = {}
for _i in range(8):
    _cut = CUTS.get(_i, "EL")
    _row = 0
    for _name, _size in zip(_cut, SIZES[_cut]):
        PART[str(_i) + _name] = len(PIECES)
        PIECES.append((_i, _row, _size))
        _row += _size
NP = len(PIECES)
POOL = 40

TREE = (
    ("z10", 32, 80), ("x10", 0, 32),
    ("z03a", 32, 48), ("z03b", 80, 32), ("x03", 0, 32), ("z01a", 32, 48), ("z01b", 80, 32), ("x01", 0, 32),
    ("x02a", 0, 16), ("x02b", 16, 16), ("z02a", 32, 48), ("z02b", 80, 32),
    ("z13a", 32, 48), ("z13b", 80, 32), ("z11a", 32, 48), ("z11b", 80, 32), ("x13", 0, 32), ("x11", 0, 32),
    ("x12a", 0, 16), ("x12b", 16, 16), ("z12a", 64, 16), ("z12b", 32, 32),
    ("z12c", 80, 16), ("z12d", 96, 16),
)
TREE_ID = {name: i for i, (name, _, _) in enumerate(TREE)}
NT = len(TREE)


def body_kernel(bands_all, w_hbm, p_hbm, occ_ref, species_ref, lin_hbm, bias_ref, lout_ref, app, tab,
                w, wt, pin, lraw, part, part16, ry, zs, zr, cfull, lin, dsend, dpart, drecv, xs, xall, appt, bd, bds,
                lsem, pool, tss, tsr, d2r, ryr, zsr, agr, dens_r, xsr, rounds):
    band = lax.axis_index("band")
    ga = lax.axis_index("ga")
    zh, x, c = band // 8, (band // 2) % 4, band % 2
    y, zl = ga // 2, ga % 2

    def at(dz=0, dx=0, dc=0, dy=0, dl=0):
        nzh, nx, nc = (zh + dz) % 2, (x + dx) % 4, (c + dc) % 2
        ny, nzl = (y + dy) % 4, (zl + dl) % 2
        return (nzh * 8 + nx * 2 + nc, ny * 2 + nzl)

    def slot_row(dz, dx, dc):
        nzh, nx, nc = (zh + dz) % 2, (x + dx) % 4, (c + dc) % 2
        return (nzh * 8 + nx * 2 + nc) * SLOT

    def pair_row(dz, dx):
        return (((zh + dz) % 2) * 4 + (x + dx) % 4) * PAIR

    def row_in_slot(first, count, dc=0):
        return jnp.where((c + dc) % 2 == 0, first, SLOT - first - count)

    def rows(ref, start, count):
        return ref.at[pl.ds(pl.multiple_of(start, 16), count)]

    wcopy = pltpu.make_async_copy(w_hbm, w, lsem.at[0])
    own_row = slot_row(0, 0, 0)
    pcopy = pltpu.make_async_copy(p_hbm, pin, lsem.at[1])
    lcopy = pltpu.make_async_copy(lin_hbm, lraw, lsem.at[2])
    pcopy.start()
    wcopy.start()
    lcopy.start()

    barrier = pltpu.get_barrier_semaphore()
    near = [at(dc=1), at(dx=1), at(dx=3), at(dz=1), at(dy=1), at(dy=3), at(dl=1)]
    for partner in near:
        pl.semaphore_signal(barrier, inc=1, device_id=partner, device_id_type=MESH)
    pcopy.wait()

    def pack(t, carry):
        cols = pl.ds(pl.multiple_of(t * 512, 512), 512)
        flat = pin[:, :, cols].astype(F32).reshape(4 * K, 512)
        full = jnp.concatenate([flat, jnp.zeros((SLOT - 4 * K, 512), F32)], axis=0)
        tab[pl.ds(pl.multiple_of(own_row, 16), SLOT), cols] = full.astype(BF16)
        return carry

    lax.fori_loop(0, 8, pack, 0)
    pl.semaphore_wait(barrier, len(near))

    def tell(r):
        for partner in near:
            pl.semaphore_signal(rounds.at[r], inc=1, device_id=partner, device_id_type=MESH)

    def known(r):
        pl.semaphore_wait(rounds.at[r], len(near))
        if r < 2:
            tell(r + 1)


    sends = []

    pooled = []

    def remote(src, dst, rs, device, own=None):
        n = len(pooled)
        if own is None:
            if n >= POOL:
                pooled[n - POOL].wait_send()
            own = pool.at[n % POOL]
            keep = pooled
        else:
            keep = sends
        copy = pltpu.make_async_remote_copy(
            src_ref=src, dst_ref=dst, send_sem=own, recv_sem=rs, device_id=device, device_id_type=MESH
        )
        copy.start()
        keep.append(copy)

    def arrived(dst, rs):
        pltpu.make_async_remote_copy(
            src_ref=dst, dst_ref=dst, send_sem=pool.at[0], recv_sem=rs, device_id=at(dc=1), device_id_type=MESH
        ).wait_recv()

    def tree_send(name, dz, dx, device):
        i = TREE_ID[name]
        _, first, count = TREE[i]
        ref = rows(tab, slot_row(dz, dx, 0) + row_in_slot(first, count), count)
        remote(ref, ref, tsr.at[i], device, tss.at[i])

    def tree_wait(name, dz, dx):
        i = TREE_ID[name]
        _, first, count = TREE[i]
        arrived(rows(tab, slot_row(dz, dx, 0) + row_in_slot(first, count), count), tsr.at[i])

    crossings = {}

    def crossing(i, part):
        first, count = ((0, SLOT), (0, 80), (80, 32), (0, 32), (32, 80), (32, 48))[part]
        return ORDER[i], first, count, crossings.setdefault((i, part), len(crossings))

    def across(i, part=0):
        (dz, dx), first, count, sem = crossing(i, part)
        ref = rows(tab, slot_row(dz, dx, 0) + row_in_slot(first, count), count)
        remote(ref, ref, d2r.at[sem], at(dc=1))

    def across_wait(i, part=0):
        (dz, dx), first, count, sem = crossing(i, part)
        arrived(rows(tab, slot_row(dz, dx, 1) + row_in_slot(first, count, 1), count), d2r.at[sem])

    right, left, over = at(dx=1), at(dx=3), at(dz=1)

    def project(s):
        i, first, count = PIECES[s]
        base = pair_row(*ORDER[i])

        def read(start, size):
            return tab[pl.ds(pl.multiple_of(base + start, 16), size), :]

        def half(t, carry):
            cols = pl.ds(pl.multiple_of(t * 256, 256), 256)

            def times(table):
                if i == 0:
                    dims, by = (((1,), (1,)), ((), ())), w[cols, :]
                else:
                    dims, by = (((1,), (0,)), ((), ())), wt[:, cols]
                return lax.dot_general(table, by, dims, preferred_element_type=F32)

            def keep(to, got):
                part[i, to:to + got.shape[0], cols] = got
                part16[i, to:to + got.shape[0], cols] = got.astype(BF16)

            spans = []
            to = 0
            for span in SPANS:
                if first <= to < first + count:
                    spans.append(span)
                to += span[1]
            if count == PAIR:
                got = times(read(0, PAIR))
                to = 0
                for start, size in spans:
                    keep(to, got[start:start + size])
                    to += size
            else:
                table = [read(*span) for span in spans]
                keep(first, times(table[0] if len(table) == 1 else jnp.concatenate(table, axis=0)))
            return carry

        lax.fori_loop(0, 2, half, 0)
        here = pl.ds(first, count)
        for dy in (2, 1, 3):
            lanes = pl.ds(pl.multiple_of(((y + dy) % 4) * 128, 128), 128)
            remote(part16.at[i, here, lanes], ry.at[i, 3 - dy, here], ryr.at[s], at(dy=dy))

    mine = pl.ds(pl.multiple_of(y * 128, 128), 128)

    def reduce_y(s):
        i, first, count = PIECES[s]
        here = pl.ds(first, count)
        total = part[i, here, mine]
        arrived(ry.at[i, :, here], ryr.at[s])
        for j in range(3):
            total = total + ry[i, j, here].astype(F32)
        part[i, here, mine] = total
        zs[i, here] = total.astype(BF16)
        remote(zs.at[i, here], zr.at[i, here], zsr.at[s], at(dl=1))

    def direct(s):
        return PIECES[s][0] == 7

    def block_at(s, dy):
        i, first, count = PIECES[s]
        lanes = pl.ds(pl.multiple_of(((y + dy) % 4) * 128, 128), 128)
        return pl.ds(pl.multiple_of(pair_row(*ORDER[i]) + first, 16), count), lanes

    def block(s, dy):
        return cfull.at[block_at(s, dy)]

    def reduce_z(s):
        i, first, count = PIECES[s]
        here = pl.ds(first, count)
        arrived(zr.at[i, here], zsr.at[s])
        cfull[block_at(s, 0)] = (part[i, here, mine] + zr[i, here].astype(F32)).astype(BF16)
        for dy in (2, 1, 3) if direct(s) else (1, 3):
            remote(block(s, 0), block(s, 0), agr.at[s, 3 - dy], at(dy=dy))

    def relay(s):
        for dy in (1, 3):
            arrived(block(s, dy), agr.at[s, dy - 1])
        dy = 1 + 2 * (s % 2)
        remote(block(s, dy), block(s, dy), agr.at[s, 1], at(dy=4 - dy))

    def gathered(s):
        for dy in (1, 2, 3) if direct(s) else (2,):
            arrived(block(s, dy), agr.at[s, dy - 1])

    def coef_of(pair, h):
        cuts = ((0, 32), (64, 48), (160, 32)) if h == 0 else ((192, 32), (112, 48), (32, 32))
        return jnp.concatenate([cfull[pl.ds(pl.multiple_of(pair * PAIR + a, 16), n), :] for a, n in cuts], axis=0)

    tell(0)
    tree_send("z10", 0, 0, over)
    tree_send("x03", 0, 0, right)
    tree_send("x01", 0, 0, left)
    across(0, 0)
    tree_send("z03a", 0, 0, right)
    tree_send("z01a", 0, 0, left)
    tree_send("z03b", 0, 0, right)
    tree_send("z01b", 0, 0, left)
    wcopy.wait()
    known(0)
    across_wait(0, 0)
    project(PART["0E"])
    tree_wait("x03", 0, 3)
    tree_send("x02a", 0, 3, right)
    tree_wait("x01", 0, 1)
    tree_send("x02b", 0, 1, left)
    reduce_y(PART["0E"])
    known(1)
    tree_send("x10", 0, 0, over)
    tree_send("x13", 0, 3, over)
    tree_send("x11", 0, 1, over)

    def turn_wave(t, carry):
        block = pl.ds(pl.multiple_of(t * 256, 256), 256)
        wt[block, :] = w[:, block].T
        return carry

    lax.fori_loop(0, w.shape[1] // 256, turn_wave, 0)
    lcopy.wait()
    for kind in range(SPECIES):
        turned = lraw[:, kind, :].T
        for k in range(K):
            lin[kind, k, 0:K, :] = turned[k * K:(k + 1) * K, :]
    tree_wait("z03a", 0, 3)
    across(1, 1)
    tree_wait("z01a", 0, 1)
    across(2, 1)
    tree_wait("z10", 1, 0)
    tree_send("z13a", 1, 0, right)
    tree_send("z11a", 1, 0, left)
    tree_send("z13b", 1, 0, right)
    tree_send("z11b", 1, 0, left)
    tree_send("z02a", 0, 3, right)
    reduce_z(PART["0E"])
    across_wait(1, 1)
    project(PART["1E"])
    across_wait(2, 1)
    project(PART["2E"])
    tree_wait("z03b", 0, 3)
    across(1, 2)
    tree_wait("z01b", 0, 1)
    tree_send("z02b", 0, 1, left)
    across(2, 2)
    tree_wait("x10", 1, 0)
    across(3, 0)
    across_wait(1, 2)
    project(PART["1L"])
    relay(PART["0E"])
    known(2)
    reduce_y(PART["1E"])
    across_wait(2, 2)
    project(PART["2L"])
    reduce_y(PART["2E"])
    across_wait(3, 0)
    project(PART["3E"])
    tree_wait("x02a", 0, 2)
    tree_wait("x02b", 0, 2)
    across(6, 3)
    reduce_y(PART["1L"])
    reduce_y(PART["2L"])
    tree_send("x12a", 0, 2, over)
    tree_send("x12b", 0, 2, over)
    across_wait(6, 3)
    project(PART["6X"])
    tree_wait("z13a", 1, 3)
    tree_send("z12a", 1, 3, right)
    tree_wait("z11a", 1, 1)
    tree_send("z12b", 1, 1, left)
    tree_wait("x13", 1, 3)
    across(4, 1)
    tree_wait("x11", 1, 1)
    across(5, 1)
    reduce_y(PART["3E"])
    across_wait(4, 1)
    project(PART["4E"])
    across_wait(5, 1)
    project(PART["5E"])
    reduce_z(PART["1E"])
    reduce_z(PART["2E"])
    tree_wait("z13b", 1, 3)
    tree_send("z12c", 1, 3, right)
    across(4, 2)
    tree_wait("z11b", 1, 1)
    tree_send("z12d", 1, 1, left)
    across(5, 2)
    reduce_z(PART["1L"])
    reduce_z(PART["2L"])
    reduce_y(PART["6X"])
    across_wait(4, 2)
    project(PART["4L"])
    reduce_y(PART["4E"])
    across_wait(5, 2)
    project(PART["5L"])
    reduce_z(PART["3E"])
    reduce_z(PART["6X"])
    relay(PART["1E"])
    relay(PART["2E"])
    tree_wait("x12a", 1, 2)
    tree_wait("x12b", 1, 2)
    across(7, 3)
    reduce_y(PART["5E"])
    reduce_z(PART["4E"])
    tree_wait("z02a", 0, 2)
    tree_wait("z02b", 0, 2)
    across(6, 4)
    across_wait(7, 3)
    project(PART["7X"])
    reduce_y(PART["4L"])
    reduce_y(PART["5L"])
    relay(PART["1L"])
    relay(PART["2L"])
    reduce_z(PART["5E"])
    across_wait(6, 4)
    project(PART["6L"])
    tree_wait("z12a", 1, 2)
    tree_wait("z12b", 1, 2)
    across(7, 5)
    reduce_z(PART["4L"])
    reduce_z(PART["5L"])
    across_wait(7, 5)
    project(PART["7E"])
    tree_wait("z12c", 1, 2)
    tree_wait("z12d", 1, 2)
    across(7, 2)
    relay(PART["3E"])
    relay(PART["6X"])
    reduce_y(PART["7X"])
    relay(PART["4E"])
    relay(PART["5E"])
    across_wait(7, 2)
    project(PART["7L"])
    reduce_y(PART["6L"])
    reduce_z(PART["7X"])
    reduce_y(PART["7E"])
    reduce_y(PART["7L"])
    reduce_z(PART["6L"])
    reduce_z(PART["7E"])
    reduce_z(PART["7L"])
    relay(PART["4L"])
    relay(PART["5L"])
    relay(PART["6L"])
    for s in range(NP):
        gathered(s)

    lane_atom = lax.broadcasted_iota(jnp.int32, (KP, SLOT), 1) % 4
    occ = occ_ref[...]
    for h in range(2):
        coef = coef_of(ga, h)
        weighted = coef.astype(F32) * occ
        high = weighted.astype(BF16)
        low = (weighted - high.astype(F32)).astype(BF16)
        dims = (((1,), (1,)), ((), ()))
        gram = lax.dot_general(high, coef, dims, preferred_element_type=F32) + lax.dot_general(
            low, coef, dims, preferred_element_type=F32
        )
        bd[0:SLOT, 0:SLOT] = gram
        packed = jnp.zeros((KP, SLOT), F32)
        for a in range(4):
            packed = packed + jnp.where(lane_atom == a, bd[pl.ds(a, KP, stride=4), :][:, 0:SLOT], 0.0)
        dsend[h, 0:KP, 0:SLOT] = packed
    remote(dsend.at[1 - c], drecv.at[7], dens_r.at[1], at(dc=1))
    arrived(drecv.at[7], dens_r.at[1])
    dpart[...] = dsend[c] + drecv[7]
    for dz, dx in ((1, 2), (0, 2), (1, 1), (1, 3), (1, 0), (0, 1), (0, 3)):
        j = dz * 4 + (4 - dx) % 4 - 1
        remote(dpart, drecv.at[j], dens_r.at[0], at(dz=dz, dx=dx))
    arrived(drecv.at[pl.ds(0, 7)], dens_r.at[0])
    density = dpart[...]
    for j in range(7):
        density = density + drecv[j]
    density = density * (1.0 / bands_all)

    lane = lax.broadcasted_iota(jnp.int32, (K, SLOT), 1)
    grad_t = jnp.zeros((K, SLOT), F32)
    slot = 2 * ga + c
    for a in range(4):
        kind = species_ref[4 * slot + a]
        acc = jnp.zeros((K, HID), F32)
        for k in range(K):
            acc = acc + density[0:K, 4 * k + a:4 * k + a + 1] * lin[kind, k, 0:K, :]
        preact = jnp.sum(acc, axis=0, keepdims=True) + bias_ref[kind]
        act = jnp.tanh(preact)
        slope = lout_ref[kind] * (1.0 - act * act)
        for k in range(K):
            column = jnp.sum(lin[kind, k, 0:K, :] * slope, axis=1, keepdims=True)
            grad_t = jnp.where(lane == 4 * k + a, column, grad_t)
    bd[...] = jnp.zeros(bd.shape, F32)
    pad = jnp.zeros((K, 128 - SLOT), F32)
    for a in range(4):
        bd[pl.ds(a, K, stride=4), :] = jnp.concatenate([jnp.where(lane % 4 == a, grad_t, 0.0), pad], axis=1)
    square = bd[0:SLOT, 0:SLOT]
    bd[0:SLOT, 0:SLOT] = square + square.T
    packed = jnp.zeros((KP, 128), F32)
    for a in range(4):
        packed = packed + bd[pl.ds(a, KP, stride=4), :]
    xs[0:KP, :] = packed
    xall[15] = xs[...]
    for dy in (2, 1, 3, 0):
        for dl in (1, 0):
            for dc in range(2):
                if dy or dl or dc:
                    j = (((4 - dy) % 4) * 2 + dl) * 2 + dc
                    remote(xs, xall.at[j - 1], xsr.at[0], at(dy=dy, dl=dl, dc=dc))
    arrived(xall.at[pl.ds(0, 15)], xsr.at[0])

    factor = 1.0 / math.sqrt(64 * K)
    rows4 = lax.broadcasted_iota(jnp.int32, (SLOT, SLOT), 0) % 4
    lanes4 = lax.broadcasted_iota(jnp.int32, (SLOT, SLOT), 1) % 4
    same = rows4 == lanes4

    def apply(pair, carry):
        for h in range(2):
            j = 2 * pair + h
            place = (((pair // 2 - y + 4) % 4 * 2 + (pair - zl + 2) % 2) * 2 + (h - c + 2) % 2 + 15) % 16
            for a in range(4):
                bds[j, pl.ds(a, KP, stride=4), :] = xall[place, 0:KP, :]
            full = jnp.where(same, bds[j, 0:SLOT, 0:SLOT], 0.0)
            high = full.astype(BF16)
            low = (full - high.astype(F32)).astype(BF16)
            coef = coef_of(pair, h)
            got = jnp.dot(high, coef, preferred_element_type=F32) + jnp.dot(low, coef, preferred_element_type=F32)
            appt[pl.ds(pl.multiple_of(j * SLOT, 16), SLOT), :] = (got * factor).astype(BF16)
        return carry

    lax.fori_loop(0, 8, apply, 0, unroll=2)

    def turn(j, carry):
        block = pl.ds(pl.multiple_of(j * 256, 256), 256)
        app[:, block] = appt[block, :].T
        return carry

    lax.fori_loop(0, 7, turn, 0)
    for copy in sends + pooled[-POOL:]:
        copy.wait_send()


def correct_kernel(app, tab, out_hbm, out, sems):
    def store(t):
        cols = pl.ds(pl.multiple_of(t * 1024, 1024), 1024)
        return pltpu.make_async_copy(out.at[:, cols], out_hbm.at[:, cols], sems.at[t])

    def one(t, carry):
        cols = pl.ds(pl.multiple_of(t * 1024, 1024), 1024)
        out[:, cols] = jnp.dot(app[...], tab[:, cols], preferred_element_type=F32).astype(BF16)
        store(t).start()
        return carry

    steps = out.shape[1] // 1024
    lax.fori_loop(0, steps, one, 0)
    for t in range(steps):
        store(t).wait()


def body(wave_coef, projector, occupation, species, layer_in, bias_in, layer_out):
    atoms_here, orbitals, gs = projector.shape
    bands = wave_coef.shape[0]
    bands_all = bands * lax.axis_size("band")
    assert atoms_here == 4 and orbitals == K and bands == 512
    hbm = pl.BlockSpec(memory_space=pltpu.HBM)
    vmem = pl.BlockSpec(memory_space=pltpu.VMEM)
    smem = pl.BlockSpec(memory_space=pltpu.SMEM)
    dma = pltpu.SemaphoreType.DMA
    applied, table = pl.pallas_call(
        functools.partial(body_kernel, bands_all),
        out_shape=[pltpu.VMEM((bands, 16 * SLOT), BF16), pltpu.VMEM((16 * SLOT, gs), BF16)],
        in_specs=[hbm, hbm, vmem, smem, hbm, vmem, vmem],
        out_specs=[vmem, vmem],
        scratch_shapes=[
            pltpu.VMEM((bands, gs), BF16),
            pltpu.VMEM((gs, bands), BF16),
            pltpu.VMEM((K, 4, gs), BF16),
            pltpu.VMEM((HID, SPECIES, K * K), F32),
            pltpu.VMEM((8, PAIR, bands), F32),
            pltpu.VMEM((8, PAIR, bands), BF16),
            pltpu.VMEM((8, 3, PAIR, 128), BF16),
            pltpu.VMEM((8, PAIR, 128), BF16),
            pltpu.VMEM((8, PAIR, 128), BF16),
            pltpu.VMEM((16 * SLOT, bands), BF16),
            pltpu.VMEM((SPECIES, K, 32, HID), F32),
            pltpu.VMEM((2, 32, 128), F32),
            pltpu.VMEM((32, 128), F32),
            pltpu.VMEM((8, 32, 128), F32),
            pltpu.VMEM((32, 128), F32),
            pltpu.VMEM((16, 32, 128), F32),
            pltpu.VMEM((16 * SLOT, bands), BF16),
            pltpu.VMEM((SLOT + 8, 128), F32),
            pltpu.VMEM((16, SLOT + 8, 128), F32),
            dma((3,)), dma((POOL,)), dma((NT,)), dma((NT,)), dma((16,)), dma((NP,)), dma((NP,)), dma((NP, 3)), dma((2,)), dma((1,)), pltpu.SemaphoreType.REGULAR((3,)),
        ],
        compiler_params=pltpu.CompilerParams(
            collective_id=0, has_side_effects=True, vmem_limit_bytes=44 * 2**20
        ),
        name="step",
    )(wave_coef, jnp.transpose(projector, (1, 0, 2)), occupation.reshape(1, bands), species,
      jnp.transpose(layer_in, (2, 0, 1)), bias_in.reshape(-1, 1, HID), layer_out.reshape(-1, 1, HID))
    return pl.pallas_call(
        correct_kernel,
        out_shape=jax.ShapeDtypeStruct((bands, gs), BF16),
        in_specs=[vmem, vmem],
        out_specs=pl.BlockSpec(memory_space=pl.ANY),
        scratch_shapes=[pltpu.VMEM((bands, gs), BF16), dma((gs // 1024,))],
        compiler_params=pltpu.CompilerParams(vmem_limit_bytes=16 * 2**20),
        name="correct",
    )(applied, table)


def solution(mesh):
    in_specs = (P("band", "ga"), P("band", None, "ga"), P("band"), P(), P(), P(), P())
    out_specs = P("band", "ga")
    return jax.shard_map(body, mesh=mesh, in_specs=in_specs, out_specs=out_specs, check_vma=False)
```

```python
import functools
import math

import jax
import jax.numpy as jnp
from jax import lax
from jax.experimental import pallas as pl
from jax.experimental.pallas import tpu as pltpu
from jax.sharding import PartitionSpec as P

MESH = pl.DeviceIdType.MESH
F32 = jnp.float32
BF16 = jnp.bfloat16

K = 27
KP = 28
SLOT = 4 * KP
PAIR = 2 * SLOT
HID = 100
SPECIES = 4

ORDER = ((0, 0), (0, 3), (0, 1), (1, 0), (1, 3), (1, 1), (0, 2), (1, 2))

SPANS = ((0, 32), (192, 32), (32, 48), (144, 48), (80, 64))
CUTS = {0: "E", 3: "E", 6: "XL", 7: "XEL"}
SIZES = {"E": (224,), "EL": (160, 64), "XL": (64, 160), "XEL": (64, 96, 64)}
PIECES = []
PART = {}
for _i in range(8):
    _cut = CUTS.get(_i, "EL")
    _row = 0
    for _name, _size in zip(_cut, SIZES[_cut]):
        PART[str(_i) + _name] = len(PIECES)
        PIECES.append((_i, _row, _size))
        _row += _size
NP = len(PIECES)
POOL = 40

TREE = (
    ("z10", 32, 80), ("x10", 0, 32),
    ("z03a", 32, 48), ("z03b", 80, 32), ("x03", 0, 32), ("z01a", 32, 48), ("z01b", 80, 32), ("x01", 0, 32),
    ("x02a", 0, 16), ("x02b", 16, 16), ("z02a", 32, 48), ("z02b", 80, 32),
    ("z13a", 32, 48), ("z13b", 80, 32), ("z11a", 32, 48), ("z11b", 80, 32), ("x13", 0, 32), ("x11", 0, 32),
    ("x12a", 0, 16), ("x12b", 16, 16), ("z12a", 64, 16), ("z12b", 32, 32),
    ("z12c", 80, 16), ("z12d", 96, 16),
)
TREE_ID = {name: i for i, (name, _, _) in enumerate(TREE)}
NT = len(TREE)


def body_kernel(bands_all, w_hbm, p_hbm, occ_ref, species_ref, lin_hbm, bias_ref, lout_ref, app, tab,
                w, wt, pin, lraw, part, part16, ry, zs, zr, cfull, lin, dsend, dpart, drecv, xs, xall, appt, bd, bds,
                lsem, pool, tss, tsr, d2r, ryr, zsr, agr, dens_r, xsr, rounds):
    band = lax.axis_index("band")
    ga = lax.axis_index("ga")
    zh, x, c = band // 8, (band // 2) % 4, band % 2
    y, zl = ga // 2, ga % 2

    def at(dz=0, dx=0, dc=0, dy=0, dl=0):
        nzh, nx, nc = (zh + dz) % 2, (x + dx) % 4, (c + dc) % 2
        ny, nzl = (y + dy) % 4, (zl + dl) % 2
        return (nzh * 8 + nx * 2 + nc, ny * 2 + nzl)

    def slot_row(dz, dx, dc):
        nzh, nx, nc = (zh + dz) % 2, (x + dx) % 4, (c + dc) % 2
        return (nzh * 8 + nx * 2 + nc) * SLOT

    def pair_row(dz, dx):
        return (((zh + dz) % 2) * 4 + (x + dx) % 4) * PAIR

    def row_in_slot(first, count, dc=0):
        return jnp.where((c + dc) % 2 == 0, first, SLOT - first - count)

    def rows(ref, start, count):
        return ref.at[pl.ds(pl.multiple_of(start, 16), count)]

    wcopy = pltpu.make_async_copy(w_hbm, w, lsem.at[0])
    own_row = slot_row(0, 0, 0)
    pcopy = pltpu.make_async_copy(p_hbm, pin, lsem.at[1])
    lcopy = pltpu.make_async_copy(lin_hbm, lraw, lsem.at[2])
    pcopy.start()
    wcopy.start()
    lcopy.start()

    barrier = pltpu.get_barrier_semaphore()
    near = [at(dc=1), at(dx=1), at(dx=3), at(dz=1), at(dy=1), at(dy=3), at(dl=1)]
    for partner in near:
        pl.semaphore_signal(barrier, inc=1, device_id=partner, device_id_type=MESH)
    pcopy.wait()

    def pack(t, carry):
        cols = pl.ds(pl.multiple_of(t * 512, 512), 512)
        flat = pin[:, :, cols].astype(F32).reshape(4 * K, 512)
        full = jnp.concatenate([flat, jnp.zeros((SLOT - 4 * K, 512), F32)], axis=0)
        tab[pl.ds(pl.multiple_of(own_row, 16), SLOT), cols] = full.astype(BF16)
        return carry

    lax.fori_loop(0, 8, pack, 0)
    pl.semaphore_wait(barrier, len(near))

    def tell(r):
        for partner in near:
            pl.semaphore_signal(rounds.at[r], inc=1, device_id=partner, device_id_type=MESH)

    def known(r):
        pl.semaphore_wait(rounds.at[r], len(near))
        if r < 2:
            tell(r + 1)


    sends = []

    pooled = []

    def remote(src, dst, rs, device, own=None):
        n = len(pooled)
        if own is None:
            if n >= POOL:
                pooled[n - POOL].wait_send()
            own = pool.at[n % POOL]
            keep = pooled
        else:
            keep = sends
        copy = pltpu.make_async_remote_copy(
            src_ref=src, dst_ref=dst, send_sem=own, recv_sem=rs, device_id=device, device_id_type=MESH
        )
        copy.start()
        keep.append(copy)

    def arrived(dst, rs):
        pltpu.make_async_remote_copy(
            src_ref=dst, dst_ref=dst, send_sem=pool.at[0], recv_sem=rs, device_id=at(dc=1), device_id_type=MESH
        ).wait_recv()

    def tree_send(name, dz, dx, device):
        i = TREE_ID[name]
        _, first, count = TREE[i]
        ref = rows(tab, slot_row(dz, dx, 0) + row_in_slot(first, count), count)
        remote(ref, ref, tsr.at[i], device, tss.at[i])

    def tree_wait(name, dz, dx):
        i = TREE_ID[name]
        _, first, count = TREE[i]
        arrived(rows(tab, slot_row(dz, dx, 0) + row_in_slot(first, count), count), tsr.at[i])

    crossings = {}

    def crossing(i, part):
        first, count = ((0, SLOT), (0, 80), (80, 32), (0, 32), (32, 80), (32, 48))[part]
        return ORDER[i], first, count, crossings.setdefault((i, part), len(crossings))

    def across(i, part=0):
        (dz, dx), first, count, sem = crossing(i, part)
        ref = rows(tab, slot_row(dz, dx, 0) + row_in_slot(first, count), count)
        remote(ref, ref, d2r.at[sem], at(dc=1))

    def across_wait(i, part=0):
        (dz, dx), first, count, sem = crossing(i, part)
        arrived(rows(tab, slot_row(dz, dx, 1) + row_in_slot(first, count, 1), count), d2r.at[sem])

    right, left, over = at(dx=1), at(dx=3), at(dz=1)

    def project(s):
        i, first, count = PIECES[s]
        base = pair_row(*ORDER[i])

        def read(start, size):
            return tab[pl.ds(pl.multiple_of(base + start, 16), size), :]

        def half(t, carry):
            cols = pl.ds(pl.multiple_of(t * 256, 256), 256)

            def times(table):
                if i == 0:
                    dims, by = (((1,), (1,)), ((), ())), w[cols, :]
                else:
                    dims, by = (((1,), (0,)), ((), ())), wt[:, cols]
                return lax.dot_general(table, by, dims, preferred_element_type=F32)

            def keep(to, got):
                part[i, to:to + got.shape[0], cols] = got
                part16[i, to:to + got.shape[0], cols] = got.astype(BF16)

            spans = []
            to = 0
            for span in SPANS:
                if first <= to < first + count:
                    spans.append(span)
                to += span[1]
            if count == PAIR:
                got = times(read(0, PAIR))
                to = 0
                for start, size in spans:
                    keep(to, got[start:start + size])
                    to += size
            else:
                table = [read(*span) for span in spans]
                keep(first, times(table[0] if len(table) == 1 else jnp.concatenate(table, axis=0)))
            return carry

        lax.fori_loop(0, 2, half, 0)
        here = pl.ds(first, count)
        for dy in (2, 1, 3):
            lanes = pl.ds(pl.multiple_of(((y + dy) % 4) * 128, 128), 128)
            remote(part16.at[i, here, lanes], ry.at[i, 3 - dy, here], ryr.at[s], at(dy=dy))

    mine = pl.ds(pl.multiple_of(y * 128, 128), 128)

    def reduce_y(s):
        i, first, count = PIECES[s]
        here = pl.ds(first, count)
        total = part[i, here, mine]
        arrived(ry.at[i, :, here], ryr.at[s])
        for j in range(3):
            total = total + ry[i, j, here].astype(F32)
        part[i, here, mine] = total
        zs[i, here] = total.astype(BF16)
        remote(zs.at[i, here], zr.at[i, here], zsr.at[s], at(dl=1))

    def direct(s):
        return PIECES[s][0] == 7

    def block_at(s, dy):
        i, first, count = PIECES[s]
        lanes = pl.ds(pl.multiple_of(((y + dy) % 4) * 128, 128), 128)
        return pl.ds(pl.multiple_of(pair_row(*ORDER[i]) + first, 16), count), lanes

    def block(s, dy):
        return cfull.at[block_at(s, dy)]

    def reduce_z(s):
        i, first, count = PIECES[s]
        here = pl.ds(first, count)
        arrived(zr.at[i, here], zsr.at[s])
        cfull[block_at(s, 0)] = (part[i, here, mine] + zr[i, here].astype(F32)).astype(BF16)
        for dy in (2, 1, 3) if direct(s) else (1, 3):
            remote(block(s, 0), block(s, 0), agr.at[s, 3 - dy], at(dy=dy))

    def relay(s):
        for dy in (1, 3):
            arrived(block(s, dy), agr.at[s, dy - 1])
        dy = 1 + 2 * (s % 2)
        remote(block(s, dy), block(s, dy), agr.at[s, 1], at(dy=4 - dy))

    def gathered(s):
        for dy in (1, 2, 3) if direct(s) else (2,):
            arrived(block(s, dy), agr.at[s, dy - 1])

    def coef_of(pair, h):
        cuts = ((0, 32), (64, 48), (160, 32)) if h == 0 else ((192, 32), (112, 48), (32, 32))
        return jnp.concatenate([cfull[pl.ds(pl.multiple_of(pair * PAIR + a, 16), n), :] for a, n in cuts], axis=0)

    tell(0)
    tree_send("z10", 0, 0, over)
    tree_send("x03", 0, 0, right)
    tree_send("x01", 0, 0, left)
    across(0, 0)
    tree_send("z03a", 0, 0, right)
    tree_send("z01a", 0, 0, left)
    tree_send("z03b", 0, 0, right)
    tree_send("z01b", 0, 0, left)
    wcopy.wait()
    known(0)
    across_wait(0, 0)
    project(PART["0E"])
    tree_wait("x03", 0, 3)
    tree_send("x02a", 0, 3, right)
    tree_wait("x01", 0, 1)
    tree_send("x02b", 0, 1, left)
    reduce_y(PART["0E"])
    known(1)
    tree_send("x10", 0, 0, over)
    tree_send("x13", 0, 3, over)
    tree_send("x11", 0, 1, over)

    def turn_wave(t, carry):
        block = pl.ds(pl.multiple_of(t * 256, 256), 256)
        wt[block, :] = w[:, block].T
        return carry

    lax.fori_loop(0, w.shape[1] // 256, turn_wave, 0)
    lcopy.wait()
    for kind in range(SPECIES):
        turned = lraw[:, kind, :].T
        for k in range(K):
            lin[kind, k, 0:K, :] = turned[k * K:(k + 1) * K, :]
    tree_wait("z03a", 0, 3)
    across(1, 1)
    tree_wait("z01a", 0, 1)
    across(2, 1)
    tree_wait("z10", 1, 0)
    tree_send("z13a", 1, 0, right)
    tree_send("z11a", 1, 0, left)
    tree_send("z13b", 1, 0, right)
    tree_send("z11b", 1, 0, left)
    tree_send("z02a", 0, 3, right)
    reduce_z(PART["0E"])
    across_wait(1, 1)
    project(PART["1E"])
    across_wait(2, 1)
    project(PART["2E"])
    tree_wait("z03b", 0, 3)
    across(1, 2)
    tree_wait("z01b", 0, 1)
    tree_send("z02b", 0, 1, left)
    across(2, 2)
    tree_wait("x10", 1, 0)
    across(3, 0)
    across_wait(1, 2)
    project(PART["1L"])
    relay(PART["0E"])
    known(2)
    reduce_y(PART["1E"])
    across_wait(2, 2)
    project(PART["2L"])
    reduce_y(PART["2E"])
    across_wait(3, 0)
    project(PART["3E"])
    tree_wait("x02a", 0, 2)
    tree_wait("x02b", 0, 2)
    across(6, 3)
    reduce_y(PART["1L"])
    reduce_y(PART["2L"])
    tree_send("x12a", 0, 2, over)
    tree_send("x12b", 0, 2, over)
    across_wait(6, 3)
    project(PART["6X"])
    tree_wait("z13a", 1, 3)
    tree_send("z12a", 1, 3, right)
    tree_wait("z11a", 1, 1)
    tree_send("z12b", 1, 1, left)
    tree_wait("x13", 1, 3)
    across(4, 1)
    tree_wait("x11", 1, 1)
    across(5, 1)
    reduce_y(PART["3E"])
    across_wait(4, 1)
    project(PART["4E"])
    across_wait(5, 1)
    project(PART["5E"])
    reduce_z(PART["1E"])
    reduce_z(PART["2E"])
    tree_wait("z13b", 1, 3)
    tree_send("z12c", 1, 3, right)
    across(4, 2)
    tree_wait("z11b", 1, 1)
    tree_send("z12d", 1, 1, left)
    across(5, 2)
    reduce_z(PART["1L"])
    reduce_z(PART["2L"])
    reduce_y(PART["6X"])
    across_wait(4, 2)
    project(PART["4L"])
    reduce_y(PART["4E"])
    across_wait(5, 2)
    project(PART["5L"])
    reduce_z(PART["3E"])
    reduce_z(PART["6X"])
    relay(PART["1E"])
    relay(PART["2E"])
    tree_wait("x12a", 1, 2)
    tree_wait("x12b", 1, 2)
    across(7, 3)
    reduce_y(PART["5E"])
    reduce_z(PART["4E"])
    tree_wait("z02a", 0, 2)
    tree_wait("z02b", 0, 2)
    across(6, 4)
    across_wait(7, 3)
    project(PART["7X"])
    reduce_y(PART["4L"])
    reduce_y(PART["5L"])
    relay(PART["1L"])
    relay(PART["2L"])
    reduce_z(PART["5E"])
    across_wait(6, 4)
    project(PART["6L"])
    tree_wait("z12a", 1, 2)
    tree_wait("z12b", 1, 2)
    across(7, 5)
    reduce_z(PART["4L"])
    reduce_z(PART["5L"])
    across_wait(7, 5)
    project(PART["7E"])
    tree_wait("z12c", 1, 2)
    tree_wait("z12d", 1, 2)
    across(7, 2)
    relay(PART["3E"])
    relay(PART["6X"])
    reduce_y(PART["7X"])
    relay(PART["4E"])
    relay(PART["5E"])
    across_wait(7, 2)
    project(PART["7L"])
    reduce_y(PART["6L"])
    reduce_z(PART["7X"])
    reduce_y(PART["7E"])
    reduce_z(PART["6L"])
    reduce_y(PART["7L"])
    reduce_z(PART["7E"])
    reduce_z(PART["7L"])
    relay(PART["4L"])
    relay(PART["5L"])
    relay(PART["6L"])
    for s in range(NP):
        gathered(s)

    lane_atom = lax.broadcasted_iota(jnp.int32, (KP, SLOT), 1) % 4
    occ = occ_ref[...]
    for h in range(2):
        coef = coef_of(ga, h)
        weighted = coef.astype(F32) * occ
        high = weighted.astype(BF16)
        low = (weighted - high.astype(F32)).astype(BF16)
        dims = (((1,), (1,)), ((), ()))
        gram = lax.dot_general(high, coef, dims, preferred_element_type=F32) + lax.dot_general(
            low, coef, dims, preferred_element_type=F32
        )
        bd[0:SLOT, 0:SLOT] = gram
        packed = jnp.zeros((KP, SLOT), F32)
        for a in range(4):
            packed = packed + jnp.where(lane_atom == a, bd[pl.ds(a, KP, stride=4), :][:, 0:SLOT], 0.0)
        dsend[h, 0:KP, 0:SLOT] = packed
    remote(dsend.at[1 - c], drecv.at[7], dens_r.at[1], at(dc=1))
    arrived(drecv.at[7], dens_r.at[1])
    dpart[...] = dsend[c] + drecv[7]
    for dz, dx in ((1, 2), (0, 2), (1, 1), (1, 3), (1, 0), (0, 1), (0, 3)):
        j = dz * 4 + (4 - dx) % 4 - 1
        remote(dpart, drecv.at[j], dens_r.at[0], at(dz=dz, dx=dx))
    arrived(drecv.at[pl.ds(0, 7)], dens_r.at[0])
    density = dpart[...]
    for j in range(7):
        density = density + drecv[j]
    density = density * (1.0 / bands_all)

    lane = lax.broadcasted_iota(jnp.int32, (K, SLOT), 1)
    grad_t = jnp.zeros((K, SLOT), F32)
    slot = 2 * ga + c
    for a in range(4):
        kind = species_ref[4 * slot + a]
        acc = jnp.zeros((K, HID), F32)
        for k in range(K):
            acc = acc + density[0:K, 4 * k + a:4 * k + a + 1] * lin[kind, k, 0:K, :]
        preact = jnp.sum(acc, axis=0, keepdims=True) + bias_ref[kind]
        act = jnp.tanh(preact)
        slope = lout_ref[kind] * (1.0 - act * act)
        for k in range(K):
            column = jnp.sum(lin[kind, k, 0:K, :] * slope, axis=1, keepdims=True)
            grad_t = jnp.where(lane == 4 * k + a, column, grad_t)
    bd[...] = jnp.zeros(bd.shape, F32)
    pad = jnp.zeros((K, 128 - SLOT), F32)
    for a in range(4):
        bd[pl.ds(a, K, stride=4), :] = jnp.concatenate([jnp.where(lane % 4 == a, grad_t, 0.0), pad], axis=1)
    square = bd[0:SLOT, 0:SLOT]
    bd[0:SLOT, 0:SLOT] = square + square.T
    packed = jnp.zeros((KP, 128), F32)
    for a in range(4):
        packed = packed + bd[pl.ds(a, KP, stride=4), :]
    xs[0:KP, :] = packed
    xall[15] = xs[...]
    for dy in (2, 1, 3, 0):
        for dl in (1, 0):
            for dc in range(2):
                if dy or dl or dc:
                    j = (((4 - dy) % 4) * 2 + dl) * 2 + dc
                    remote(xs, xall.at[j - 1], xsr.at[0], at(dy=dy, dl=dl, dc=dc))
    arrived(xall.at[pl.ds(0, 15)], xsr.at[0])

    factor = 1.0 / math.sqrt(64 * K)
    rows4 = lax.broadcasted_iota(jnp.int32, (SLOT, SLOT), 0) % 4
    lanes4 = lax.broadcasted_iota(jnp.int32, (SLOT, SLOT), 1) % 4
    same = rows4 == lanes4

    def apply(pair, carry):
        for h in range(2):
            j = 2 * pair + h
            place = (((pair // 2 - y + 4) % 4 * 2 + (pair - zl + 2) % 2) * 2 + (h - c + 2) % 2 + 15) % 16
            for a in range(4):
                bds[j, pl.ds(a, KP, stride=4), :] = xall[place, 0:KP, :]
            full = jnp.where(same, bds[j, 0:SLOT, 0:SLOT], 0.0)
            high = full.astype(BF16)
            low = (full - high.astype(F32)).astype(BF16)
            coef = coef_of(pair, h)
            got = jnp.dot(high, coef, preferred_element_type=F32) + jnp.dot(low, coef, preferred_element_type=F32)
            appt[pl.ds(pl.multiple_of(j * SLOT, 16), SLOT), :] = (got * factor).astype(BF16)
        return carry

    lax.fori_loop(0, 8, apply, 0, unroll=2)

    def turn(j, carry):
        block = pl.ds(pl.multiple_of(j * 256, 256), 256)
        app[:, block] = appt[block, :].T
        return carry

    lax.fori_loop(0, 7, turn, 0)
    for copy in sends + pooled[-POOL:]:
        copy.wait_send()


def correct_kernel(app, tab, out_hbm, out, sems):
    def store(t):
        cols = pl.ds(pl.multiple_of(t * 1024, 1024), 1024)
        return pltpu.make_async_copy(out.at[:, cols], out_hbm.at[:, cols], sems.at[t])

    def one(t, carry):
        cols = pl.ds(pl.multiple_of(t * 1024, 1024), 1024)
        out[:, cols] = jnp.dot(app[...], tab[:, cols], preferred_element_type=F32).astype(BF16)
        store(t).start()
        return carry

    steps = out.shape[1] // 1024
    lax.fori_loop(0, steps, one, 0)
    for t in range(steps):
        store(t).wait()


def body(wave_coef, projector, occupation, species, layer_in, bias_in, layer_out):
    atoms_here, orbitals, gs = projector.shape
    bands = wave_coef.shape[0]
    bands_all = bands * lax.axis_size("band")
    assert atoms_here == 4 and orbitals == K and bands == 512
    hbm = pl.BlockSpec(memory_space=pltpu.HBM)
    vmem = pl.BlockSpec(memory_space=pltpu.VMEM)
    smem = pl.BlockSpec(memory_space=pltpu.SMEM)
    dma = pltpu.SemaphoreType.DMA
    applied, table = pl.pallas_call(
        functools.partial(body_kernel, bands_all),
        out_shape=[pltpu.VMEM((bands, 16 * SLOT), BF16), pltpu.VMEM((16 * SLOT, gs), BF16)],
        in_specs=[hbm, hbm, vmem, smem, hbm, vmem, vmem],
        out_specs=[vmem, vmem],
        scratch_shapes=[
            pltpu.VMEM((bands, gs), BF16),
            pltpu.VMEM((gs, bands), BF16),
            pltpu.VMEM((K, 4, gs), BF16),
            pltpu.VMEM((HID, SPECIES, K * K), F32),
            pltpu.VMEM((8, PAIR, bands), F32),
            pltpu.VMEM((8, PAIR, bands), BF16),
            pltpu.VMEM((8, 3, PAIR, 128), BF16),
            pltpu.VMEM((8, PAIR, 128), BF16),
            pltpu.VMEM((8, PAIR, 128), BF16),
            pltpu.VMEM((16 * SLOT, bands), BF16),
            pltpu.VMEM((SPECIES, K, 32, HID), F32),
            pltpu.VMEM((2, 32, 128), F32),
            pltpu.VMEM((32, 128), F32),
            pltpu.VMEM((8, 32, 128), F32),
            pltpu.VMEM((32, 128), F32),
            pltpu.VMEM((16, 32, 128), F32),
            pltpu.VMEM((16 * SLOT, bands), BF16),
            pltpu.VMEM((SLOT + 8, 128), F32),
            pltpu.VMEM((16, SLOT + 8, 128), F32),
            dma((3,)), dma((POOL,)), dma((NT,)), dma((NT,)), dma((16,)), dma((NP,)), dma((NP,)), dma((NP, 3)), dma((2,)), dma((1,)), pltpu.SemaphoreType.REGULAR((3,)),
        ],
        compiler_params=pltpu.CompilerParams(
            collective_id=0, has_side_effects=True, vmem_limit_bytes=44 * 2**20
        ),
        name="step",
    )(wave_coef, jnp.transpose(projector, (1, 0, 2)), occupation.reshape(1, bands), species,
      jnp.transpose(layer_in, (2, 0, 1)), bias_in.reshape(-1, 1, HID), layer_out.reshape(-1, 1, HID))
    return pl.pallas_call(
        correct_kernel,
        out_shape=jax.ShapeDtypeStruct((bands, gs), BF16),
        in_specs=[vmem, vmem],
        out_specs=pl.BlockSpec(memory_space=pl.ANY),
        scratch_shapes=[pltpu.VMEM((bands, gs), BF16), dma((gs // 1024,))],
        compiler_params=pltpu.CompilerParams(vmem_limit_bytes=16 * 2**20),
        name="correct",
    )(applied, table)


def solution(mesh):
    in_specs = (P("band", "ga"), P("band", None, "ga"), P("band"), P(), P(), P(), P())
    out_specs = P("band", "ga")
    return jax.shard_map(body, mesh=mesh, in_specs=in_specs, out_specs=out_specs, check_vma=False)
```
